32 devices in a mesh: gx: 4 (over y, x), gy: 4 (over z), gz: 2 (over core).
Axes of the slice: x: 2, y: 2, z: 4, core: 2. Of those that a mesh axis runs over, the one named last changes fastest.
Arguments:
- coords: float32 [4, 4, 6, 3, 128], P('gx', 'gy', 'gz'), as said below
- polar: float32 [4, 4, 6, 128], P('gx', 'gy', 'gz'), may hold values from 0.3 to 1.2
- field: float32 [4, 4, 6, 6, 128], P('gx', 'gy', 'gz'), may hold values from -6 to 6
- atom_count: int32 [4, 4, 6], P('gx', 'gy', 'gz'), may hold values from 64 to 128, as said below
- pair_list: int32 [4, 4, 6, 13], P('gx', 'gy', 'gz'), may hold values from -1 to 26, as said below
Outputs:
- dipoles: float32 [4, 4, 6, 6, 128], P('gx', 'gy', 'gz')
- residual: float32 [4, 4, 6, 6, 128], P('gx', 'gy', 'gz')
The draws below stay inside these ranges and needn't reach their ends.
Inputs may be any that keep to these rules, and one draw needn't show every extreme that they name: `coords`: each coordinate lies within a quarter of 2.2 of its lattice site: atom slot a sits at 2.2 (a % 4 + 0.5, (a // 4) % 4 + 0.5, a // 16 + 0.5). `atom_count`: some block holds 128 atoms. `pair_list`: each block's row holds distinct codes above 13 in ascending order, followed by -1 in the unused entries.
All inputs are finite; a program needn't handle non-finite values.
Results may differ from the reference program's by a relative error of at most 0.0003.
Values sent between devices are 32-bit elements; how exact they have to be, the bound alone decides.
A program may use at most 64 MiB of HBM per device.

```python
import math
import jax
import jax.numpy as jnp
from jax import lax

ATOMS = 128
ITERS = 2
NBX = 4
NBY = 4
NBZ = 6


spacing = 2.2


def draw_coords(key, part):
    lattice_ids = jnp.arange(ATOMS, dtype=jnp.int32)
    lattice = jnp.stack([lattice_ids % 4, lattice_ids // 4 % 4, lattice_ids // 16]).astype(jnp.float32)
    lattice_pos = (lattice + 0.5) * spacing
    jitter = jax.random.uniform(key, (NBX, NBY, NBZ, 3, ATOMS), jnp.float32, -0.2, 0.2)
    return (lattice_pos + jitter * spacing).astype(jnp.float32)


def draw_atom_count(key, part):
    counts = jax.random.randint(key, (NBX, NBY, NBZ), ATOMS // 2, ATOMS + 1)
    return counts.at[0, 0, 0].set(ATOMS).astype(jnp.int32)


def draw_pair_list(key, part):
    dice_rolls = jax.random.randint(key, (NBX, NBY, NBZ, 13), 0, 100)
    density = jnp.arange(NBX, dtype=jnp.int32) * 60 // NBX + 30
    chosen = dice_rolls < density[:, None, None, None]
    forward_codes = jnp.arange(14, 27, dtype=jnp.int32)
    sort_keys = jnp.where(chosen, forward_codes, forward_codes + 100)
    ordered = jnp.sort(sort_keys, axis=-1)
    return jnp.where(ordered < 100, ordered, -1).astype(jnp.int32)


def shard_levels(stream_key, extent, pieces, least, top_value):
    def one(position, parts):
        draws = jax.random.uniform(jax.random.fold_in(jax.random.fold_in(stream_key, 6), position), (parts,), jnp.float32, least / len(pieces), top_value / len(pieces))
        return jnp.repeat(jnp.exp(draws), extent[position] // parts).reshape((-1,) + (1,) * (len(extent) - position - 1))

    gain = one(*pieces[0])
    for cut in pieces[1:]:
        gain = gain * one(*cut)
    return gain


def noise(rng, shape, scale, bound, split=(), held_as=jnp.bfloat16):
    result = jax.random.normal(rng, shape, jnp.float32) * scale
    if len(split) > 0:
        result = shard_levels(rng, shape, split, -0.22, 0.18) * result
    return jnp.clip(result, min=-bound, max=bound).astype(held_as)


def setup_inputs(seed: int = 0) -> dict:
    seeds = jax.random.split(jax.random.key(seed), 6)
    return {
        "coords": draw_coords(jax.random.fold_in(seeds[5], 71), 0),
        "polar": jnp.clip(jnp.exp(math.log(1.2) - 1.3862944 * jax.random.uniform(seeds[1], (NBX, NBY, NBZ, ATOMS), jnp.float32) ** shard_levels(seeds[1], (NBX, NBY, NBZ, ATOMS), ((0, 4), (1, 4), (2, 2)), -0.2, 0.2)), 0.3, 1.2),
        "field": noise(seeds[2], (NBX, NBY, NBZ, 6, ATOMS), 1.0, 6.0, ((0, 4), (1, 4), (2, 2)), jnp.float32),
        "atom_count": draw_atom_count(jax.random.fold_in(seeds[5], 71), 0),
        "pair_list": draw_pair_list(jax.random.fold_in(seeds[5], 71), 0),
    }


spacing = 2.2
cutoff_square = 49.0
thole = 0.39
highest = lax.Precision.HIGHEST

def pair_weights(geometry_row, geometry_col, offset_vec, self_flag):
    separation = offset_vec[:, None, None] + geometry_col[0:3][:, None, :] - geometry_row[0:3][:, :, None]
    range_square = lax.optimization_barrier(jnp.sum(separation * separation, axis=0))
    diagonal = self_flag * jnp.eye(geometry_row.shape[1], dtype=jnp.float32)
    weight_mask = geometry_row[4][:, None] * geometry_col[4][None, :] * (1.0 - diagonal)
    range_square = range_square + diagonal
    inverse_range = lax.rsqrt(range_square)
    inverse_cube = inverse_range * inverse_range * inverse_range
    damp_argument = thole * range_square * jnp.sqrt(range_square) * lax.rsqrt(geometry_row[3][:, None] * geometry_col[3][None, :])
    damping = jnp.exp(-damp_argument)
    lam_three = 1.0 - damping
    lam_five = 1.0 - (1.0 + damp_argument) * damping
    switch = jnp.square(jnp.maximum(1.0 - range_square / cutoff_square, 0.0))
    weight_three = weight_mask * switch * lam_three * inverse_cube
    weight_five = 3.0 * weight_mask * switch * lam_five * inverse_cube * inverse_range * inverse_range
    return (weight_three, weight_five, separation)

def field_rows(weight_three, weight_five, separation, dipole_col):
    dipole_sets = dipole_col.reshape(2, 3, -1)
    projected = jnp.einsum('cij,scj->sij', separation, dipole_sets, precision=highest)
    radial = jnp.einsum('ij,cij,sij->sci', weight_five, separation, projected, precision=highest)
    direct = jnp.einsum('ij,scj->sci', weight_three, dipole_sets, precision=highest)
    return (radial - direct).reshape(6, -1)

def block_fields(geometry, neighbour_geo, neighbour_dip, active, offset_vec, self_flag):

    def slab_fields(inputs):
        geo_slab, near_geo, near_dip, act_slab = inputs
        atom_slots = geo_slab.shape[-1]

        def single_pair(geometry_row, geometry_col, dipole_col, switch_on):
            weight_three, weight_five, separation = pair_weights(geometry_row, geometry_col, offset_vec, self_flag)
            return switch_on * field_rows(weight_three, weight_five, separation, dipole_col)
        fields = jax.vmap(single_pair)(geo_slab.reshape(-1, 5, atom_slots), near_geo.reshape(-1, 5, atom_slots), near_dip.reshape(-1, 6, atom_slots), act_slab.reshape(-1))
        return fields.reshape(geo_slab.shape[0:2] + (6, atom_slots))
    return lax.map(slab_fields, (geometry, neighbour_geo, neighbour_dip, active))

def apply_operator(vector, geometry, forward, box_size):
    accumulated = jnp.zeros_like(vector)
    for pair_code in range(27):
        roll_by = (1 - pair_code // 9, 1 - pair_code // 3 % 3, 1 - pair_code % 3)
        neighbour_geo = jnp.roll(geometry, roll_by, axis=(0, 1, 2))
        neighbour_dip = jnp.roll(vector, roll_by, axis=(0, 1, 2))
        if pair_code == 13:
            active = jnp.ones(forward.shape[0:3], jnp.float32)
        elif pair_code > 13:
            active = forward[..., pair_code]
        else:
            active = jnp.roll(forward[..., 26 - pair_code], roll_by, axis=(0, 1, 2))
        offset_vec = box_size * jnp.array([pair_code // 9 - 1, pair_code // 3 % 3 - 1, pair_code % 3 - 1], jnp.float32)
        self_flag = 1.0 if pair_code == 13 else 0.0
        accumulated = accumulated + block_fields(geometry, neighbour_geo, neighbour_dip, active, offset_vec, self_flag)
    return vector / geometry[:, :, :, 3:4, :] - accumulated

def set_sums(former, latter):
    product = (former * latter).reshape(former.shape[0:3] + (2, 3, former.shape[-1]))
    return lax.optimization_barrier(jnp.sum(product, axis=(0, 1, 2, 4, 5)))

def spread(values):
    return jnp.repeat(values, 3)[:, None]

def reference(coords, polar, field, atom_count, pair_list):
    atom_slots = coords.shape[-1]
    slot_ids = jnp.arange(atom_slots, dtype=jnp.int32)
    atom_mask = (slot_ids[None, None, None, :] < atom_count[..., None]).astype(jnp.float32)
    geometry = jnp.concatenate([coords, polar[..., None, :], atom_mask[..., None, :]], axis=3)
    pair_codes = jnp.arange(27, dtype=jnp.int32)
    forward = jnp.any(pair_list[..., :, None] == pair_codes, axis=-2).astype(jnp.float32)
    box_size = jnp.array([4.0 * spacing, 4.0 * spacing, spacing * (atom_slots // 16)], jnp.float32)
    polar_col = geometry[:, :, :, 3:4, :]
    source = field * atom_mask[..., None, :]
    dipoles = polar_col * source
    residual = source - apply_operator(dipoles, geometry, forward, box_size)
    precond = polar_col * residual
    direction = precond
    norm_now = set_sums(residual, precond)
    for iteration in range(ITERS):
        operated = apply_operator(direction, geometry, forward, box_size)
        step_len = spread(norm_now / set_sums(direction, operated))
        dipoles = dipoles + step_len * direction
        residual = residual - step_len * operated
        if iteration + 1 < ITERS:
            precond = polar_col * residual
            norm_next = set_sums(residual, precond)
            direction = precond + spread(norm_next / norm_now) * direction
            norm_now = norm_next
    return (dipoles, residual)
```

```python
import functools

import jax
import jax.numpy as jnp
from jax import lax
from jax.experimental import pallas as pl
from jax.experimental.pallas import tpu as pltpu
from jax.sharding import PartitionSpec as P

MESH = pl.DeviceIdType.MESH
AXES = ("gx", "gy", "gz")
spacing = 2.2
cutoff_square = 49.0
thole = 0.39
SIDE = 4
GROUP = SIDE * SIDE
REACH = 3
SHIFTS = 2 * REACH + 1
COLUMNS = [(cx, cy) for cx in (-1, 0, 1) for cy in (-1, 0, 1)]
CENTRE = COLUMNS.index((0, 0))
SIDES = [index for index in range(9) if index != CENTRE]


def gather(value, index):
    return jnp.take_along_axis(value, index, axis=1, mode="promise_in_bounds")


def kernel(
    sizes, deep, pairs_ref, count_ref, coords_ref, polar_ref, field_ref, dip_out, res_out,
    send_dip, send_geo, main_dip, above_dip, below_dip, main_geo, above_geo, below_geo,
    near, near_geo, switch, tensor, sums_out, sums_in, send_sems, recv_sems, geo_send, geo_recv,
    sum_send, sum_recv,
):
    total_devices = sizes[0] * sizes[1] * sizes[2]
    me = [lax.axis_index(name) for name in AXES]
    my_id = (me[0] * sizes[1] + me[1]) * sizes[2] + me[2]

    def device_at(linear):
        return (
            linear // (sizes[1] * sizes[2]),
            linear // sizes[2] % sizes[1],
            linear % sizes[2],
        )

    def neighbour(cx, cy, cz):
        return tuple(
            lax.rem(place + step + size, size)
            for place, step, size in zip(me, (cx, cy, cz), sizes)
        )

    barrier = pltpu.get_barrier_semaphore()
    for step in range(1, total_devices):
        other = lax.rem(my_id + step, total_devices)
        pl.semaphore_signal(barrier, inc=1, device_id=device_at(other), device_id_type=MESH)

    lane = lax.broadcasted_iota(jnp.int32, (8, 128), 1)
    row = lax.broadcasted_iota(jnp.int32, (8, 128), 0)
    group = lane // GROUP
    place_y = lane // SIDE % SIDE
    place_x = lane % SIDE
    site = lane % GROUP
    shift_x = group - REACH
    unpack = GROUP * row + site

    def rows_of(line):
        return gather(jnp.broadcast_to(line, (8, 128)), unpack)

    site_x = spacing * (place_x.astype(jnp.float32) + 0.5)
    site_y = spacing * (place_y.astype(jnp.float32) + 0.5)
    site_z = spacing * (row.astype(jnp.float32) + 0.5)

    def packed(parts):
        value = parts[0]
        for index in range(1, len(parts)):
            value = jnp.where(group == index, parts[index], value)
        return value

    own, polar, mask, source, dipoles = [], [], [], [], []
    for k in range(deep):
        places = [
            rows_of(coords_ref[3 * k + part]) - offset
            for part, offset in enumerate((site_x, site_y, site_z))
        ]
        polar_k = rows_of(polar_ref[k])
        mask_k = jnp.where(unpack < count_ref[k], 1.0, 0.0)
        source_k = [rows_of(field_ref[6 * k + part]) * mask_k for part in range(6)]
        dipoles_k = [polar_k * value for value in source_k]
        root = lax.rsqrt(polar_k)
        slot = lane - 5 * GROUP + 14
        flag = pairs_ref[k, 0] == slot
        for entry in range(1, 13):
            flag = jnp.logical_or(flag, pairs_ref[k, entry] == slot)
        flags = jnp.where(flag, 1.0, 0.0)
        send_dip[0, pl.ds(8 * k, 8), :] = packed(dipoles_k)
        send_geo[pl.ds(8 * k, 8), :] = packed(places + [root, mask_k, flags])
        own.append(places + [thole * root])
        polar.append(polar_k)
        mask.append(mask_k)
        source.append(source_k)
        dipoles.append(dipoles_k)

    pl.semaphore_wait(barrier, total_devices - 1)

    def exchange(source_ref, main, above, below, send_sem, recv_sem):
        copies = []

        def send(src, dst, number, target):
            copy = pltpu.make_async_remote_copy(
                src_ref=src,
                dst_ref=dst,
                send_sem=send_sem.at[number],
                recv_sem=recv_sem.at[number],
                device_id=target,
                device_id_type=MESH,
            )
            copy.start()
            copies.append(copy)

        order = sorted(range(9), key=lambda index: -abs(COLUMNS[index][0]) - abs(COLUMNS[index][1]))
        for index in order:
            cx, cy = COLUMNS[index]
            there = COLUMNS.index((-cx, -cy))
            if index != CENTRE:
                send(source_ref, main.at[there], there, neighbour(cx, cy, 0))
            send(
                source_ref.at[pl.ds(0, 8)], above.at[there], 9 + there, neighbour(cx, cy, -1)
            )
            send(
                source_ref.at[pl.ds(8 * (deep - 1), 8)], below.at[there], 18 + there,
                neighbour(cx, cy, 1),
            )
        return copies

    def column_tiles(source_ref, main, above, below, index):
        halo = jnp.where(row < 4, above[index], below[index])
        tiles = [halo]
        for k in range(deep):
            if index == CENTRE:
                tiles.append(source_ref[pl.ds(8 * k, 8), :])
            else:
                tiles.append(main[index, pl.ds(8 * k, 8), :])
        return tiles

    reached_x = place_x + shift_x
    turn_x = [GROUP * part + SIDE * place_y + (reached_x & (SIDE - 1)) for part in range(6)]
    turn_y = [GROUP * group + SIDE * ((place_y + step) & (SIDE - 1)) + place_x for step in range(SIDE)]

    def spread_out(source_ref, main, above, below, out, parts):
        for part in range(parts):
            lined = {}
            for cy in (-1, 0, 1):
                columns = [
                    column_tiles(source_ref, main, above, below, COLUMNS.index((cx, cy)))
                    for cx in (-1, 0, 1)
                ]
                for v in range(deep + 1):
                    low, mid, high = (gather(columns[cx][v], turn_x[part]) for cx in range(3))
                    value = jnp.where(reached_x < 0, low, jnp.where(reached_x < SIDE, mid, high))
                    lined[cy, v] = value
            for number in range(SHIFTS):
                sy = number - REACH
                for v in range(deep + 1):
                    value = lined[0, v]
                    if sy > 0:
                        value = jnp.where(place_y < sy, lined[1, v], value)
                    if sy < 0:
                        value = jnp.where(place_y >= SIDE + sy, lined[-1, v], value)
                    if sy != 0:
                        value = gather(value, turn_y[sy % SIDE])
                    out[number, part, pl.ds(8 * v, 8), :] = value
                    if v == 0:
                        out[number, part, pl.ds(8 * (deep + 1), 8), :] = value

    def finish(sums, vector):
        result = []
        for k in range(deep):
            values = []
            for part in range(6):
                value = sums[k][part]
                for step in (64, 32, 16):
                    value = value + pltpu.roll(value, step, 1)
                values.append(vector[k][part] / polar[k] - mask[k] * value)
            result.append(values)
        return result

    def nest(flat):
        return [[flat[6 * k + part] for part in range(6)] for k in range(deep)]

    zeros = tuple(jnp.zeros((8, 128), jnp.float32) for _ in range(6 * deep))

    def contract(sums, k, parts, vec):
        xx, yy, zz, xy, xz, yz = parts
        for first in (0, 3):
            vx, vy, vz = vec[first : first + 3]
            base = 6 * k + first
            sums[base] = sums[base] + (xx * vx + xy * vy + xz * vz)
            sums[base + 1] = sums[base + 1] + (xy * vx + yy * vy + yz * vz)
            sums[base + 2] = sums[base + 2] + (xz * vx + yz * vy + zz * vz)

    def apply(vec_ref):
        def step(number, sums):
            sums = list(sums)
            for k in range(deep):
                for index in range(SHIFTS):
                    span = pl.ds(8 * k + 8 + index - REACH, 8)
                    parts = [tensor[number, k * SHIFTS + index, part] for part in range(6)]
                    vec = [vec_ref[number, part, span, :] for part in range(6)]
                    contract(sums, k, parts, vec)
            return tuple(sums)

        return nest(lax.fori_loop(0, SHIFTS, step, zeros))

    far_x = spacing * shift_x.astype(jnp.float32)

    def build(vec_ref):
        def step(number, sums):
            sums = list(sums)
            sy = number - REACH
            far_y = spacing * sy.astype(jnp.float32)
            is_self = jnp.logical_and(group == REACH, sy == 0)
            for k in range(deep):
                own_x = own[k][0] - far_x
                own_y = own[k][1] - far_y
                for index in range(SHIFTS):
                    start = 8 + index - REACH
                    span = pl.ds(8 * k + start, 8)
                    dx = near_geo[number, 0, span, :] - own_x
                    dy = near_geo[number, 1, span, :] - own_y
                    dz = near_geo[number, 2, span, :] - (own[k][2] - spacing * (index - REACH))
                    weight = switch[k, number, pl.ds(start, 8), :]
                    if index == REACH:
                        weight = jnp.where(is_self, 0.0, weight)
                    square = jnp.maximum(dx * dx + dy * dy + dz * dz, 1.0)
                    inverse = lax.rsqrt(square)
                    inverse_square = inverse * inverse
                    damp = square * square * inverse * (near_geo[number, 3, span, :] * own[k][3])
                    damping = jnp.exp(-damp)
                    fade = jnp.maximum(1.0 - square * (1.0 / cutoff_square), 0.0)
                    scale = fade * fade * (inverse_square * inverse) * weight
                    three = scale * (1.0 - damping)
                    five = (1.0 - (1.0 + damp) * damping) * scale * (3.0 * inverse_square)
                    tx, ty, tz = five * dx, five * dy, five * dz
                    parts = (
                        tx * dx - three, ty * dy - three, tz * dz - three, tx * dy, tx * dz, ty * dz
                    )
                    for part in range(6):
                        tensor[number, k * SHIFTS + index, part] = parts[part]
                    vec = [vec_ref[number, part, span, :] for part in range(6)]
                    contract(sums, k, parts, vec)
            return tuple(sums)

        return nest(lax.fori_loop(0, SHIFTS, step, zeros))

    def build_switch():
        def code_of(cx, cy, cz):
            return 9 * (cx + 1) + 3 * (cy + 1) + cz + 1

        def flag_lane(code):
            return 5 * GROUP + code - 14

        def pick(tile, at):
            return gather(tile, jnp.full((8, 128), at, jnp.int32))

        tiles = {
            index: column_tiles(send_geo, main_geo, above_geo, below_geo, index)
            for index in range(9)
            if COLUMNS[index] < (0, 1)
        }
        for k in range(deep):
            for cz in (-1, 0, 1):
                v = (k + 1 + cz) % (deep + 1)
                active = {}
                for cy in (-1, 0, 1):
                    sides = []
                    for cx in (-1, 0, 1):
                        code = code_of(cx, cy, cz)
                        if code == 13:
                            sides.append(jnp.ones((8, 128), jnp.float32))
                        elif code > 13:
                            sides.append(pick(tiles[CENTRE][k + 1], flag_lane(code)))
                        else:
                            near_tile = tiles[COLUMNS.index((cx, cy))][v]
                            sides.append(pick(near_tile, flag_lane(26 - code)))
                    value = jnp.where(
                        reached_x < 0, sides[0], jnp.where(reached_x < SIDE, sides[1], sides[2])
                    )
                    active[cy] = jnp.where(group < SHIFTS, value, 0.0)
                for number in range(SHIFTS):
                    sy = number - REACH
                    value = active[0]
                    if sy > 0:
                        value = jnp.where(place_y + sy >= SIDE, active[1], value)
                    if sy < 0:
                        value = jnp.where(place_y + sy < 0, active[-1], value)
                    row_mask = near_geo[number, 4, pl.ds(8 * (k + 1 + cz), 8), :]
                    switch[k, number, pl.ds(8 * (cz + 1), 8), :] = value * row_mask

    def partial(first, second, dipole_set):
        value = None
        for k in range(deep):
            for part in range(3 * dipole_set, 3 * dipole_set + 3):
                term = first[k][part] * second[k][part]
                value = term if value is None else value + term
        return value

    def start_sums(number, values):
        line = jnp.sum(packed(values), axis=0, keepdims=True)
        sums_out[number] = line
        sums_in[number, my_id] = line
        copies = []
        for step in range(1, total_devices):
            other = lax.rem(my_id + step, total_devices)
            copy = pltpu.make_async_remote_copy(
                src_ref=sums_out.at[number],
                dst_ref=sums_in.at[number, my_id],
                send_sem=sum_send.at[number, step],
                recv_sem=sum_recv.at[number, step],
                device_id=device_at(other),
                device_id_type=MESH,
            )
            copy.start()
            copies.append(copy)
        return copies

    def end_sums(number, copies, amount):
        for copy in copies:
            copy.wait_recv()
        lines = [sums_in[number, index] for index in range(total_devices)]
        while len(lines) > 1:
            lines = [
                lines[index] + lines[index + 1] if index + 1 < len(lines) else lines[index]
                for index in range(0, len(lines), 2)
            ]
        line = lines[0]
        line_group = lax.broadcasted_iota(jnp.int32, (1, 128), 1) // GROUP
        return [
            jnp.broadcast_to(
                jnp.sum(jnp.where(line_group == index, line, 0.0), axis=1, keepdims=True), (8, 128)
            )
            for index in range(amount)
        ]

    def each(function, *vectors):
        return [
            [function(k, part, *(vector[k][part] for vector in vectors)) for part in range(6)]
            for k in range(deep)
        ]

    started = []
    geo_copies = exchange(send_geo, main_geo, above_geo, below_geo, geo_send, geo_recv)
    started += geo_copies

    def vector_exchange(phase):
        refs = (send_dip.at[phase], main_dip.at[phase], above_dip.at[phase], below_dip.at[phase])
        copies = exchange(*refs, send_sems.at[phase], recv_sems.at[phase])
        started.extend(copies)
        return refs, copies

    def arrive(refs, copies):
        for copy in copies:
            copy.wait_recv()
        spread_out(*refs, near, 6)

    refs, copies = vector_exchange(0)
    for copy in geo_copies:
        copy.wait_recv()
    spread_out(send_geo, main_geo, above_geo, below_geo, near_geo, 5)
    build_switch()
    arrive(refs, copies)
    image = finish(build(near), dipoles)
    residual = each(lambda k, part, s, a: s - a, source, image)
    precond = each(lambda k, part, r: polar[k] * r, residual)
    for k in range(deep):
        send_dip[1, pl.ds(8 * k, 8), :] = packed(precond[k])
    arrive(*vector_exchange(1))
    image = finish(apply(near), precond)
    turned = each(lambda k, part, q: polar[k] * q, image)
    for k in range(deep):
        send_dip[2, pl.ds(8 * k, 8), :] = packed(turned[k])
    refs, copies = vector_exchange(2)
    first_sums = start_sums(
        0,
        [partial(residual, precond, s) for s in range(2)]
        + [partial(precond, image, s) for s in range(2)],
    )
    started += first_sums
    arrive(refs, copies)
    turned_image = finish(apply(near), turned)
    totals = end_sums(0, first_sums, 4)
    norm, curve = totals[0:2], totals[2:4]
    gamma = [norm[s] / curve[s] for s in range(2)]
    dipoles = each(lambda k, part, d, p: d + gamma[part // 3] * p, dipoles, precond)
    residual = each(lambda k, part, r, q: r - gamma[part // 3] * q, residual, image)
    second = each(lambda k, part, r: polar[k] * r, residual)
    second_image = each(lambda k, part, q, t: q - gamma[part // 3] * t, image, turned_image)
    last_sums = start_sums(
        1,
        [partial(residual, second, s) for s in range(2)]
        + [partial(second, second_image, s) for s in range(2)]
        + [partial(second, image, s) for s in range(2)]
        + [partial(precond, second_image, s) for s in range(2)],
    )
    started += last_sums
    totals = end_sums(1, last_sums, 8)
    ratio = [totals[s] / norm[s] for s in range(2)]
    gamma = [
        totals[s]
        / (totals[2 + s] + ratio[s] * (totals[4 + s] + totals[6 + s] + ratio[s] * curve[s]))
        for s in range(2)
    ]
    for k in range(deep):
        for part in range(6):
            s = part // 3
            direction = second[k][part] + ratio[s] * precond[k][part]
            along = second_image[k][part] + ratio[s] * image[k][part]
            for out, value in (
                (dip_out, dipoles[k][part] + gamma[s] * direction),
                (res_out, residual[k][part] - gamma[s] * along),
            ):
                line = jnp.sum(jnp.where(group == row, value, 0.0), axis=0, keepdims=True)
                out[6 * k + part] = line
    for copy in started:
        copy.wait_send()


def on_device(sizes, coords, polar, field, atom_count, pair_list):
    deep, slots = coords.shape[2], coords.shape[-1]
    assert coords.shape[0:2] == (1, 1) and slots == 128
    vmem = pl.BlockSpec(memory_space=pltpu.VMEM)
    smem = pl.BlockSpec(memory_space=pltpu.SMEM)
    rows = 8 * deep
    total = sizes[0] * sizes[1] * sizes[2]

    def buffer(*shape):
        return pltpu.VMEM(shape, jnp.float32)

    line = jax.ShapeDtypeStruct((6 * deep, 1, slots), jnp.float32)
    dma = pltpu.SemaphoreType.DMA
    dipoles, residual = pl.pallas_call(
        functools.partial(kernel, sizes, deep),
        out_shape=(line, line),
        in_specs=[smem, smem, vmem, vmem, vmem],
        out_specs=(vmem, vmem),
        scratch_shapes=[
            buffer(3, rows, slots),
            buffer(rows, slots),
            buffer(3, 9, rows, slots),
            buffer(3, 9, 8, slots),
            buffer(3, 9, 8, slots),
            buffer(9, rows, slots),
            buffer(9, 8, slots),
            buffer(9, 8, slots),
            buffer(SHIFTS, 6, rows + 16, slots),
            buffer(SHIFTS, 5, rows + 16, slots),
            buffer(deep, SHIFTS, 24, slots),
            buffer(SHIFTS, SHIFTS * deep, 6, 8, slots),
            buffer(2, 1, slots),
            buffer(2, total, 1, slots),
            dma((3, 27)),
            dma((3, 27)),
            dma((27,)),
            dma((27,)),
            dma((2, total)),
            dma((2, total)),
        ],
        compiler_params=pltpu.CompilerParams(collective_id=0, has_side_effects=True),
    )(
        pair_list.reshape(deep, 13),
        atom_count.reshape(deep),
        coords.reshape(3 * deep, 1, slots),
        polar.reshape(deep, 1, slots),
        field.reshape(6 * deep, 1, slots),
    )
    return dipoles.reshape(field.shape), residual.reshape(field.shape)


def solution(mesh):
    sizes = tuple(mesh.shape[name] for name in AXES)
    block = P(*AXES, None, None)
    return jax.shard_map(
        functools.partial(on_device, sizes),
        mesh=mesh,
        in_specs=(block, P(*AXES, None), block, P(*AXES), P(*AXES, None)),
        out_specs=(block, block),
        check_vma=False,
    )
```

```python
import functools

import jax
import jax.numpy as jnp
from jax import lax
from jax.experimental import pallas as pl
from jax.experimental.pallas import tpu as pltpu
from jax.sharding import PartitionSpec as P

MESH = pl.DeviceIdType.MESH
AXES = ("gx", "gy", "gz")
spacing = 2.2
cutoff_square = 49.0
thole = 0.39
SIDE = 4
GROUP = SIDE * SIDE
REACH = 3
SHIFTS = range(-REACH, REACH + 1)
SPAN = 2 * REACH + 1
COLUMNS = [(cx, cy) for cx in (-1, 0, 1) for cy in (-1, 0, 1)]
EDGE = 12
OWN = (0, 48)
LOW = ((48, 60, 72), (36, 96, 108))
HIGH = ((84, 96, 108), (0, 12, 24))
RIDE_LOW = 0
RIDE_HIGH = 36
FLAGS = 4


def gather(value, index):
    return jnp.take_along_axis(value, index, axis=1, mode="promise_in_bounds")


def flag_slot(flag):
    return 4 * flag if flag < 4 else 4 * ((flag - 4) // 3) + 1 + (flag - 4) % 3


def plan(deep, rings):
    riders = [k for k in range(deep) if k % 3 == 2]
    tile_of, tiles = {}, 0
    for k in range(deep):
        if k not in riders:
            tile_of[k] = tiles
            tiles += 1
    slots, total = {}, 0
    for column in COLUMNS:
        if column != (0, 0):
            slots[column] = total
            total += tiles if column[0] else deep
    halos = {}
    for column in COLUMNS:
        halos[column] = total
        total += rings
    return riders, tile_of, tiles, slots, halos, total


def kernel(
    sizes, deep, pairs_hbm, count_hbm, coords_hbm, polar_hbm, field_hbm, dip_out, res_out,
    pairs_ref, count_ref, coords_ref, polar_ref, field_ref, send, held, near, near_geo, own_ref,
    switch, tensor, sums_out, sums_in, load_sems, send_sems, recv_sems, sum_send, sum_recv,
):
    total_devices = sizes[0] * sizes[1] * sizes[2]
    rings = 1 if sizes[2] == 2 else 2
    riders, tile_of, tiles, slots, halos, total_tiles = plan(deep, rings)
    me = [lax.axis_index(name) for name in AXES]
    my_id = (me[0] * sizes[1] + me[1]) * sizes[2] + me[2]
    scope = jax.named_scope

    def device_at(linear):
        return (
            linear // (sizes[1] * sizes[2]),
            linear // sizes[2] % sizes[1],
            linear % sizes[2],
        )

    def neighbour(cx, cy, cz):
        return tuple(
            lax.rem(place + step + size, size)
            for place, step, size in zip(me, (cx, cy, cz), sizes)
        )

    with scope("signal"):
        barrier = pltpu.get_barrier_semaphore()
        for step in range(1, total_devices):
            other = lax.rem(my_id + step, total_devices)
            pl.semaphore_signal(barrier, inc=1, device_id=device_at(other), device_id_type=MESH)
        loads = [
            pltpu.make_async_copy(src, dst, load_sems.at[index])
            for index, (src, dst) in enumerate(
                (
                    (pairs_hbm, pairs_ref),
                    (count_hbm, count_ref),
                    (coords_hbm, coords_ref),
                    (polar_hbm, polar_ref),
                    (field_hbm, field_ref),
                )
            )
        ]
        for copy in loads:
            copy.start()

    lane = lax.broadcasted_iota(jnp.int32, (8, 128), 1)
    row = lax.broadcasted_iota(jnp.int32, (8, 128), 0)
    group = lane // GROUP
    place_y = lane // SIDE % SIDE
    place_x = lane % SIDE
    site = lane % GROUP
    shift_x = group - REACH
    unpack = GROUP * row + site
    far_x = spacing * shift_x.astype(jnp.float32)

    def within(first, size):
        return jnp.logical_and(lane >= first, lane < first + size)

    def choose(cases, default):
        for condition, value in cases:
            default = jnp.where(condition, value, default)
        return default

    def edge_index(bases, at, first_x):
        cases = []
        for base, start in zip(bases, at):
            local = lane - base
            value = start + SIDE * (local // 3) + local % 3 + first_x
            cases.append((within(base, EDGE), value))
        return choose(cases, jnp.zeros_like(lane))

    all_parts = [GROUP * part for part in range(6)]
    take_low = edge_index(LOW[0] + LOW[1], all_parts, 1)
    take_high = edge_index(HIGH[0] + HIGH[1], all_parts, 0)
    ride_low = [
        edge_index([RIDE_LOW + EDGE * part for part in range(3)], all_parts[3 * s : 3 * s + 3], 1)
        for s in range(2)
    ]
    ride_high = [
        edge_index([RIDE_HIGH + EDGE * part for part in range(3)], all_parts[3 * s : 3 * s + 3], 0)
        for s in range(2)
    ]

    def unride(regions, start):
        cases = []
        for bases in regions:
            for part, base in enumerate(bases):
                cases.append((within(base, EDGE), lane - base + start + EDGE * part))
        return choose(cases, jnp.zeros_like(lane))

    leave_low = unride(LOW, RIDE_LOW)
    leave_high = unride(HIGH, RIDE_HIGH)

    def inside(bases, size):
        result = within(bases[0], size)
        for base in bases[1:]:
            result = jnp.logical_or(result, within(base, size))
        return result

    is_own = [within(OWN[s], 3 * GROUP) for s in range(2)]
    is_low = [inside(LOW[s], EDGE) for s in range(2)]

    reached = place_x + shift_x
    turn_x = []
    for part in range(6):
        s, c = part // 3, part % 3
        low = LOW[s][c] + 3 * place_y + reached + SIDE - 1
        high = HIGH[s][c] + 3 * place_y + jnp.minimum(reached - SIDE, 2)
        own = OWN[s] + GROUP * c + SIDE * place_y + reached
        turn_x.append(jnp.where(reached < 0, low, jnp.where(reached < SIDE, own, high)))

    def packed(parts):
        value = parts[0]
        for index in range(1, len(parts)):
            value = jnp.where(group == index, parts[index], value)
        return value

    def rows_of(line):
        return gather(jnp.broadcast_to(line, (8, 128)), unpack)

    MIDDLE = 0
    SENT = {0: 0, 1: deep + 1, -1: deep + 2 + tiles}
    HALO = {0: deep, 1: deep + 1 + tiles, -1: deep + 2 + 2 * tiles}

    def put(phase, blocks):
        last = deep - 1
        for k in range(deep):
            send[phase, MIDDLE + k] = blocks[k]
        send[phase, HALO[0]] = jnp.where(row < 4, blocks[0], blocks[last])
        for direction, take, ride, ride_at in (
            (1, take_low, ride_low, RIDE_LOW),
            (-1, take_high, ride_high, RIDE_HIGH),
        ):
            cut = {k: gather(blocks[k], take) for k in range(deep) if k not in riders or k == last}
            send[phase, HALO[direction]] = jnp.where(row < 4, cut[0], cut[last])
            for rider in riders:
                for s in range(2):
                    host = rider - 2 + s
                    cut[host] = jnp.where(
                        within(ride_at, 3 * EDGE), gather(blocks[rider], ride[s]), cut[host]
                    )
            for k in tile_of:
                send[phase, SENT[direction] + tile_of[k]] = cut[k]

    def exchange(phase):
        def start(src, dst, target):
            pltpu.make_async_remote_copy(
                src_ref=send.at[phase, src],
                dst_ref=held.at[phase, dst],
                send_sem=send_sems.at[phase],
                recv_sem=recv_sems.at[phase],
                device_id=target,
                device_id_type=MESH,
            ).start()

        for cx, cy in sorted(COLUMNS, key=lambda column: -abs(column[0]) - abs(column[1])):
            there = (-cx, -cy)
            if (cx, cy) != (0, 0):
                amount = tiles if cx else deep
                start(
                    pl.ds(SENT[cx], amount), pl.ds(slots[there], amount), neighbour(cx, cy, 0)
                )
            for ring in range(rings):
                start(
                    pl.ds(HALO[cx], 1),
                    pl.ds(halos[there] + ring, 1),
                    neighbour(cx, cy, -1 if ring == 0 else 1),
                )

    def wait_all(phase, sems):
        pltpu.make_async_copy(held.at[phase], held.at[phase], sems.at[phase]).wait()

    def merged_tiles(phase):
        result = {}
        for cy in (-1, 0, 1):
            def halo(cx):
                at = halos[cx, cy]
                if rings == 1:
                    return held[phase, at]
                return jnp.where(row < 4, held[phase, at], held[phase, at + 1])

            both = []
            for s in range(2):
                row_of_tiles = []
                for v in range(deep + 1):
                    k = v - 1
                    if v == 0:
                        low, own, high = halo(-1), halo(0), halo(1)
                    else:
                        own = send[phase, MIDDLE + k] if cy == 0 else held[phase, slots[0, cy] + k]
                        if k in riders:
                            host = tile_of[k - 2 + s]
                            low = gather(held[phase, slots[-1, cy] + host], leave_low)
                            high = gather(held[phase, slots[1, cy] + host], leave_high)
                        else:
                            low = held[phase, slots[-1, cy] + tile_of[k]]
                            high = held[phase, slots[1, cy] + tile_of[k]]
                    row_of_tiles.append(
                        jnp.where(is_own[s], own, jnp.where(is_low[s], low, high))
                    )
                both.append(row_of_tiles)
            result[cy] = both
        return result

    def by_shift_y(values, sy):
        if sy > 0:
            return jnp.where(place_y < sy, values[1], values[0])
        if sy < 0:
            return jnp.where(place_y >= SIDE + sy, values[-1], values[0])
        return values[0]

    def spread_out(tiles_in, out, parts):
        for v in range(deep + 1):
            for part in range(parts):
                lined = {
                    cy: gather(tiles_in[cy][part // 3][v], turn_x[part]) for cy in (-1, 0, 1)
                }
                for sy in SHIFTS:
                    value = by_shift_y(lined, sy)
                    out[sy + REACH, part, pl.ds(8 * v, 8), :] = value
                    if v == 0:
                        out[sy + REACH, part, pl.ds(8 * (deep + 1), 8), :] = value

    def contract(sums, parts, vec):
        xx, yy, zz, xy, xz, yz = parts
        for first in (0, 3):
            vx, vy, vz = vec[first : first + 3]
            sums[first] = sums[first] + (xx * vx + xy * vy + xz * vz)
            sums[first + 1] = sums[first + 1] + (xy * vx + yy * vy + yz * vz)
            sums[first + 2] = sums[first + 2] + (xz * vx + yz * vy + zz * vz)

    def tile_number(k, sy, sz):
        return (k * SPAN + sy + REACH) * SPAN + sz + REACH

    def build_tile(k, sy, sz):
        turn = sy % SIDE
        start = 8 + sz
        span = pl.ds(8 * k + start, 8)
        dx = near_geo[sy + REACH, 0, span, :] - own_ref[turn, k, 0]
        dy = near_geo[sy + REACH, 1, span, :] - (own_ref[turn, k, 1] - spacing * sy)
        dz = near_geo[sy + REACH, 2, span, :] - (own_ref[turn, k, 2] - spacing * sz)
        weight = switch[k, sy + REACH, pl.ds(start, 8), :]
        if sy == 0 and sz == 0:
            weight = jnp.where(group == REACH, 0.0, weight)
        square = jnp.maximum(dx * dx + dy * dy + dz * dz, 1.0)
        inverse = lax.rsqrt(square)
        inverse_square = inverse * inverse
        damp = square * square * inverse * (near_geo[sy + REACH, 3, span, :] * own_ref[turn, k, 3])
        damping = jnp.exp(-damp)
        fade = jnp.maximum(1.0 - square * (1.0 / cutoff_square), 0.0)
        scale = fade * fade * (inverse_square * inverse) * weight
        three = scale * (1.0 - damping)
        five = (1.0 - (1.0 + damp) * damping) * scale * (3.0 * inverse_square)
        tx, ty, tz = five * dx, five * dy, five * dz
        parts = (tx * dx - three, ty * dy - three, tz * dz - three, tx * dy, tx * dz, ty * dz)
        for part in range(6):
            tensor[tile_number(k, sy, sz), part] = parts[part]
        return parts

    def load_tile(k, sy, sz):
        return [tensor[tile_number(k, sy, sz), part] for part in range(6)]

    def fold(parts):
        width = GROUP
        while len(parts) > 1 or width < 128:
            upper = (lane // width) % 2 == 1
            merged = []
            for index in range(0, len(parts), 2):
                first = parts[index]
                second = parts[index + 1] if index + 1 < len(parts) else first
                kept = jnp.where(upper, second, first)
                moved = jnp.where(upper, first, second)
                merged.append(kept + pltpu.roll(moved, width, 1))
            parts = merged
            width *= 2
        return parts[0]

    def operate(make_tile, vector):
        image = []
        for k in range(deep):
            total = [None] * 6
            for turn in (1, 2, 3, 0):
                sums = [jnp.zeros((8, 128), jnp.float32)] * 6
                for sy in SHIFTS:
                    if sy % SIDE != turn:
                        continue
                    for sz in SHIFTS:
                        if abs(sy) == REACH and abs(sz) == REACH:
                            continue
                        span = pl.ds(8 * k + 8 + sz, 8)
                        vec = [near[sy + REACH, part, span, :] for part in range(6)]
                        contract(sums, make_tile(k, sy, sz), vec)
                for part in range(6):
                    value = sums[part]
                    if turn:
                        value = pltpu.roll(value, 128 - SIDE * turn, 1)
                    total[part] = value if total[part] is None else total[part] + value
            image.append(vector[k] / polar[k] - mask[k] * fold(total))
        return image

    def build_switch(tiles_in):
        def full(at):
            return jnp.full((8, 128), at, jnp.int32)

        def pick(first, second, third):
            return jnp.where(reached < 0, first, jnp.where(reached < SIDE, second, third))

        own_lane = OWN[1] + GROUP * (FLAGS - 3)
        for cz in (-1, 0, 1):
            active = [{} for _ in range(deep)]
            for cy in (-1, 0, 1):
                low, middle, high = (9 * (cx + 1) + 3 * (cy + 1) + cz + 1 for cx in (-1, 0, 1))
                low_at = full(LOW[1][FLAGS - 3] + 12 - low - 4)
                high_at = full(own_lane + flag_slot(high - 14))
                if middle < 13:
                    theirs = jnp.where(
                        reached < 0, low_at, full(own_lane + flag_slot(12 - middle))
                    )
                    ours = high_at
                else:
                    theirs = low_at
                    ours = jnp.where(
                        reached < SIDE, full(own_lane + flag_slot(max(middle - 14, 0))), high_at
                    )
                for k in range(deep):
                    v = (k + 1 + cz) % (deep + 1)
                    there = gather(tiles_in[cy][1][v], theirs)
                    here = gather(tiles_in[0][1][k + 1], ours)
                    value = pick(there, there if middle < 13 else here, here)
                    if middle == 13:
                        value = pick(value, 1.0, value)
                    active[k][cy] = jnp.where(group < SPAN, value, 0.0)
            for k in range(deep):
                for sy in SHIFTS:
                    switch[k, sy + REACH, pl.ds(8 * (cz + 1), 8), :] = by_shift_y(active[k], sy)

    in_set = [group < 3, jnp.logical_and(group >= 3, group < 6)]

    def start_sums(number, products):
        values = []
        for first, second in products:
            value = first[0] * second[0]
            for k in range(1, deep):
                value = value + first[k] * second[k]
            line = jnp.sum(value, axis=0, keepdims=True)
            for s in range(2):
                chosen = jnp.where(in_set[s][0:1], line, 0.0)
                values.append(jnp.sum(chosen, axis=1, keepdims=True))
        line = jnp.broadcast_to(values[0], (1, 128))
        for index in range(1, len(values)):
            line = jnp.where(group[0:1] == index, values[index], line)
        sums_out[number] = line
        sums_in[number, my_id] = line
        for step in range(1, total_devices):
            other = lax.rem(my_id + step, total_devices)
            pltpu.make_async_remote_copy(
                src_ref=sums_out.at[number],
                dst_ref=sums_in.at[number, my_id],
                send_sem=sum_send.at[number],
                recv_sem=sum_recv.at[number],
                device_id=device_at(other),
                device_id_type=MESH,
            ).start()

    def wait_sums(number, sems):
        rows = sums_in.at[number, pl.ds(0, total_devices - 1)]
        pltpu.make_async_copy(rows, rows, sems.at[number]).wait()

    def end_sums(number, amount):
        wait_sums(number, sum_recv)
        lines = [sums_in[number, index] for index in range(total_devices)]
        while len(lines) > 1:
            lines = [
                lines[index] + lines[index + 1] if index + 1 < len(lines) else lines[index]
                for index in range(0, len(lines), 2)
            ]
        line = jnp.broadcast_to(lines[0], (8, 128))
        return [
            gather(line, jnp.where(group < 3, GROUP * 2 * index, GROUP * (2 * index + 1)))
            for index in range(amount)
        ]

    def each(function, *vectors):
        return [function(k, *(vector[k] for vector in vectors)) for k in range(deep)]

    with scope("setup"):
        for copy in loads:
            copy.wait()
        site_x = spacing * (place_x.astype(jnp.float32) + 0.5)
        site_y = spacing * (place_y.astype(jnp.float32) + 0.5)
        site_z = spacing * (row.astype(jnp.float32) + 0.5)
        polar, mask, source, geometry = [], [], [], []
        for k in range(deep):
            places = [
                rows_of(coords_ref[3 * k + part]) - offset
                for part, offset in enumerate((site_x, site_y, site_z))
            ]
            polar_k = rows_of(polar_ref[k])
            mask_k = jnp.where(unpack < count_ref[k], 1.0, 0.0)
            root = lax.rsqrt(polar_k)
            slot = 14 + jnp.where(
                place_x == 0, place_y, 4 + 3 * place_y + place_x - 1
            )
            flag = pairs_ref[k, 0, 0] == slot
            for entry in range(1, 13):
                flag = jnp.logical_or(flag, pairs_ref[k, 0, entry] == slot)
            flags = jnp.where(flag, 1.0, 0.0)
            geometry.append(packed(places + [root, flags]))
            for turn in range(SIDE):
                for part, value in enumerate(places + [thole * root]):
                    if turn:
                        value = pltpu.roll(value, SIDE * turn, 1)
                    own_ref[turn, k, part] = value - far_x if part == 0 else value
            polar.append(polar_k)
            mask.append(mask_k)
            field_k = packed([rows_of(field_ref[6 * k + part]) for part in range(6)])
            source.append(field_k * mask_k)
        dipoles = each(lambda k, s: polar[k] * s, source)
        put(0, geometry)
        put(1, each(lambda k, d: d * mask[k], dipoles))
    with scope("barrier"):
        pl.semaphore_wait(barrier, total_devices - 1)
    with scope("send0"):
        exchange(0)
        exchange(1)
    with scope("geowait"):
        wait_all(0, recv_sems)
    with scope("geospread"):
        tiles_in = merged_tiles(0)
        spread_out(tiles_in, near_geo, 4)
        build_switch(tiles_in)
    with scope("wait0"):
        wait_all(1, recv_sems)
    with scope("build"):
        spread_out(merged_tiles(1), near, 6)
        image = operate(build_tile, dipoles)
    with scope("finish0"):
        residual = each(lambda k, s, a: s - a, source, image)
        precond = each(lambda k, r: polar[k] * r, residual)
        put(2, each(lambda k, p: p * mask[k], precond))
    with scope("send1"):
        exchange(2)
    with scope("wait1"):
        wait_all(2, recv_sems)
    with scope("apply1"):
        spread_out(merged_tiles(2), near, 6)
        image = operate(load_tile, precond)
    with scope("finish1"):
        turned = each(lambda k, q: polar[k] * q, image)
        put(3, each(lambda k, t: t * mask[k], turned))
    with scope("send2"):
        exchange(3)
    with scope("sum1"):
        start_sums(0, [(residual, precond), (precond, image)])
    with scope("wait2"):
        wait_all(3, recv_sems)
    with scope("apply2"):
        spread_out(merged_tiles(3), near, 6)
        turned_image = operate(load_tile, turned)
    with scope("sum1wait"):
        norm, curve = end_sums(0, 2)
    with scope("mid"):
        gamma = norm / curve
        dipoles = each(lambda k, d, p: d + gamma * p, dipoles, precond)
        residual = each(lambda k, r, q: r - gamma * q, residual, image)
        second = each(lambda k, r: polar[k] * r, residual)
        second_image = each(lambda k, q, t: q - gamma * t, image, turned_image)
        start_sums(
            1,
            [
                (residual, second), (second, second_image), (second, image),
                (precond, second_image),
            ],
        )
    with scope("sum2wait"):
        norm_next, second_curve, cross, cross_back = end_sums(1, 4)
    with scope("out"):
        ratio = norm_next / norm
        gamma = norm_next / (second_curve + ratio * (cross + cross_back + ratio * curve))
        for k in range(deep):
            direction = second[k] + ratio * precond[k]
            along = second_image[k] + ratio * image[k]
            for out, value in (
                (dip_out, dipoles[k] + gamma * direction),
                (res_out, residual[k] - gamma * along),
            ):
                for part in range(6):
                    turned_part = gather(value, GROUP * part + site)
                    line = jnp.where(group == row, turned_part, 0.0)
                    out[6 * k + part] = jnp.sum(line, axis=0, keepdims=True)
    with scope("sendwait"):
        for phase in range(4):
            wait_all(phase, send_sems)
        for number in range(2):
            wait_sums(number, sum_send)


def on_device(sizes, coords, polar, field, atom_count, pair_list):
    deep, slots = coords.shape[2], coords.shape[-1]
    assert coords.shape[0:2] == (1, 1) and slots == 128
    vmem = pl.BlockSpec(memory_space=pltpu.VMEM)
    hbm = pl.BlockSpec(memory_space=pl.ANY)
    rows = 8 * deep
    devices = sizes[0] * sizes[1] * sizes[2]
    tiles, total_tiles = (plan(deep, 1 if sizes[2] == 2 else 2)[index] for index in (2, 5))

    def buffer(*shape):
        return pltpu.VMEM(shape, jnp.float32)

    line = jax.ShapeDtypeStruct((6 * deep, 1, slots), jnp.float32)
    dma = pltpu.SemaphoreType.DMA
    dipoles, residual = pl.pallas_call(
        functools.partial(kernel, sizes, deep),
        out_shape=(line, line),
        in_specs=[hbm] * 5,
        out_specs=(vmem, vmem),
        scratch_shapes=[
            pltpu.SMEM((deep, 1, pair_list.shape[-1]), jnp.int32),
            pltpu.SMEM((deep,), jnp.int32),
            buffer(3 * deep, 1, slots),
            buffer(deep, 1, slots),
            buffer(6 * deep, 1, slots),
            buffer(4, deep + 2 * tiles + 3, 8, slots),
            buffer(4, total_tiles, 8, slots),
            buffer(SPAN, 6, rows + 16, slots),
            buffer(SPAN, 4, rows + 16, slots),
            buffer(SIDE, deep, 4, 8, slots),
            buffer(deep, SPAN, 24, slots),
            buffer(SPAN * SPAN * deep, 6, 8, slots),
            buffer(2, 1, slots),
            buffer(2, devices, 1, slots),
            dma((5,)),
            dma((4,)),
            dma((4,)),
            dma((2,)),
            dma((2,)),
        ],
        compiler_params=pltpu.CompilerParams(collective_id=0, has_side_effects=True),
    )(
        pair_list.reshape(deep, 1, -1),
        atom_count.reshape(deep),
        coords.reshape(3 * deep, 1, slots),
        polar.reshape(deep, 1, slots),
        field.reshape(6 * deep, 1, slots),
    )
    return dipoles.reshape(field.shape), residual.reshape(field.shape)


def solution(mesh):
    sizes = tuple(mesh.shape[name] for name in AXES)
    block = P(*AXES, None, None)
    return jax.shard_map(
        functools.partial(on_device, sizes),
        mesh=mesh,
        in_specs=(block, P(*AXES, None), block, P(*AXES), P(*AXES, None)),
        out_specs=(block, block),
        check_vma=False,
    )
```

```python
import functools

import jax
import jax.numpy as jnp
from jax import lax
from jax.experimental import pallas as pl
from jax.experimental.pallas import tpu as pltpu
from jax.sharding import PartitionSpec as P

MESH = pl.DeviceIdType.MESH
AXES = ("gx", "gy", "gz")
spacing = 2.2
cutoff_square = 49.0
thole = 0.39
SIDE = 4
GROUP = SIDE * SIDE
REACH = 3
SHIFTS = range(-REACH, REACH + 1)
SPAN = 2 * REACH + 1
COLUMNS = [(cx, cy) for cx in (-1, 0, 1) for cy in (-1, 0, 1)]
EDGE = 12
OWN = (0, 48)
LOW = ((48, 60, 72), (36, 96, 108))
HIGH = ((84, 96, 108), (0, 12, 24))
RIDE_LOW = 0
RIDE_HIGH = 36
FLAGS = 4


def gather(value, index):
    return jnp.take_along_axis(value, index, axis=1, mode="promise_in_bounds")


def flag_slot(flag):
    return 4 * flag if flag < 4 else 4 * ((flag - 4) // 3) + 1 + (flag - 4) % 3


def plan(deep, rings):
    riders = [k for k in range(deep) if k % 3 == 2]
    tile_of, tiles = {}, 0
    for k in range(deep):
        if k not in riders:
            tile_of[k] = tiles
            tiles += 1
    slots, total = {}, 0
    for column in COLUMNS:
        if column != (0, 0):
            slots[column] = total
            total += tiles if column[0] else deep
    halos = {}
    for column in COLUMNS:
        halos[column] = total
        total += rings
    return riders, tile_of, tiles, slots, halos, total


def kernel(
    sizes, deep, pairs_hbm, count_hbm, coords_hbm, polar_hbm, field_hbm, dip_out, res_out,
    pairs_ref, count_ref, coords_ref, polar_ref, field_ref, send, held, near, near_geo, own_ref,
    switch, tensor, sums_out, sums_in, load_sems, send_sems, recv_sems, sum_send, sum_recv,
):
    total_devices = sizes[0] * sizes[1] * sizes[2]
    rings = 1 if sizes[2] == 2 else 2
    riders, tile_of, tiles, slots, halos, total_tiles = plan(deep, rings)
    me = [lax.axis_index(name) for name in AXES]
    my_id = (me[0] * sizes[1] + me[1]) * sizes[2] + me[2]
    scope = jax.named_scope

    def device_at(linear):
        return (
            linear // (sizes[1] * sizes[2]),
            linear // sizes[2] % sizes[1],
            linear % sizes[2],
        )

    def neighbour(cx, cy, cz):
        return tuple(
            lax.rem(place + step + size, size)
            for place, step, size in zip(me, (cx, cy, cz), sizes)
        )

    with scope("signal"):
        barrier = pltpu.get_barrier_semaphore()
        if max(sizes) <= 5:
            steps = [(1, -1, 0) if size > 2 else (1, 0) for size in sizes]
            greeted = [
                neighbour(cx, cy, cz)
                for cx in steps[0] for cy in steps[1] for cz in steps[2]
                if (cx, cy, cz) != (0, 0, 0)
            ]
        else:
            greeted = [
                device_at(lax.rem(my_id + step, total_devices)) for step in range(1, total_devices)
            ]
        for target in greeted:
            pl.semaphore_signal(barrier, inc=1, device_id=target, device_id_type=MESH)
        loads = [
            pltpu.make_async_copy(src, dst, load_sems.at[index])
            for index, (src, dst) in enumerate(
                (
                    (pairs_hbm, pairs_ref),
                    (count_hbm, count_ref),
                    (coords_hbm, coords_ref),
                    (polar_hbm, polar_ref),
                    (field_hbm, field_ref),
                )
            )
        ]
        for copy in loads:
            copy.start()

    lane = lax.broadcasted_iota(jnp.int32, (8, 128), 1)
    row = lax.broadcasted_iota(jnp.int32, (8, 128), 0)
    group = lane // GROUP
    place_y = lane // SIDE % SIDE
    place_x = lane % SIDE
    site = lane % GROUP
    shift_x = group - REACH
    unpack = GROUP * row + site
    far_x = spacing * shift_x.astype(jnp.float32)

    def within(first, size):
        return jnp.logical_and(lane >= first, lane < first + size)

    def choose(cases, default):
        for condition, value in cases:
            default = jnp.where(condition, value, default)
        return default

    def edge_index(bases, at, first_x):
        cases = []
        for base, start in zip(bases, at):
            local = lane - base
            value = start + SIDE * (local // 3) + local % 3 + first_x
            cases.append((within(base, EDGE), value))
        return choose(cases, jnp.zeros_like(lane))

    all_parts = [GROUP * part for part in range(6)]
    take_low = edge_index(LOW[0] + LOW[1], all_parts, 1)
    take_high = edge_index(HIGH[0] + HIGH[1], all_parts, 0)
    ride_low = [
        edge_index([RIDE_LOW + EDGE * part for part in range(3)], all_parts[3 * s : 3 * s + 3], 1)
        for s in range(2)
    ]
    ride_high = [
        edge_index([RIDE_HIGH + EDGE * part for part in range(3)], all_parts[3 * s : 3 * s + 3], 0)
        for s in range(2)
    ]

    def unride(regions, start):
        cases = []
        for bases in regions:
            for part, base in enumerate(bases):
                cases.append((within(base, EDGE), lane - base + start + EDGE * part))
        return choose(cases, jnp.zeros_like(lane))

    leave_low = unride(LOW, RIDE_LOW)
    leave_high = unride(HIGH, RIDE_HIGH)

    def inside(bases, size):
        result = within(bases[0], size)
        for base in bases[1:]:
            result = jnp.logical_or(result, within(base, size))
        return result

    is_own = [within(OWN[s], 3 * GROUP) for s in range(2)]
    is_low = [inside(LOW[s], EDGE) for s in range(2)]

    reached = place_x + shift_x
    turn_x = []
    for part in range(6):
        s, c = part // 3, part % 3
        low = LOW[s][c] + 3 * place_y + reached + SIDE - 1
        high = HIGH[s][c] + 3 * place_y + jnp.minimum(reached - SIDE, 2)
        own = OWN[s] + GROUP * c + SIDE * place_y + reached
        turn_x.append(jnp.where(reached < 0, low, jnp.where(reached < SIDE, own, high)))

    def packed(parts):
        value = parts[0]
        for index in range(1, len(parts)):
            value = jnp.where(group == index, parts[index], value)
        return value

    def rows_of(line):
        return gather(jnp.broadcast_to(line, (8, 128)), unpack)

    MIDDLE = 0
    SENT = {0: 0, 1: deep + 1, -1: deep + 2 + tiles}
    HALO = {0: deep, 1: deep + 1 + tiles, -1: deep + 2 + 2 * tiles}

    def put(phase, blocks):
        last = deep - 1
        for k in range(deep):
            send[phase, MIDDLE + k] = blocks[k]
        send[phase, HALO[0]] = jnp.where(row < 4, blocks[0], blocks[last])
        for direction, take, ride, ride_at in (
            (1, take_low, ride_low, RIDE_LOW),
            (-1, take_high, ride_high, RIDE_HIGH),
        ):
            cut = {k: gather(blocks[k], take) for k in range(deep) if k not in riders or k == last}
            send[phase, HALO[direction]] = jnp.where(row < 4, cut[0], cut[last])
            for rider in riders:
                for s in range(2):
                    host = rider - 2 + s
                    cut[host] = jnp.where(
                        within(ride_at, 3 * EDGE), gather(blocks[rider], ride[s]), cut[host]
                    )
            for k in tile_of:
                send[phase, SENT[direction] + tile_of[k]] = cut[k]

    def exchange(phase):
        def start(src, dst, target):
            pltpu.make_async_remote_copy(
                src_ref=send.at[phase, src],
                dst_ref=held.at[phase, dst],
                send_sem=send_sems.at[phase],
                recv_sem=recv_sems.at[phase],
                device_id=target,
                device_id_type=MESH,
            ).start()

        for cx, cy in sorted(COLUMNS, key=lambda column: -abs(column[0]) - abs(column[1])):
            there = (-cx, -cy)
            if (cx, cy) != (0, 0):
                amount = tiles if cx else deep
                start(
                    pl.ds(SENT[cx], amount), pl.ds(slots[there], amount), neighbour(cx, cy, 0)
                )
            for ring in range(rings):
                start(
                    pl.ds(HALO[cx], 1),
                    pl.ds(halos[there] + ring, 1),
                    neighbour(cx, cy, -1 if ring == 0 else 1),
                )

    def wait_all(phase, sems):
        pltpu.make_async_copy(held.at[phase], held.at[phase], sems.at[phase]).wait()

    def merged_tiles(phase):
        result = {}
        for cy in (-1, 0, 1):
            def halo(cx):
                at = halos[cx, cy]
                if rings == 1:
                    return held[phase, at]
                return jnp.where(row < 4, held[phase, at], held[phase, at + 1])

            both = []
            for s in range(2):
                row_of_tiles = []
                for v in range(deep + 1):
                    k = v - 1
                    if v == 0:
                        low, own, high = halo(-1), halo(0), halo(1)
                    else:
                        own = send[phase, MIDDLE + k] if cy == 0 else held[phase, slots[0, cy] + k]
                        if k in riders:
                            host = tile_of[k - 2 + s]
                            low = gather(held[phase, slots[-1, cy] + host], leave_low)
                            high = gather(held[phase, slots[1, cy] + host], leave_high)
                        else:
                            low = held[phase, slots[-1, cy] + tile_of[k]]
                            high = held[phase, slots[1, cy] + tile_of[k]]
                    row_of_tiles.append(
                        jnp.where(is_own[s], own, jnp.where(is_low[s], low, high))
                    )
                both.append(row_of_tiles)
            result[cy] = both
        return result

    def by_shift_y(values, sy):
        if sy > 0:
            return jnp.where(place_y < sy, values[1], values[0])
        if sy < 0:
            return jnp.where(place_y >= SIDE + sy, values[-1], values[0])
        return values[0]

    def spread_out(tiles_in, out, parts):
        for v in range(deep + 1):
            for part in range(parts):
                lined = {
                    cy: gather(tiles_in[cy][part // 3][v], turn_x[part]) for cy in (-1, 0, 1)
                }
                for sy in SHIFTS:
                    value = by_shift_y(lined, sy)
                    out[sy + REACH, part, pl.ds(8 * v, 8), :] = value
                    if v == 0:
                        out[sy + REACH, part, pl.ds(8 * (deep + 1), 8), :] = value

    def contract(sums, parts, vec):
        xx, yy, zz, xy, xz, yz = parts
        for first in (0, 3):
            vx, vy, vz = vec[first : first + 3]
            sums[first] = sums[first] + (xx * vx + xy * vy + xz * vz)
            sums[first + 1] = sums[first + 1] + (xy * vx + yy * vy + yz * vz)
            sums[first + 2] = sums[first + 2] + (xz * vx + yz * vy + zz * vz)

    def tile_number(k, sy, sz):
        return (k * SPAN + sy + REACH) * SPAN + sz + REACH

    def build_tile(k, sy, sz):
        turn = sy % SIDE
        start = 8 + sz
        span = pl.ds(8 * k + start, 8)
        dx = near_geo[sy + REACH, 0, span, :] - own_ref[turn, k, 0]
        dy = near_geo[sy + REACH, 1, span, :] - (own_ref[turn, k, 1] - spacing * sy)
        dz = near_geo[sy + REACH, 2, span, :] - (own_ref[turn, k, 2] - spacing * sz)
        weight = switch[k, sy + REACH, pl.ds(start, 8), :]
        if sy == 0 and sz == 0:
            weight = jnp.where(group == REACH, 0.0, weight)
        square = jnp.maximum(dx * dx + dy * dy + dz * dz, 1.0)
        inverse = lax.rsqrt(square)
        inverse_square = inverse * inverse
        damp = square * square * inverse * (near_geo[sy + REACH, 3, span, :] * own_ref[turn, k, 3])
        damping = jnp.exp(-damp)
        fade = jnp.maximum(1.0 - square * (1.0 / cutoff_square), 0.0)
        scale = fade * fade * (inverse_square * inverse) * weight
        three = scale * (1.0 - damping)
        five = (1.0 - (1.0 + damp) * damping) * scale * (3.0 * inverse_square)
        tx, ty, tz = five * dx, five * dy, five * dz
        parts = (tx * dx - three, ty * dy - three, tz * dz - three, tx * dy, tx * dz, ty * dz)
        for part in range(6):
            tensor[tile_number(k, sy, sz), part] = parts[part]
        return parts

    def load_tile(k, sy, sz):
        return [tensor[tile_number(k, sy, sz), part] for part in range(6)]

    def fold(parts):
        width = GROUP
        while len(parts) > 1 or width < 128:
            upper = (lane // width) % 2 == 1
            merged = []
            for index in range(0, len(parts), 2):
                first = parts[index]
                second = parts[index + 1] if index + 1 < len(parts) else first
                kept = jnp.where(upper, second, first)
                moved = jnp.where(upper, first, second)
                merged.append(kept + pltpu.roll(moved, width, 1))
            parts = merged
            width *= 2
        return parts[0]

    def operate(make_tile, vector):
        image = []
        for k in range(deep):
            total = [None] * 6
            for turn in (1, 2, 3, 0):
                sums = [jnp.zeros((8, 128), jnp.float32)] * 6
                for sy in SHIFTS:
                    if sy % SIDE != turn:
                        continue
                    for sz in SHIFTS:
                        if abs(sy) == REACH and abs(sz) == REACH:
                            continue
                        span = pl.ds(8 * k + 8 + sz, 8)
                        vec = [near[sy + REACH, part, span, :] for part in range(6)]
                        contract(sums, make_tile(k, sy, sz), vec)
                for part in range(6):
                    value = sums[part]
                    if turn:
                        value = pltpu.roll(value, 128 - SIDE * turn, 1)
                    total[part] = value if total[part] is None else total[part] + value
            image.append(vector[k] / polar[k] - mask[k] * fold(total))
        return image

    def build_switch(tiles_in):
        def full(at):
            return jnp.full((8, 128), at, jnp.int32)

        def pick(first, second, third):
            return jnp.where(reached < 0, first, jnp.where(reached < SIDE, second, third))

        own_lane = OWN[1] + GROUP * (FLAGS - 3)
        for cz in (-1, 0, 1):
            active = [{} for _ in range(deep)]
            for cy in (-1, 0, 1):
                low, middle, high = (9 * (cx + 1) + 3 * (cy + 1) + cz + 1 for cx in (-1, 0, 1))
                low_at = full(LOW[1][FLAGS - 3] + 12 - low - 4)
                high_at = full(own_lane + flag_slot(high - 14))
                if middle < 13:
                    theirs = jnp.where(
                        reached < 0, low_at, full(own_lane + flag_slot(12 - middle))
                    )
                    ours = high_at
                else:
                    theirs = low_at
                    ours = jnp.where(
                        reached < SIDE, full(own_lane + flag_slot(max(middle - 14, 0))), high_at
                    )
                for k in range(deep):
                    v = (k + 1 + cz) % (deep + 1)
                    there = gather(tiles_in[cy][1][v], theirs)
                    here = gather(tiles_in[0][1][k + 1], ours)
                    value = pick(there, there if middle < 13 else here, here)
                    if middle == 13:
                        value = pick(value, 1.0, value)
                    active[k][cy] = jnp.where(group < SPAN, value, 0.0)
            for k in range(deep):
                for sy in SHIFTS:
                    switch[k, sy + REACH, pl.ds(8 * (cz + 1), 8), :] = by_shift_y(active[k], sy)

    in_set = [group < 3, jnp.logical_and(group >= 3, group < 6)]

    def start_sums(number, products):
        values = []
        for first, second in products:
            value = first[0] * second[0]
            for k in range(1, deep):
                value = value + first[k] * second[k]
            line = jnp.sum(value, axis=0, keepdims=True)
            for s in range(2):
                chosen = jnp.where(in_set[s][0:1], line, 0.0)
                values.append(jnp.sum(chosen, axis=1, keepdims=True))
        line = jnp.broadcast_to(values[0], (1, 128))
        for index in range(1, len(values)):
            line = jnp.where(group[0:1] == index, values[index], line)
        sums_out[number] = line
        sums_in[number, my_id] = line
        for step in range(1, total_devices):
            other = lax.rem(my_id + step, total_devices)
            pltpu.make_async_remote_copy(
                src_ref=sums_out.at[number],
                dst_ref=sums_in.at[number, my_id],
                send_sem=sum_send.at[number],
                recv_sem=sum_recv.at[number],
                device_id=device_at(other),
                device_id_type=MESH,
            ).start()

    def wait_sums(number, sems):
        rows = sums_in.at[number, pl.ds(0, total_devices - 1)]
        pltpu.make_async_copy(rows, rows, sems.at[number]).wait()

    def end_sums(number, amount):
        wait_sums(number, sum_recv)
        lines = [sums_in[number, index] for index in range(total_devices)]
        while len(lines) > 1:
            lines = [
                lines[index] + lines[index + 1] if index + 1 < len(lines) else lines[index]
                for index in range(0, len(lines), 2)
            ]
        line = jnp.broadcast_to(lines[0], (8, 128))
        return [
            gather(line, jnp.where(group < 3, GROUP * 2 * index, GROUP * (2 * index + 1)))
            for index in range(amount)
        ]

    def each(function, *vectors):
        return [function(k, *(vector[k] for vector in vectors)) for k in range(deep)]

    with scope("setup"):
        for copy in loads:
            copy.wait()
        site_x = spacing * (place_x.astype(jnp.float32) + 0.5)
        site_y = spacing * (place_y.astype(jnp.float32) + 0.5)
        site_z = spacing * (row.astype(jnp.float32) + 0.5)
        polar, mask, source, geometry = [], [], [], []
        for k in range(deep):
            places = [
                rows_of(coords_ref[3 * k + part]) - offset
                for part, offset in enumerate((site_x, site_y, site_z))
            ]
            polar_k = rows_of(polar_ref[k])
            mask_k = jnp.where(unpack < count_ref[k], 1.0, 0.0)
            root = lax.rsqrt(polar_k)
            slot = 14 + jnp.where(
                place_x == 0, place_y, 4 + 3 * place_y + place_x - 1
            )
            flag = pairs_ref[k, 0, 0] == slot
            for entry in range(1, 13):
                flag = jnp.logical_or(flag, pairs_ref[k, 0, entry] == slot)
            flags = jnp.where(flag, 1.0, 0.0)
            geometry.append(packed(places + [root, flags]))
            for turn in range(SIDE):
                for part, value in enumerate(places + [thole * root]):
                    if turn:
                        value = pltpu.roll(value, SIDE * turn, 1)
                    own_ref[turn, k, part] = value - far_x if part == 0 else value
            polar.append(polar_k)
            mask.append(mask_k)
            field_k = packed([rows_of(field_ref[6 * k + part]) for part in range(6)])
            source.append(field_k * mask_k)
        dipoles = each(lambda k, s: polar[k] * s, source)
        put(0, geometry)
        put(1, each(lambda k, d: d * mask[k], dipoles))
    with scope("barrier"):
        pl.semaphore_wait(barrier, len(greeted))
    with scope("send0"):
        exchange(0)
        exchange(1)
    with scope("geowait"):
        wait_all(0, recv_sems)
    with scope("geospread"):
        tiles_in = merged_tiles(0)
        spread_out(tiles_in, near_geo, 4)
        build_switch(tiles_in)
    with scope("wait0"):
        wait_all(1, recv_sems)
    with scope("build"):
        spread_out(merged_tiles(1), near, 6)
        image = operate(build_tile, dipoles)
    with scope("finish0"):
        residual = each(lambda k, s, a: s - a, source, image)
        precond = each(lambda k, r: polar[k] * r, residual)
        put(2, each(lambda k, p: p * mask[k], precond))
    with scope("send1"):
        exchange(2)
    with scope("wait1"):
        wait_all(2, recv_sems)
    with scope("apply1"):
        spread_out(merged_tiles(2), near, 6)
        image = operate(load_tile, precond)
    with scope("finish1"):
        turned = each(lambda k, q: polar[k] * q, image)
        put(3, each(lambda k, t: t * mask[k], turned))
    with scope("send2"):
        exchange(3)
    with scope("sum1"):
        start_sums(0, [(residual, precond), (precond, image)])
    with scope("wait2"):
        wait_all(3, recv_sems)
    with scope("apply2"):
        spread_out(merged_tiles(3), near, 6)
        turned_image = operate(load_tile, turned)
    with scope("sum1wait"):
        norm, curve = end_sums(0, 2)
    with scope("mid"):
        gamma = norm / curve
        dipoles = each(lambda k, d, p: d + gamma * p, dipoles, precond)
        residual = each(lambda k, r, q: r - gamma * q, residual, image)
        second = each(lambda k, r: polar[k] * r, residual)
        second_image = each(lambda k, q, t: q - gamma * t, image, turned_image)
        start_sums(
            1,
            [
                (residual, second), (second, second_image), (second, image),
                (precond, second_image),
            ],
        )
    with scope("sum2wait"):
        norm_next, second_curve, cross, cross_back = end_sums(1, 4)
    with scope("out"):
        ratio = norm_next / norm
        gamma = norm_next / (second_curve + ratio * (cross + cross_back + ratio * curve))
        for k in range(deep):
            direction = second[k] + ratio * precond[k]
            along = second_image[k] + ratio * image[k]
            for out, value in (
                (dip_out, dipoles[k] + gamma * direction),
                (res_out, residual[k] - gamma * along),
            ):
                for part in range(6):
                    turned_part = gather(value, GROUP * part + site)
                    line = jnp.where(group == row, turned_part, 0.0)
                    out[6 * k + part] = jnp.sum(line, axis=0, keepdims=True)
    with scope("sendwait"):
        for phase in range(4):
            wait_all(phase, send_sems)
        for number in range(2):
            wait_sums(number, sum_send)


def store(dipoles, residual, dip_out, res_out, sems):
    copies = [
        pltpu.make_async_copy(dipoles, dip_out, sems.at[0]),
        pltpu.make_async_copy(residual, res_out, sems.at[1]),
    ]
    for copy in copies:
        copy.start()
    for copy in copies:
        copy.wait()


def on_device(sizes, coords, polar, field, atom_count, pair_list):
    deep, slots = coords.shape[2], coords.shape[-1]
    assert coords.shape[0:2] == (1, 1) and slots == 128
    vmem = pl.BlockSpec(memory_space=pltpu.VMEM)
    hbm = pl.BlockSpec(memory_space=pl.ANY)
    rows = 8 * deep
    devices = sizes[0] * sizes[1] * sizes[2]
    tiles, total_tiles = (plan(deep, 1 if sizes[2] == 2 else 2)[index] for index in (2, 5))

    def buffer(*shape):
        return pltpu.VMEM(shape, jnp.float32)

    line = pltpu.VMEM((6 * deep, 1, slots), jnp.float32)
    result = jax.ShapeDtypeStruct((6 * deep, 1, slots), jnp.float32)
    dma = pltpu.SemaphoreType.DMA
    dipoles, residual = pl.pallas_call(
        functools.partial(kernel, sizes, deep),
        out_shape=(line, line),
        in_specs=[hbm] * 5,
        out_specs=(vmem, vmem),
        scratch_shapes=[
            pltpu.SMEM((deep, 1, pair_list.shape[-1]), jnp.int32),
            pltpu.SMEM((deep,), jnp.int32),
            buffer(3 * deep, 1, slots),
            buffer(deep, 1, slots),
            buffer(6 * deep, 1, slots),
            buffer(4, deep + 2 * tiles + 3, 8, slots),
            buffer(4, total_tiles, 8, slots),
            buffer(SPAN, 6, rows + 16, slots),
            buffer(SPAN, 4, rows + 16, slots),
            buffer(SIDE, deep, 4, 8, slots),
            buffer(deep, SPAN, 24, slots),
            buffer(SPAN * SPAN * deep, 6, 8, slots),
            buffer(2, 1, slots),
            buffer(2, devices, 1, slots),
            dma((5,)),
            dma((4,)),
            dma((4,)),
            dma((2,)),
            dma((2,)),
        ],
        compiler_params=pltpu.CompilerParams(collective_id=0, has_side_effects=True),
    )(
        pair_list.reshape(deep, 1, -1),
        atom_count.reshape(deep),
        coords.reshape(3 * deep, 1, slots),
        polar.reshape(deep, 1, slots),
        field.reshape(6 * deep, 1, slots),
    )
    dipoles, residual = pl.pallas_call(
        store,
        out_shape=(result, result),
        in_specs=[vmem, vmem],
        out_specs=(hbm, hbm),
        scratch_shapes=[dma((2,))],
    )(
        pltpu.with_memory_space_constraint(dipoles, pltpu.VMEM),
        pltpu.with_memory_space_constraint(residual, pltpu.VMEM),
    )
    return dipoles.reshape(field.shape), residual.reshape(field.shape)


def solution(mesh):
    sizes = tuple(mesh.shape[name] for name in AXES)
    block = P(*AXES, None, None)
    return jax.shard_map(
        functools.partial(on_device, sizes),
        mesh=mesh,
        in_specs=(block, P(*AXES, None), block, P(*AXES), P(*AXES, None)),
        out_specs=(block, block),
        check_vma=False,
    )
```

```python
import functools

import jax
import jax.numpy as jnp
from jax import lax
from jax.experimental import pallas as pl
from jax.experimental.pallas import tpu as pltpu
from jax.sharding import PartitionSpec as P

MESH = pl.DeviceIdType.MESH
AXES = ("gx", "gy", "gz")
spacing = 2.2
cutoff_square = 49.0
thole = 0.39
SIDE = 4
GROUP = SIDE * SIDE
REACH = 3
SHIFTS = range(-REACH, REACH + 1)
PAGES = 1 + 2 * REACH
SPAN = 2 * REACH + 1
COLUMNS = [(cx, cy) for cx in (-1, 0, 1) for cy in (-1, 0, 1)]
EDGE = 12
OWN = (0, 48)
LOW = ((48, 60, 72), (36, 96, 108))
HIGH = ((84, 96, 108), (0, 12, 24))
RIDE_LOW = 0
RIDE_HIGH = 36
FLAGS = 4


def gather(value, index):
    return jnp.take_along_axis(value, index, axis=1, mode="promise_in_bounds")


def plan(deep, rings):
    riders = [k for k in range(deep) if k % 3 == 2]
    tile_of, tiles = {}, 0
    for k in range(deep):
        if k not in riders:
            tile_of[k] = tiles
            tiles += 1
    inner, halos, counts = {}, {}, {}
    for cy in (0, 1):
        total = 0
        for cx in (-1, 0, 1):
            if (cx, cy) != (0, 0):
                inner[cx, cy] = total
                total += tiles if cx else deep
        for cx in (-1, 0, 1):
            halos[cx, cy] = total
            total += rings
        counts[cy] = total
    return riders, tile_of, tiles, inner, halos, counts


def kernel(
    sizes, deep, pairs_hbm, count_hbm, coords_hbm, polar_hbm, field_hbm, dip_out, res_out,
    pairs_ref, count_ref, coords_ref, polar_ref, field_ref, send, held, near, near_geo, own_ref,
    switch, tensor, sums_out, sums_in, load_sems, send_sems, recv_sems, sum_send, sum_recv,
):
    total_devices = sizes[0] * sizes[1] * sizes[2]
    rings = 1 if sizes[2] == 2 else 2
    riders, tile_of, tiles, inner, halos, counts = plan(deep, rings)
    me = [lax.axis_index(name) for name in AXES]
    my_id = (me[0] * sizes[1] + me[1]) * sizes[2] + me[2]
    scope = jax.named_scope
    up = jnp.where(2 * me[1] < sizes[1], 1, 0)
    side_is_up = (None, up, 1 - up)
    side_sign = (None, 2 * up - 1, 1 - 2 * up)

    def device_at(linear):
        return (
            linear // (sizes[1] * sizes[2]),
            linear // sizes[2] % sizes[1],
            linear % sizes[2],
        )

    def neighbour(cx, cy, cz):
        return tuple(
            lax.rem(place + step + size, size)
            for place, step, size in zip(me, (cx, cy, cz), sizes)
        )

    with scope("signal"):
        barrier = pltpu.get_barrier_semaphore()
        if max(sizes) <= 5:
            steps = [(1, -1, 0) if size > 2 else (1, 0) for size in sizes]
            greeted = [
                neighbour(cx, cy, cz)
                for cx in steps[0] for cy in steps[1] for cz in steps[2]
                if (cx, cy, cz) != (0, 0, 0)
            ]
        else:
            greeted = [
                device_at(lax.rem(my_id + step, total_devices)) for step in range(1, total_devices)
            ]
        for target in greeted:
            pl.semaphore_signal(barrier, inc=1, device_id=target, device_id_type=MESH)
        loads = [
            pltpu.make_async_copy(src, dst, load_sems.at[index])
            for index, (src, dst) in enumerate(
                (
                    (pairs_hbm, pairs_ref),
                    (count_hbm, count_ref),
                    (coords_hbm, coords_ref),
                    (polar_hbm, polar_ref),
                    (field_hbm, field_ref),
                )
            )
        ]
        for copy in loads:
            copy.start()

    lane = lax.broadcasted_iota(jnp.int32, (8, 128), 1)
    row = lax.broadcasted_iota(jnp.int32, (8, 128), 0)
    group = lane // GROUP
    place_y = lane // SIDE % SIDE
    place_x = lane % SIDE
    site = lane % GROUP
    shift_x = group - REACH
    unpack = GROUP * row + site
    far_x = spacing * shift_x.astype(jnp.float32)

    def within(first, size):
        return jnp.logical_and(lane >= first, lane < first + size)

    def choose(cases, default):
        for condition, value in cases:
            default = jnp.where(condition, value, default)
        return default

    def edge_index(bases, at, first_x):
        cases = []
        for base, start in zip(bases, at):
            local = lane - base
            value = start + SIDE * (local // 3) + local % 3 + first_x
            cases.append((within(base, EDGE), value))
        return choose(cases, jnp.zeros_like(lane))

    all_parts = [GROUP * part for part in range(6)]
    take_low = edge_index(LOW[0] + LOW[1], all_parts, 1)
    take_high = edge_index(HIGH[0] + HIGH[1], all_parts, 0)
    ride_low = [
        edge_index([RIDE_LOW + EDGE * part for part in range(3)], all_parts[3 * s : 3 * s + 3], 1)
        for s in range(2)
    ]
    ride_high = [
        edge_index([RIDE_HIGH + EDGE * part for part in range(3)], all_parts[3 * s : 3 * s + 3], 0)
        for s in range(2)
    ]

    def unride(regions, start):
        cases = []
        for bases in regions:
            for part, base in enumerate(bases):
                cases.append((within(base, EDGE), lane - base + start + EDGE * part))
        return choose(cases, jnp.zeros_like(lane))

    leave_low = unride(LOW, RIDE_LOW)
    leave_high = unride(HIGH, RIDE_HIGH)

    def inside(bases, size):
        result = within(bases[0], size)
        for base in bases[1:]:
            result = jnp.logical_or(result, within(base, size))
        return result

    is_own = [within(OWN[s], 3 * GROUP) for s in range(2)]
    is_low = [inside(LOW[s], EDGE) for s in range(2)]

    reached = place_x + shift_x
    turn_x = []
    for part in range(6):
        s, c = part // 3, part % 3
        low = LOW[s][c] + 3 * place_y + reached + SIDE - 1
        high = HIGH[s][c] + 3 * place_y + jnp.minimum(reached - SIDE, 2)
        own = OWN[s] + GROUP * c + SIDE * place_y + reached
        turn_x.append(jnp.where(reached < 0, low, jnp.where(reached < SIDE, own, high)))

    def packed(parts):
        value = parts[0]
        for index in range(1, len(parts)):
            value = jnp.where(group == index, parts[index], value)
        return value

    def rows_of(line):
        return gather(jnp.broadcast_to(line, (8, 128)), unpack)

    MIDDLE = 0
    SENT = {0: 0, 1: deep + 1, -1: deep + 2 + tiles}
    HALO = {0: deep, 1: deep + 1 + tiles, -1: deep + 2 + 2 * tiles}

    def put(phase, blocks):
        last = deep - 1
        for k in range(deep):
            send[phase, MIDDLE + k] = blocks[k]
        send[phase, HALO[0]] = jnp.where(row < 4, blocks[0], blocks[last])
        for direction, take, ride, ride_at in (
            (1, take_low, ride_low, RIDE_LOW),
            (-1, take_high, ride_high, RIDE_HIGH),
        ):
            cut = {k: gather(blocks[k], take) for k in range(deep) if k not in riders or k == last}
            send[phase, HALO[direction]] = jnp.where(row < 4, cut[0], cut[last])
            for rider in riders:
                for s in range(2):
                    host = rider - 2 + s
                    cut[host] = jnp.where(
                        within(ride_at, 3 * EDGE), gather(blocks[rider], ride[s]), cut[host]
                    )
            for k in tile_of:
                send[phase, SENT[direction] + tile_of[k]] = cut[k]

    def place_of(cy):
        return 0 if cy == 0 else counts[0] + counts[1] * (cy == 1)

    def exchange(*phases):
        def start(phase, src, at, there_y, amount, target):
            pltpu.make_async_remote_copy(
                src_ref=send.at[phase, pl.ds(src, amount)],
                dst_ref=held.at[phase, pl.ds(place_of(there_y) + at, amount)],
                send_sem=send_sems.at[phase],
                recv_sem=recv_sems.at[phase, 1 + there_y],
                device_id=target,
                device_id_type=MESH,
            ).start()

        for cx, cy in sorted(COLUMNS, key=lambda column: -abs(column[0]) - abs(column[1])):
            for phase in phases:
                if (cx, cy) != (0, 0):
                    amount = tiles if cx else deep
                    at = inner[-cx, abs(cy)]
                    start(phase, SENT[cx], at, -cy, amount, neighbour(cx, cy, 0))
                for ring in range(rings):
                    at = halos[-cx, abs(cy)] + ring
                    start(phase, HALO[cx], at, -cy, 1, neighbour(cx, cy, -1 if ring == 0 else 1))

    def first_tile(stage):
        return counts[0] + counts[1] * side_is_up[stage] if stage else 0

    def arrival(phase, stage):
        rows = held.at[phase, pl.ds(first_tile(stage), counts[1 if stage else 0])]
        which = 1 + side_sign[stage] if stage else 1
        pltpu.make_async_copy(rows, rows, recv_sems.at[phase, which]).wait()

    def wait_all(phase, sems):
        pltpu.make_async_copy(held.at[phase], held.at[phase], sems.at[phase]).wait()

    def merged_tiles(phase, stage):
        first = first_tile(stage)
        far = 1 if stage else 0

        def halo(cx):
            at = first + halos[cx, far]
            if rings == 1:
                return held[phase, at]
            return jnp.where(row < 4, held[phase, at], held[phase, at + 1])

        def tile(cx, number):
            return held[phase, first + inner[cx, far] + number]

        both = []
        for s in range(2):
            row_of_tiles = []
            for v in range(deep + 1):
                k = v - 1
                if v == 0:
                    low, own, high = halo(-1), halo(0), halo(1)
                else:
                    own = tile(0, k) if stage else send[phase, MIDDLE + k]
                    if k in riders:
                        host = tile_of[k - 2 + s]
                        low = gather(tile(-1, host), leave_low)
                        high = gather(tile(1, host), leave_high)
                    else:
                        low, high = tile(-1, tile_of[k]), tile(1, tile_of[k])
                row_of_tiles.append(jnp.where(is_own[s], own, jnp.where(is_low[s], low, high)))
            both.append(row_of_tiles)
        return both

    def page_of(stage, j):
        return REACH * (stage - 1) + j if stage else 0

    depth_y = [None] + [
        jnp.where(side_is_up[stage] > 0, place_y, SIDE - 1 - place_y) for stage in (1, 2)
    ]

    def spread_out(tiles_in, out, parts, stage):
        for v in range(deep + 1):
            for part in range(parts):
                value = gather(tiles_in[part // 3][v], turn_x[part])
                pages = {0: value}
                if stage:
                    base = out[0, part, pl.ds(8 * v, 8), :]
                    pages = {
                        page_of(stage, j): jnp.where(depth_y[stage] < j, value, base)
                        for j in range(1, REACH + 1)
                    }
                for page, value in pages.items():
                    out[page, part, pl.ds(8 * v, 8), :] = value
                    if v == 0:
                        out[page, part, pl.ds(8 * (deep + 1), 8), :] = value

    def contract(sums, parts, vec):
        xx, yy, zz, xy, xz, yz = parts
        for first in (0, 3):
            vx, vy, vz = vec[first : first + 3]
            sums[first] = sums[first] + (xx * vx + xy * vy + xz * vz)
            sums[first + 1] = sums[first + 1] + (xy * vx + yy * vy + yz * vz)
            sums[first + 2] = sums[first + 2] + (xz * vx + yz * vy + zz * vz)

    def tile_number(k, page, sz):
        return (k * PAGES + page) * SPAN + sz + REACH

    def build_tile(k, page, sz):
        start = 8 + sz
        span = pl.ds(8 * k + start, 8)
        dx = near_geo[page, 0, span, :] - own_ref[page, k, 0]
        dy = near_geo[page, 1, span, :] - own_ref[page, k, 1]
        dz = near_geo[page, 2, span, :] - (own_ref[page, k, 2] - spacing * sz)
        weight = switch[k, page, pl.ds(start, 8), :]
        if page == 0 and sz == 0:
            weight = jnp.where(group == REACH, 0.0, weight)
        square = jnp.maximum(dx * dx + dy * dy + dz * dz, 1.0)
        inverse = lax.rsqrt(square)
        inverse_square = inverse * inverse
        damp = square * square * inverse * (near_geo[page, 3, span, :] * own_ref[page, k, 3])
        damping = jnp.exp(-damp)
        fade = jnp.maximum(1.0 - square * (1.0 / cutoff_square), 0.0)
        scale = fade * fade * (inverse_square * inverse) * weight
        three = scale * (1.0 - damping)
        five = (1.0 - (1.0 + damp) * damping) * scale * (3.0 * inverse_square)
        tx, ty, tz = five * dx, five * dy, five * dz
        parts = (tx * dx - three, ty * dy - three, tz * dz - three, tx * dy, tx * dz, ty * dz)
        for part in range(6):
            tensor[tile_number(k, page, sz), part] = parts[part]
        return parts

    def load_tile(k, page, sz):
        return [tensor[tile_number(k, page, sz), part] for part in range(6)]

    def fold(parts):
        width = GROUP
        while len(parts) > 1 or width < 128:
            upper = (lane // width) % 2 == 1
            merged = []
            for index in range(0, len(parts), 2):
                first = parts[index]
                second = parts[index + 1] if index + 1 < len(parts) else first
                kept = jnp.where(upper, second, first)
                moved = jnp.where(upper, first, second)
                merged.append(kept + pltpu.roll(moved, width, 1))
            parts = merged
            width *= 2
        return parts[0]

    def add_stage(make_tile, totals, stage, k):
        for j in range(1, REACH + 1) if stage else [0]:
            sums = [jnp.zeros((8, 128), jnp.float32)] * 6
            page = page_of(stage, j)
            for sz in SHIFTS:
                if j == REACH and abs(sz) == REACH:
                    continue
                span = pl.ds(8 * k + 8 + sz, 8)
                vec = [near[page, part, span, :] for part in range(6)]
                contract(sums, make_tile(k, page, sz), vec)
            for part in range(6):
                if stage:
                    back = 128 - SIDE * side_sign[stage] * j
                    value = pltpu.roll(sums[part], lax.rem(back, 128), 1)
                    totals[k][part] = totals[k][part] + value
                else:
                    totals[k][part] = sums[part]

    def operate(phase, make_tile, vector, prepare=None):
        totals = [[None] * 6 for _ in range(deep)]
        image = []
        for stage in range(3):
            if prepare is not None:
                prepare(stage)
            with scope(f"arrive{phase}_{stage}"):
                arrival(phase, stage)
            with scope(f"stage{phase}_{stage}"):
                spread_out(merged_tiles(phase, stage), near, 6, stage)
                for k in range(deep):
                    add_stage(make_tile, totals, stage, k)
                    if stage == 2:
                        image.append(vector[k] / polar[k] - mask[k] * fold(totals[k]))
        return image

    def build_switch(tiles_in, stage):
        def full(at):
            return jnp.broadcast_to(jnp.asarray(at, jnp.int32), (8, 128))

        own_lane = OWN[1] + GROUP * (FLAGS - 3)
        low_lane = LOW[1][FLAGS - 3]
        cy = side_sign[stage] if stage else 0
        for cz in (-1, 0, 1):
            low_at = full(low_lane + 7 - 3 * (cy + 1) - cz)
            high_at = full(own_lane + SIDE * (cy + 1) + cz + 2)
            middle_at = full(own_lane + SIDE * (2 + cy * cz) if stage else own_lane)
            theirs = jnp.where(reached < 0, low_at, middle_at)
            ours = jnp.where(reached < SIDE, middle_at, high_at)
            ahead = cy > 0 if stage else cz > 0
            use_own = jnp.where(ahead, reached, reached - SIDE) >= 0
            for k in range(deep):
                v = (k + 1 + cz) % (deep + 1)
                there = gather(tiles_in[1][v], theirs)
                here = gather(send[0, MIDDLE + k], ours)
                value = jnp.where(use_own, here, there)
                if stage == 0 and cz == 0:
                    inside_own = jnp.logical_and(reached >= 0, reached < SIDE)
                    value = jnp.where(inside_own, 1.0, value)
                value = jnp.where(group < SPAN, value, 0.0)
                span = pl.ds(8 * (cz + 1), 8)
                if stage == 0:
                    switch[k, 0, span, :] = value
                for j in range(1, REACH + 1) if stage else []:
                    switch[k, page_of(stage, j), span, :] = jnp.where(
                        depth_y[stage] < j, value, switch[k, 0, span, :]
                    )

    in_set = [group < 3, jnp.logical_and(group >= 3, group < 6)]

    def start_sums(number, products):
        values = []
        for first, second in products:
            value = first[0] * second[0]
            for k in range(1, deep):
                value = value + first[k] * second[k]
            line = jnp.sum(value, axis=0, keepdims=True)
            for s in range(2):
                chosen = jnp.where(in_set[s][0:1], line, 0.0)
                values.append(jnp.sum(chosen, axis=1, keepdims=True))
        line = jnp.broadcast_to(values[0], (1, 128))
        for index in range(1, len(values)):
            line = jnp.where(group[0:1] == index, values[index], line)
        sums_out[number] = line
        sums_in[number, my_id] = line
        for step in range(1, total_devices):
            other = lax.rem(my_id + step, total_devices)
            pltpu.make_async_remote_copy(
                src_ref=sums_out.at[number],
                dst_ref=sums_in.at[number, my_id],
                send_sem=sum_send.at[number],
                recv_sem=sum_recv.at[number],
                device_id=device_at(other),
                device_id_type=MESH,
            ).start()

    def wait_sums(number, sems):
        rows = sums_in.at[number, pl.ds(0, total_devices - 1)]
        pltpu.make_async_copy(rows, rows, sems.at[number]).wait()

    def end_sums(number, amount):
        wait_sums(number, sum_recv)
        lines = [sums_in[number, index] for index in range(total_devices)]
        while len(lines) > 1:
            lines = [
                lines[index] + lines[index + 1] if index + 1 < len(lines) else lines[index]
                for index in range(0, len(lines), 2)
            ]
        line = jnp.broadcast_to(lines[0], (8, 128))
        return [
            gather(line, jnp.where(group < 3, GROUP * 2 * index, GROUP * (2 * index + 1)))
            for index in range(amount)
        ]

    def each(function, *vectors):
        return [function(k, *(vector[k] for vector in vectors)) for k in range(deep)]

    with scope("setup"):
        for copy in loads:
            copy.wait()
        site_x = spacing * (place_x.astype(jnp.float32) + 0.5)
        site_y = spacing * (place_y.astype(jnp.float32) + 0.5)
        site_z = spacing * (row.astype(jnp.float32) + 0.5)
        polar, mask, source, geometry = [], [], [], []
        for k in range(deep):
            places = [
                rows_of(coords_ref[3 * k + part]) - offset
                for part, offset in enumerate((site_x, site_y, site_z))
            ]
            polar_k = rows_of(polar_ref[k])
            mask_k = jnp.where(unpack < count_ref[k], 1.0, 0.0)
            root = lax.rsqrt(polar_k)
            slot = 14 + jnp.where(
                place_x == 0, place_y, 4 + 3 * place_y + place_x - 1
            )
            flag = pairs_ref[k, 0, 0] == slot
            for entry in range(1, 13):
                flag = jnp.logical_or(flag, pairs_ref[k, 0, entry] == slot)
            flags = jnp.where(flag, 1.0, 0.0)
            geometry.append(packed(places + [root, flags]))
            for stage in range(3):
                for j in range(1, REACH + 1) if stage else [0]:
                    for part, value in enumerate(places + [thole * root]):
                        if stage:
                            shift_y = side_sign[stage] * j
                            value = pltpu.roll(value, lax.rem(128 + SIDE * shift_y, 128), 1)
                            if part == 1:
                                value = value - spacing * shift_y.astype(jnp.float32)
                        own_ref[page_of(stage, j), k, part] = value - far_x if part == 0 else value
            polar.append(polar_k)
            mask.append(mask_k)
            field_k = packed([rows_of(field_ref[6 * k + part]) for part in range(6)])
            source.append(field_k * mask_k)
        dipoles = each(lambda k, s: polar[k] * s, source)
        put(0, geometry)
        put(1, each(lambda k, d: d * mask[k], dipoles))
    with scope("barrier"):
        pl.semaphore_wait(barrier, len(greeted))
    with scope("send0"):
        exchange(0, 1)

    def prepare(stage):
        with scope(f"geoarrive_{stage}"):
            arrival(0, stage)
        with scope(f"geo_{stage}"):
            tiles_in = merged_tiles(0, stage)
            spread_out(tiles_in, near_geo, 4, stage)
            build_switch(tiles_in, stage)

    image = operate(1, build_tile, dipoles, prepare)
    with scope("finish0"):
        residual = each(lambda k, s, a: s - a, source, image)
        precond = each(lambda k, r: polar[k] * r, residual)
        put(2, each(lambda k, p: p * mask[k], precond))
    with scope("send1"):
        exchange(2)
    image = operate(2, load_tile, precond)
    with scope("finish1"):
        turned = each(lambda k, q: polar[k] * q, image)
        put(3, each(lambda k, t: t * mask[k], turned))
    with scope("send2"):
        exchange(3)
    with scope("sum1"):
        start_sums(0, [(residual, precond), (precond, image)])
    turned_image = operate(3, load_tile, turned)
    with scope("sum1wait"):
        norm, curve = end_sums(0, 2)
    with scope("mid"):
        gamma = norm / curve
        dipoles = each(lambda k, d, p: d + gamma * p, dipoles, precond)
        residual = each(lambda k, r, q: r - gamma * q, residual, image)
        second = each(lambda k, r: polar[k] * r, residual)
        second_image = each(lambda k, q, t: q - gamma * t, image, turned_image)
        start_sums(
            1,
            [
                (residual, second), (second, second_image), (second, image),
                (precond, second_image),
            ],
        )
    with scope("sum2wait"):
        norm_next, second_curve, cross, cross_back = end_sums(1, 4)
    with scope("out"):
        ratio = norm_next / norm
        gamma = norm_next / (second_curve + ratio * (cross + cross_back + ratio * curve))
        for k in range(deep):
            direction = second[k] + ratio * precond[k]
            along = second_image[k] + ratio * image[k]
            for out, value in (
                (dip_out, dipoles[k] + gamma * direction),
                (res_out, residual[k] - gamma * along),
            ):
                for part in range(6):
                    turned_part = gather(value, GROUP * part + site)
                    line = jnp.where(group == row, turned_part, 0.0)
                    out[6 * k + part] = jnp.sum(line, axis=0, keepdims=True)
    with scope("sendwait"):
        for phase in range(4):
            wait_all(phase, send_sems)
        for number in range(2):
            wait_sums(number, sum_send)


def store(dipoles, residual, dip_out, res_out, sems):
    copies = [
        pltpu.make_async_copy(dipoles, dip_out, sems.at[0]),
        pltpu.make_async_copy(residual, res_out, sems.at[1]),
    ]
    for copy in copies:
        copy.start()
    for copy in copies:
        copy.wait()


def on_device(sizes, coords, polar, field, atom_count, pair_list):
    deep, slots = coords.shape[2], coords.shape[-1]
    assert coords.shape[0:2] == (1, 1) and slots == 128
    vmem = pl.BlockSpec(memory_space=pltpu.VMEM)
    hbm = pl.BlockSpec(memory_space=pl.ANY)
    rows = 8 * deep
    devices = sizes[0] * sizes[1] * sizes[2]
    tiles, counts = (plan(deep, 1 if sizes[2] == 2 else 2)[index] for index in (2, 5))

    def buffer(*shape):
        return pltpu.VMEM(shape, jnp.float32)

    line = pltpu.VMEM((6 * deep, 1, slots), jnp.float32)
    result = jax.ShapeDtypeStruct((6 * deep, 1, slots), jnp.float32)
    dma = pltpu.SemaphoreType.DMA
    dipoles, residual = pl.pallas_call(
        functools.partial(kernel, sizes, deep),
        out_shape=(line, line),
        in_specs=[hbm] * 5,
        out_specs=(vmem, vmem),
        scratch_shapes=[
            pltpu.SMEM((deep, 1, pair_list.shape[-1]), jnp.int32),
            pltpu.SMEM((deep,), jnp.int32),
            buffer(3 * deep, 1, slots),
            buffer(deep, 1, slots),
            buffer(6 * deep, 1, slots),
            buffer(4, deep + 2 * tiles + 3, 8, slots),
            buffer(4, counts[0] + 2 * counts[1], 8, slots),
            buffer(PAGES, 6, rows + 16, slots),
            buffer(PAGES, 4, rows + 16, slots),
            buffer(PAGES, deep, 4, 8, slots),
            buffer(deep, PAGES, 24, slots),
            buffer(PAGES * SPAN * deep, 6, 8, slots),
            buffer(2, 1, slots),
            buffer(2, devices, 1, slots),
            dma((5,)),
            dma((4,)),
            dma((4, 3)),
            dma((2,)),
            dma((2,)),
        ],
        compiler_params=pltpu.CompilerParams(collective_id=0, has_side_effects=True),
    )(
        pair_list.reshape(deep, 1, -1),
        atom_count.reshape(deep),
        coords.reshape(3 * deep, 1, slots),
        polar.reshape(deep, 1, slots),
        field.reshape(6 * deep, 1, slots),
    )
    dipoles, residual = pl.pallas_call(
        store,
        out_shape=(result, result),
        in_specs=[vmem, vmem],
        out_specs=(hbm, hbm),
        scratch_shapes=[dma((2,))],
    )(
        pltpu.with_memory_space_constraint(dipoles, pltpu.VMEM),
        pltpu.with_memory_space_constraint(residual, pltpu.VMEM),
    )
    return dipoles.reshape(field.shape), residual.reshape(field.shape)


def solution(mesh):
    sizes = tuple(mesh.shape[name] for name in AXES)
    block = P(*AXES, None, None)
    return jax.shard_map(
        functools.partial(on_device, sizes),
        mesh=mesh,
        in_specs=(block, P(*AXES, None), block, P(*AXES), P(*AXES, None)),
        out_specs=(block, block),
        check_vma=False,
    )
```

```python
import functools

import jax
import jax.numpy as jnp
from jax import lax
from jax.experimental import pallas as pl
from jax.experimental.pallas import tpu as pltpu
from jax.sharding import PartitionSpec as P

MESH = pl.DeviceIdType.MESH
AXES = ("gx", "gy", "gz")
spacing = 2.2
cutoff_square = 49.0
thole = 0.39
SIDE = 4
GROUP = SIDE * SIDE
REACH = 3
SHIFTS = range(-REACH, REACH + 1)
PAGES = 1 + 2 * REACH
SPAN = 2 * REACH + 1
ORDER = [(2, -1), (2, 1), (1, -1), (1, 1), (2, 0), (0, -1), (0, 1), (1, 0), (0, 0)]
COLUMNS = [(cx, cy) for cx in (-1, 0, 1) for cy in (-1, 0, 1)]
EDGE = 12
OWN = (0, 48)
LOW = ((48, 60, 72), (36, 96, 108))
HIGH = ((84, 96, 108), (0, 12, 24))
RIDE_LOW = 0
RIDE_HIGH = 36
FLAGS = 4


def gather(value, index):
    return jnp.take_along_axis(value, index, axis=1, mode="promise_in_bounds")


def plan(deep, rings):
    riders = [k for k in range(deep) if k % 3 == 2]
    tile_of, tiles = {}, 0
    for k in range(deep):
        if k not in riders:
            tile_of[k] = tiles
            tiles += 1
    inner, halos, counts = {}, {}, {}
    for cy in (0, 1):
        total = 0
        for cx in (-1, 0, 1):
            if (cx, cy) != (0, 0):
                inner[cx, cy] = total
                total += tiles if cx else deep
        for cx in (-1, 0, 1):
            halos[cx, cy] = total
            total += rings
        counts[cy] = total
    return riders, tile_of, tiles, inner, halos, counts


def kernel(
    sizes, deep, pairs_hbm, count_hbm, coords_hbm, polar_hbm, field_hbm, dip_out, res_out,
    pairs_ref, count_ref, lines, send, held, near, near_geo, own_ref,
    switch, tensor, sums_out, sums_in, load_sem, send_sem, recv_sems, sum_send, sum_recv,
):
    total_devices = sizes[0] * sizes[1] * sizes[2]
    rings = 1 if sizes[2] == 2 else 2
    riders, tile_of, tiles, inner, halos, counts = plan(deep, rings)
    me = [lax.axis_index(name) for name in AXES]
    my_id = (me[0] * sizes[1] + me[1]) * sizes[2] + me[2]
    scope = jax.named_scope
    up = jnp.where(2 * me[1] < sizes[1], 1, 0)
    side_is_up = (None, up, 1 - up)
    side_sign = (None, 2 * up - 1, 1 - 2 * up)

    def device_at(linear):
        return (
            linear // (sizes[1] * sizes[2]),
            linear // sizes[2] % sizes[1],
            linear % sizes[2],
        )

    def neighbour(cx, cy, cz):
        return tuple(
            lax.rem(place + step + size, size)
            for place, step, size in zip(me, (cx, cy, cz), sizes)
        )

    with scope("signal"):
        barrier = pltpu.get_barrier_semaphore()
        if max(sizes) <= 5:
            steps = [(1, -1, 0) if size > 2 else (1, 0) for size in sizes]
            greeted = [
                neighbour(cx, cy, cz)
                for cx in steps[0] for cy in steps[1] for cz in steps[2]
                if (cx, cy, cz) != (0, 0, 0)
            ]
        else:
            greeted = [
                device_at(lax.rem(my_id + step, total_devices)) for step in range(1, total_devices)
            ]
        for target in greeted:
            pl.semaphore_signal(barrier, inc=1, device_id=target, device_id_type=MESH)
        coords_ref = lines.at[pl.ds(0, 3 * deep)]
        polar_ref = lines.at[pl.ds(3 * deep, deep)]
        field_ref = lines.at[pl.ds(4 * deep, 6 * deep)]
        for src, dst, sem in (
            (coords_hbm, coords_ref, load_sem),
            (polar_hbm, polar_ref, load_sem),
            (field_hbm, field_ref, load_sem),
            (pairs_hbm, pairs_ref, send_sem),
            (count_hbm, count_ref, sum_send),
        ):
            pltpu.make_async_copy(src, dst, sem).start()

    lane = lax.broadcasted_iota(jnp.int32, (8, 128), 1)
    row = lax.broadcasted_iota(jnp.int32, (8, 128), 0)
    group = lane // GROUP
    place_y = lane // SIDE % SIDE
    place_x = lane % SIDE
    site = lane % GROUP
    shift_x = group - REACH
    unpack = GROUP * row + site
    far_x = spacing * shift_x.astype(jnp.float32)

    def within(first, size):
        return jnp.logical_and(lane >= first, lane < first + size)

    def choose(cases, default):
        for condition, value in cases:
            default = jnp.where(condition, value, default)
        return default

    def edge_index(bases, at, first_x):
        cases = []
        for base, start in zip(bases, at):
            local = lane - base
            value = start + SIDE * (local // 3) + local % 3 + first_x
            cases.append((within(base, EDGE), value))
        return choose(cases, jnp.zeros_like(lane))

    all_parts = [GROUP * part for part in range(6)]
    take_low = edge_index(LOW[0] + LOW[1], all_parts, 1)
    take_high = edge_index(HIGH[0] + HIGH[1], all_parts, 0)
    ride_low = [
        edge_index([RIDE_LOW + EDGE * part for part in range(3)], all_parts[3 * s : 3 * s + 3], 1)
        for s in range(2)
    ]
    ride_high = [
        edge_index([RIDE_HIGH + EDGE * part for part in range(3)], all_parts[3 * s : 3 * s + 3], 0)
        for s in range(2)
    ]

    def unride(regions, start):
        cases = []
        for bases in regions:
            for part, base in enumerate(bases):
                cases.append((within(base, EDGE), lane - base + start + EDGE * part))
        return choose(cases, jnp.zeros_like(lane))

    leave_low = unride(LOW, RIDE_LOW)
    leave_high = unride(HIGH, RIDE_HIGH)

    def inside(bases, size):
        result = within(bases[0], size)
        for base in bases[1:]:
            result = jnp.logical_or(result, within(base, size))
        return result

    is_own = [within(OWN[s], 3 * GROUP) for s in range(2)]
    is_low = [inside(LOW[s], EDGE) for s in range(2)]

    reached = place_x + shift_x
    turn_x = []
    for part in range(6):
        s, c = part // 3, part % 3
        low = LOW[s][c] + 3 * place_y + reached + SIDE - 1
        high = HIGH[s][c] + 3 * place_y + jnp.minimum(reached - SIDE, 2)
        own = OWN[s] + GROUP * c + SIDE * place_y + reached
        turn_x.append(jnp.where(reached < 0, low, jnp.where(reached < SIDE, own, high)))

    def packed(parts):
        value = parts[0]
        for index in range(1, len(parts)):
            value = jnp.where(group == index, parts[index], value)
        return value

    def rows_of(line):
        return gather(jnp.broadcast_to(line, (8, 128)), unpack)

    MIDDLE = 0
    SENT = {0: 0, 1: deep + 1, -1: deep + 2 + tiles}
    HALO = {0: deep, 1: deep + 1 + tiles, -1: deep + 2 + 2 * tiles}

    def put(phase, blocks):
        last = deep - 1
        for k in range(deep):
            send[phase, MIDDLE + k] = blocks[k]
        send[phase, HALO[0]] = jnp.where(row < 4, blocks[0], blocks[last])
        for direction, take, ride, ride_at in (
            (1, take_low, ride_low, RIDE_LOW),
            (-1, take_high, ride_high, RIDE_HIGH),
        ):
            cut = {k: gather(blocks[k], take) for k in range(deep) if k not in riders or k == last}
            send[phase, HALO[direction]] = jnp.where(row < 4, cut[0], cut[last])
            for rider in riders:
                for s in range(2):
                    host = rider - 2 + s
                    cut[host] = jnp.where(
                        within(ride_at, 3 * EDGE), gather(blocks[rider], ride[s]), cut[host]
                    )
            for k in tile_of:
                send[phase, SENT[direction] + tile_of[k]] = cut[k]

    def exchange(*phases):
        def start(phase, src, at, stage, amount, target):
            place = counts[0] + counts[1] * (1 - side_is_up[stage]) if stage else 0
            pltpu.make_async_remote_copy(
                src_ref=send.at[phase, pl.ds(src, amount)],
                dst_ref=held.at[phase, pl.ds(place + at, amount)],
                send_sem=send_sem,
                recv_sem=recv_sems.at[max(phase - 1, 0), 1 - side_sign[stage] if stage else 1],
                device_id=target,
                device_id_type=MESH,
            ).start()

        for stage, cx in ORDER:
            cy = side_sign[stage] if stage else 0
            far = 1 if stage else 0
            for phase in phases:
                if stage or cx:
                    amount = tiles if cx else deep
                    start(
                        phase, SENT[cx], inner[-cx, far], stage, amount, neighbour(cx, cy, 0)
                    )
                for ring in range(rings):
                    at = halos[-cx, far] + ring
                    target = neighbour(cx, cy, -1 if ring == 0 else 1)
                    start(phase, HALO[cx], at, stage, 1, target)

    def first_tile(stage):
        return counts[0] + counts[1] * side_is_up[stage] if stage else 0

    def arrival(phase, stage):
        number = max(phase - 1, 0)
        first = pl.ds(0, 2) if number == 0 else pl.ds(phase, 1)
        rows = held.at[first, pl.ds(first_tile(stage), counts[1 if stage else 0])]
        which = 1 + side_sign[stage] if stage else 1
        pltpu.make_async_copy(rows, rows, recv_sems.at[number, which]).wait()

    def merged_tiles(phase, stage):
        first = first_tile(stage)
        far = 1 if stage else 0

        def halo(cx):
            at = first + halos[cx, far]
            if rings == 1:
                return held[phase, at]
            return jnp.where(row < 4, held[phase, at], held[phase, at + 1])

        def tile(cx, number):
            return held[phase, first + inner[cx, far] + number]

        both = []
        for s in range(2):
            row_of_tiles = []
            for v in range(deep + 1):
                k = v - 1
                if v == 0:
                    low, own, high = halo(-1), halo(0), halo(1)
                else:
                    own = tile(0, k) if stage else send[phase, MIDDLE + k]
                    if k in riders:
                        host = tile_of[k - 2 + s]
                        low = gather(tile(-1, host), leave_low)
                        high = gather(tile(1, host), leave_high)
                    else:
                        low, high = tile(-1, tile_of[k]), tile(1, tile_of[k])
                row_of_tiles.append(jnp.where(is_own[s], own, jnp.where(is_low[s], low, high)))
            both.append(row_of_tiles)
        return both

    def page_of(stage, j):
        return REACH * (stage - 1) + j if stage else 0

    depth_y = [None] + [
        jnp.where(side_is_up[stage] > 0, place_y, SIDE - 1 - place_y) for stage in (1, 2)
    ]

    def spread_out(tiles_in, out, parts, stage):
        for v in range(deep + 1):
            for part in range(parts):
                value = gather(tiles_in[part // 3][v], turn_x[part])
                pages = {0: value}
                if stage:
                    base = out[0, part, pl.ds(8 * v, 8), :]
                    pages = {
                        page_of(stage, j): jnp.where(depth_y[stage] < j, value, base)
                        for j in range(1, REACH + 1)
                    }
                for page, value in pages.items():
                    out[page, part, pl.ds(8 * v, 8), :] = value
                    if v == 0:
                        out[page, part, pl.ds(8 * (deep + 1), 8), :] = value

    def contract(sums, parts, vec):
        xx, yy, zz, xy, xz, yz = parts
        for first in (0, 3):
            vx, vy, vz = vec[first : first + 3]
            sums[first] = sums[first] + (xx * vx + xy * vy + xz * vz)
            sums[first + 1] = sums[first + 1] + (xy * vx + yy * vy + yz * vz)
            sums[first + 2] = sums[first + 2] + (xz * vx + yz * vy + zz * vz)

    def tile_number(k, page, sz):
        return (k * PAGES + page) * SPAN + sz + REACH

    def build_tile(k, page, sz):
        start = 8 + sz
        span = pl.ds(8 * k + start, 8)
        dx = near_geo[page, 0, span, :] - own_ref[page, k, 0]
        dy = near_geo[page, 1, span, :] - own_ref[page, k, 1]
        dz = near_geo[page, 2, span, :] - (own_ref[page, k, 2] - spacing * sz)
        weight = switch[k, page, pl.ds(start, 8), :]
        if page == 0 and sz == 0:
            weight = jnp.where(group == REACH, 0.0, weight)
        square = jnp.maximum(dx * dx + dy * dy + dz * dz, 1.0)
        inverse = lax.rsqrt(square)
        inverse_square = inverse * inverse
        damp = square * square * inverse * (near_geo[page, 3, span, :] * own_ref[page, k, 3])
        damping = jnp.exp(-damp)
        fade = jnp.maximum(1.0 - square * (1.0 / cutoff_square), 0.0)
        scale = fade * fade * (inverse_square * inverse) * weight
        three = scale * (1.0 - damping)
        five = (1.0 - (1.0 + damp) * damping) * scale * (3.0 * inverse_square)
        tx, ty, tz = five * dx, five * dy, five * dz
        parts = (tx * dx - three, ty * dy - three, tz * dz - three, tx * dy, tx * dz, ty * dz)
        for part in range(6):
            tensor[tile_number(k, page, sz), part] = parts[part]
        return parts

    def load_tile(k, page, sz):
        return [tensor[tile_number(k, page, sz), part] for part in range(6)]

    def back_roll(stage, j):
        return lax.rem(128 - SIDE * side_sign[stage] * j, 128) if stage else 0

    def gather_groups(sums, stage, j, total):
        back = back_roll(stage, j)
        ends_in = (lane + back) // GROUP % 8
        first, second = total
        for step in range(4):
            comes = (ends_in + step) % 4
            quad = sums[3]
            for part in range(3):
                quad = jnp.where(comes == part, sums[part], quad)
            pair = jnp.where(comes % 2 == 0, sums[4], sums[5])
            shift = back + GROUP * step
            if stage:
                shift = lax.rem(shift, 128)
            if stage or step:
                quad, pair = pltpu.roll(quad, shift, 1), pltpu.roll(pair, shift, 1)
            first = quad if first is None else first + quad
            second = pair if second is None else second + pair
        return first, second

    upper = group >= 4

    def fold(total):
        kept = jnp.where(upper, total[1], total[0])
        moved = jnp.where(upper, total[0], total[1])
        return kept + pltpu.roll(moved, 64, 1)

    def add_stage(make_tile, totals, stage, k):
        for j in range(1, REACH + 1) if stage else [0]:
            sums = [jnp.zeros((8, 128), jnp.float32)] * 6
            page = page_of(stage, j)
            for sz in SHIFTS:
                if j == REACH and abs(sz) == REACH:
                    continue
                span = pl.ds(8 * k + 8 + sz, 8)
                vec = [near[page, part, span, :] for part in range(6)]
                contract(sums, make_tile(k, page, sz), vec)
            totals[k] = gather_groups(sums, stage, j, totals[k])

    def operate(phase, make_tile, vector, prepare=None):
        totals = [(None, None)] * deep
        image = []
        for stage in range(3):
            with scope(f"arrive{phase}_{stage}"):
                arrival(phase, stage)
            if prepare is not None:
                prepare(stage)
            with scope(f"stage{phase}_{stage}"):
                spread_out(merged_tiles(phase, stage), near, 6, stage)
                for k in range(deep):
                    add_stage(make_tile, totals, stage, k)
                    if stage == 2:
                        image.append(vector[k] / polar[k] - mask[k] * fold(totals[k]))
        return image

    def build_switch(tiles_in, stage):
        def full(at):
            return jnp.broadcast_to(jnp.asarray(at, jnp.int32), (8, 128))

        own_lane = OWN[1] + GROUP * (FLAGS - 3)
        low_lane = LOW[1][FLAGS - 3]
        cy = side_sign[stage] if stage else 0
        for cz in (-1, 0, 1):
            low_at = full(low_lane + 7 - 3 * (cy + 1) - cz)
            high_at = full(own_lane + SIDE * (cy + 1) + cz + 2)
            middle_at = full(own_lane + SIDE * (2 + cy * cz) if stage else own_lane)
            theirs = jnp.where(reached < 0, low_at, middle_at)
            ours = jnp.where(reached < SIDE, middle_at, high_at)
            ahead = cy > 0 if stage else cz > 0
            use_own = jnp.where(ahead, reached, reached - SIDE) >= 0
            for k in range(deep):
                v = (k + 1 + cz) % (deep + 1)
                there = gather(tiles_in[1][v], theirs)
                here = gather(send[0, MIDDLE + k], ours)
                value = jnp.where(use_own, here, there)
                if stage == 0 and cz == 0:
                    inside_own = jnp.logical_and(reached >= 0, reached < SIDE)
                    value = jnp.where(inside_own, 1.0, value)
                value = jnp.where(group < SPAN, value, 0.0)
                span = pl.ds(8 * (cz + 1), 8)
                if stage == 0:
                    switch[k, 0, span, :] = value
                for j in range(1, REACH + 1) if stage else []:
                    switch[k, page_of(stage, j), span, :] = jnp.where(
                        depth_y[stage] < j, value, switch[k, 0, span, :]
                    )

    everyone = []
    for far in list(range(1, sizes[1])) + [0]:
        y = lax.rem(me[1] + side_sign[2] * far + sizes[1], sizes[1])
        for cx in range(sizes[0]):
            x = lax.rem(me[0] + cx, sizes[0])
            for cz in range(sizes[2]):
                if far or cx or cz:
                    everyone.append((x, y, lax.rem(me[2] + cz, sizes[2])))

    in_set = [group < 3, jnp.logical_and(group >= 3, group < 6)]

    def start_sums(number, products):
        values = []
        for first, second in products:
            value = first[0] * second[0]
            for k in range(1, deep):
                value = value + first[k] * second[k]
            line = jnp.sum(value, axis=0, keepdims=True)
            for s in range(2):
                chosen = jnp.where(in_set[s][0:1], line, 0.0)
                values.append(jnp.sum(chosen, axis=1, keepdims=True))
        line = jnp.broadcast_to(values[0], (1, 128))
        for index in range(1, len(values)):
            line = jnp.where(group[0:1] == index, values[index], line)
        sums_out[number] = line
        sums_in[number, my_id] = line
        for target in everyone:
            pltpu.make_async_remote_copy(
                src_ref=sums_out.at[number],
                dst_ref=sums_in.at[number, my_id],
                send_sem=sum_send,
                recv_sem=sum_recv.at[number],
                device_id=target,
                device_id_type=MESH,
            ).start()

    def end_sums(number):
        rows = sums_in.at[number, pl.ds(0, total_devices - 1)]
        pltpu.make_async_copy(rows, rows, sum_recv.at[number]).wait()
        lines = [sums_in[number, index] for index in range(total_devices)]
        while len(lines) > 1:
            lines = [
                lines[index] + lines[index + 1] if index + 1 < len(lines) else lines[index]
                for index in range(0, len(lines), 2)
            ]
        return jnp.broadcast_to(lines[0], (8, 128))

    def total_by(first_set, line, index):
        return gather(line, jnp.where(first_set, GROUP * 2 * index, GROUP * (2 * index + 1)))

    def as_rows(value):
        result = value
        for step in range(1, 8):
            moved = pltpu.roll(pltpu.roll(value, 8 - step, 0), GROUP * step, 1)
            result = jnp.where((group - row) % 8 == step, moved, result)
        return result

    def each(function, *vectors):
        return [function(k, *(vector[k] for vector in vectors)) for k in range(deep)]

    with scope("setup"):
        pltpu.make_async_copy(lines, lines, load_sem).wait()
        pltpu.make_async_copy(pairs_hbm, pairs_ref, send_sem).wait()
        pltpu.make_async_copy(count_hbm, count_ref, sum_send).wait()
        site_x = spacing * (place_x.astype(jnp.float32) + 0.5)
        site_y = spacing * (place_y.astype(jnp.float32) + 0.5)
        site_z = spacing * (row.astype(jnp.float32) + 0.5)
        polar, mask, source, geometry = [], [], [], []
        for k in range(deep):
            places = [
                rows_of(coords_ref[3 * k + part]) - offset
                for part, offset in enumerate((site_x, site_y, site_z))
            ]
            polar_k = rows_of(polar_ref[k])
            mask_k = jnp.where(unpack < count_ref[k], 1.0, 0.0)
            root = lax.rsqrt(polar_k)
            slot = 14 + jnp.where(
                place_x == 0, place_y, 4 + 3 * place_y + place_x - 1
            )
            flag = pairs_ref[k, 0, 0] == slot
            for entry in range(1, 13):
                flag = jnp.logical_or(flag, pairs_ref[k, 0, entry] == slot)
            flags = jnp.where(flag, 1.0, 0.0)
            geometry.append(packed(places + [root, flags]))
            for stage in range(3):
                for j in range(1, REACH + 1) if stage else [0]:
                    for part, value in enumerate(places + [thole * root]):
                        if stage:
                            shift_y = side_sign[stage] * j
                            value = pltpu.roll(value, lax.rem(128 + SIDE * shift_y, 128), 1)
                            if part == 1:
                                value = value - spacing * shift_y.astype(jnp.float32)
                        own_ref[page_of(stage, j), k, part] = value - far_x if part == 0 else value
            polar.append(polar_k)
            mask.append(mask_k)
            field_k = packed([rows_of(field_ref[6 * k + part]) for part in range(6)])
            source.append(field_k * mask_k)
        dipoles = each(lambda k, s: polar[k] * s, source)
        put(0, geometry)
        put(1, each(lambda k, d: d * mask[k], dipoles))
    with scope("barrier"):
        pl.semaphore_wait(barrier, len(greeted))
    with scope("send0"):
        exchange(0, 1)

    def prepare(stage):
        with scope(f"geo_{stage}"):
            tiles_in = merged_tiles(0, stage)
            spread_out(tiles_in, near_geo, 4, stage)
            build_switch(tiles_in, stage)

    image = operate(1, build_tile, dipoles, prepare)
    with scope("finish0"):
        residual = each(lambda k, s, a: s - a, source, image)
        precond = each(lambda k, r: polar[k] * r, residual)
        put(2, each(lambda k, p: p * mask[k], precond))
    with scope("send1"):
        exchange(2)
    image = operate(2, load_tile, precond)
    with scope("finish1"):
        turned = each(lambda k, q: polar[k] * q, image)
        put(3, each(lambda k, t: t * mask[k], turned))
    with scope("send2"):
        exchange(3)
    with scope("sum1"):
        start_sums(0, [(residual, precond), (precond, image)])
    turned_image = operate(3, load_tile, turned)
    with scope("sum1wait"):
        first_total = end_sums(0)
        norm, curve = (total_by(group < 3, first_total, index) for index in range(2))
    with scope("mid"):
        gamma = norm / curve
        dipoles = each(lambda k, d, p: d + gamma * p, dipoles, precond)
        residual = each(lambda k, r, q: r - gamma * q, residual, image)
        second = each(lambda k, r: polar[k] * r, residual)
        second_image = each(lambda k, q, t: q - gamma * t, image, turned_image)
        start_sums(
            1,
            [
                (residual, second), (second, second_image), (second, image),
                (precond, second_image),
            ],
        )
    with scope("turn"):
        dipoles, residual, precond, second, image, second_image = (
            each(lambda k, value: as_rows(value), vector)
            for vector in (dipoles, residual, precond, second, image, second_image)
        )
        norm, curve = (total_by(row < 3, first_total, index) for index in range(2))
    with scope("sum2wait"):
        last_total = end_sums(1)
    with scope("out"):
        norm_next, second_curve, cross, cross_back = (
            total_by(row < 3, last_total, index) for index in range(4)
        )
        ratio = norm_next / norm
        gamma = norm_next / (second_curve + ratio * (cross + cross_back + ratio * curve))
        for k in range(deep):
            direction = second[k] + ratio * precond[k]
            along = second_image[k] + ratio * image[k]
            for out, value in (
                (dip_out, dipoles[k] + gamma * direction),
                (res_out, residual[k] - gamma * along),
            ):
                for part in range(6):
                    out[6 * k + part] = value[part : part + 1]
    with scope("sendwait"):
        pltpu.make_async_copy(held, held, send_sem).wait()
        rows = sums_in.at[:, pl.ds(0, total_devices - 1)]
        pltpu.make_async_copy(rows, rows, sum_send).wait()


def store(dipoles, residual, dip_out, res_out, sems):
    copies = [
        pltpu.make_async_copy(dipoles, dip_out, sems.at[0]),
        pltpu.make_async_copy(residual, res_out, sems.at[1]),
    ]
    for copy in copies:
        copy.start()
    for copy in copies:
        copy.wait()


def on_device(sizes, coords, polar, field, atom_count, pair_list):
    deep, slots = coords.shape[2], coords.shape[-1]
    assert coords.shape[0:2] == (1, 1) and slots == 128
    vmem = pl.BlockSpec(memory_space=pltpu.VMEM)
    hbm = pl.BlockSpec(memory_space=pl.ANY)
    rows = 8 * deep
    devices = sizes[0] * sizes[1] * sizes[2]
    tiles, counts = (plan(deep, 1 if sizes[2] == 2 else 2)[index] for index in (2, 5))

    def buffer(*shape):
        return pltpu.VMEM(shape, jnp.float32)

    line = pltpu.VMEM((6 * deep, 1, slots), jnp.float32)
    result = jax.ShapeDtypeStruct((6 * deep, 1, slots), jnp.float32)
    dma = pltpu.SemaphoreType.DMA
    dipoles, residual = pl.pallas_call(
        functools.partial(kernel, sizes, deep),
        out_shape=(line, line),
        in_specs=[hbm] * 5,
        out_specs=(vmem, vmem),
        scratch_shapes=[
            pltpu.SMEM((deep, 1, pair_list.shape[-1]), jnp.int32),
            pltpu.SMEM((deep,), jnp.int32),
            buffer(10 * deep, 1, slots),
            buffer(4, deep + 2 * tiles + 3, 8, slots),
            buffer(4, counts[0] + 2 * counts[1], 8, slots),
            buffer(PAGES, 6, rows + 16, slots),
            buffer(PAGES, 4, rows + 16, slots),
            buffer(PAGES, deep, 4, 8, slots),
            buffer(deep, PAGES, 24, slots),
            buffer(PAGES * SPAN * deep, 6, 8, slots),
            buffer(2, 1, slots),
            buffer(2, devices, 1, slots),
            dma,
            dma,
            dma((3, 3)),
            dma,
            dma((2,)),
        ],
        compiler_params=pltpu.CompilerParams(collective_id=0, has_side_effects=True),
    )(
        pair_list.reshape(deep, 1, -1),
        atom_count.reshape(deep),
        coords.reshape(3 * deep, 1, slots),
        polar.reshape(deep, 1, slots),
        field.reshape(6 * deep, 1, slots),
    )
    dipoles, residual = pl.pallas_call(
        store,
        out_shape=(result, result),
        in_specs=[vmem, vmem],
        out_specs=(hbm, hbm),
        scratch_shapes=[dma((2,))],
    )(
        pltpu.with_memory_space_constraint(dipoles, pltpu.VMEM),
        pltpu.with_memory_space_constraint(residual, pltpu.VMEM),
    )
    return dipoles.reshape(field.shape), residual.reshape(field.shape)


def solution(mesh):
    sizes = tuple(mesh.shape[name] for name in AXES)
    block = P(*AXES, None, None)
    return jax.shard_map(
        functools.partial(on_device, sizes),
        mesh=mesh,
        in_specs=(block, P(*AXES, None), block, P(*AXES), P(*AXES, None)),
        out_specs=(block, block),
        check_vma=False,
    )
```

```python
import functools
import math

import jax
import jax.numpy as jnp
from jax import lax
from jax.experimental import pallas as pl
from jax.experimental.pallas import tpu as pltpu
from jax.sharding import PartitionSpec as P

MESH = pl.DeviceIdType.MESH
AXES = ("gx", "gy", "gz")
spacing = 2.2
cutoff_square = 49.0
thole = 0.39
SIDE = 4
GROUP = SIDE * SIDE
REACH = 3
SHIFTS = range(-REACH, REACH + 1)
PAGES = 1 + 2 * REACH
SPAN = 2 * REACH + 1
ORDER = [(2, -1), (2, 1), (1, -1), (1, 1), (2, 0), (0, -1), (0, 1), (1, 0), (0, 0)]
COLUMNS = [(cx, cy) for cx in (-1, 0, 1) for cy in (-1, 0, 1)]
REST = 6
EDGE = 12
OWN = (0, 48)
LOW = ((48, 60, 72), (36, 96, 108))
HIGH = ((84, 96, 108), (0, 12, 24))
RIDE_LOW = 0
RIDE_HIGH = 36
FLAGS = 4


def gather(value, index):
    return jnp.take_along_axis(value, index, axis=1, mode="promise_in_bounds")


def plan(deep, rings):
    riders = [k for k in range(deep) if k % 3 == 2]
    tile_of, tiles = {}, 0
    for k in range(deep):
        if k not in riders:
            tile_of[k] = tiles
            tiles += 1
    inner, halos, counts = {}, {}, {}
    for cy in (0, 1):
        total = 0
        for cx in (-1, 0, 1):
            if (cx, cy) != (0, 0):
                inner[cx, cy] = total
                total += tiles if cx else deep
        for cx in (-1, 0, 1):
            halos[cx, cy] = total
            total += rings
        counts[cy] = total
    return riders, tile_of, tiles, inner, halos, counts


def kernel(
    sizes, deep, pairs_hbm, count_hbm, coords_hbm, polar_hbm, field_hbm, dip_out, res_out,
    pairs_ref, count_ref, lines, send, held, near, near_geo, own_ref,
    switch, tensor, sums_out, sums_in, load_sem, send_sem, recv_sems, sum_send, sum_recv,
):
    total_devices = sizes[0] * sizes[1] * sizes[2]
    rings = 1 if sizes[2] == 2 else 2
    riders, tile_of, tiles, inner, halos, counts = plan(deep, rings)
    me = [lax.axis_index(name) for name in AXES]
    my_id = (me[0] * sizes[1] + me[1]) * sizes[2] + me[2]
    scope = jax.named_scope
    up = jnp.where(2 * me[1] < sizes[1], 1, 0)
    side_is_up = (None, up, 1 - up)
    side_sign = (None, 2 * up - 1, 1 - 2 * up)

    def device_at(linear):
        return (
            linear // (sizes[1] * sizes[2]),
            linear // sizes[2] % sizes[1],
            linear % sizes[2],
        )

    def neighbour(cx, cy, cz):
        return tuple(
            lax.rem(place + step + size, size)
            for place, step, size in zip(me, (cx, cy, cz), sizes)
        )

    with scope("signal"):
        barrier = pltpu.get_barrier_semaphore()
        if max(sizes) <= 5:
            steps = [(1, -1, 0) if size > 2 else (1, 0) for size in sizes]
            greeted = [
                neighbour(cx, cy, cz)
                for cx in steps[0] for cy in steps[1] for cz in steps[2]
                if (cx, cy, cz) != (0, 0, 0)
            ]
        else:
            greeted = [
                device_at(lax.rem(my_id + step, total_devices)) for step in range(1, total_devices)
            ]
        for target in greeted:
            pl.semaphore_signal(barrier, inc=1, device_id=target, device_id_type=MESH)
        coords_ref = lines.at[pl.ds(0, 3 * deep)]
        polar_ref = lines.at[pl.ds(3 * deep, deep)]
        field_ref = lines.at[pl.ds(4 * deep, 6 * deep)]
        for src, dst, sem in (
            (coords_hbm, coords_ref, load_sem),
            (polar_hbm, polar_ref, load_sem),
            (field_hbm, field_ref, load_sem),
            (pairs_hbm, pairs_ref, send_sem),
            (count_hbm, count_ref, sum_send),
        ):
            pltpu.make_async_copy(src, dst, sem).start()

    lane = lax.broadcasted_iota(jnp.int32, (8, 128), 1)
    row = lax.broadcasted_iota(jnp.int32, (8, 128), 0)
    group = lane // GROUP
    place_y = lane // SIDE % SIDE
    place_x = lane % SIDE
    site = lane % GROUP
    shift_x = group - REACH
    unpack = GROUP * row + site
    far_x = spacing * shift_x.astype(jnp.float32)

    def within(first, size):
        return jnp.logical_and(lane >= first, lane < first + size)

    def choose(cases, default):
        for condition, value in cases:
            default = jnp.where(condition, value, default)
        return default

    def edge_index(bases, at, first_x):
        cases = []
        for base, start in zip(bases, at):
            local = lane - base
            value = start + SIDE * (local // 3) + local % 3 + first_x
            cases.append((within(base, EDGE), value))
        return choose(cases, jnp.zeros_like(lane))

    all_parts = [GROUP * part for part in range(6)]
    take_low = edge_index(LOW[0] + LOW[1], all_parts, 1)
    take_high = edge_index(HIGH[0] + HIGH[1], all_parts, 0)
    ride_low = [
        edge_index([RIDE_LOW + EDGE * part for part in range(3)], all_parts[3 * s : 3 * s + 3], 1)
        for s in range(2)
    ]
    ride_high = [
        edge_index([RIDE_HIGH + EDGE * part for part in range(3)], all_parts[3 * s : 3 * s + 3], 0)
        for s in range(2)
    ]

    def unride(regions, start):
        cases = []
        for bases in regions:
            for part, base in enumerate(bases):
                cases.append((within(base, EDGE), lane - base + start + EDGE * part))
        return choose(cases, jnp.zeros_like(lane))

    leave_low = unride(LOW, RIDE_LOW)
    leave_high = unride(HIGH, RIDE_HIGH)

    def inside(bases, size):
        result = within(bases[0], size)
        for base in bases[1:]:
            result = jnp.logical_or(result, within(base, size))
        return result

    is_own = [within(OWN[s], 3 * GROUP) for s in range(2)]
    is_low = [inside(LOW[s], EDGE) for s in range(2)]

    reached = place_x + shift_x
    turn_x = []
    for part in range(6):
        s, c = part // 3, part % 3
        low = LOW[s][c] + 3 * place_y + reached + SIDE - 1
        high = HIGH[s][c] + 3 * place_y + jnp.minimum(reached - SIDE, 2)
        own = OWN[s] + GROUP * c + SIDE * place_y + reached
        turn_x.append(jnp.where(reached < 0, low, jnp.where(reached < SIDE, own, high)))

    def packed(parts):
        value = parts[0]
        for index in range(1, len(parts)):
            value = jnp.where(group == index, parts[index], value)
        return value

    def rows_of(line):
        return gather(jnp.broadcast_to(line, (8, 128)), unpack)

    MIDDLE = 0
    SENT = {0: 0, 1: deep + 1, -1: deep + 2 + tiles}
    HALO = {0: deep, 1: deep + 1 + tiles, -1: deep + 2 + 2 * tiles}

    sent_tiles = deep + 2 * tiles + 3
    held_tiles = counts[0] + 2 * counts[1]

    def sent_rows(phase, tile, amount=8):
        return pl.ds(8 * (phase * sent_tiles + tile), amount)

    def held_rows(phase, tile, amount=8):
        return pl.ds(pl.multiple_of(8 * (phase * held_tiles + tile), 8), amount)

    def put_tile(phase, tile, value):
        send[sent_rows(phase, tile), :] = value

    def ends(bottom, top):
        return jnp.where(row < REACH, bottom, pltpu.roll(top, REST, 0))

    def put(phase, blocks):
        last = deep - 1
        for k in range(deep):
            put_tile(phase, MIDDLE + k, blocks[k])
        put_tile(phase, HALO[0], ends(blocks[0], blocks[last]))
        for direction, take, ride, ride_at in (
            (1, take_low, ride_low, RIDE_LOW),
            (-1, take_high, ride_high, RIDE_HIGH),
        ):
            cut = {k: gather(blocks[k], take) for k in range(deep) if k not in riders or k == last}
            put_tile(phase, HALO[direction], ends(cut[0], cut[last]))
            for rider in riders:
                for s in range(2):
                    host = rider - 2 + s
                    cut[host] = jnp.where(
                        within(ride_at, 3 * EDGE), gather(blocks[rider], ride[s]), cut[host]
                    )
            for k in tile_of:
                put_tile(phase, SENT[direction] + tile_of[k], cut[k])

    def exchange(*phases):
        def start(phase, src, at, stage, rows, target):
            place = counts[0] + counts[1] * (1 - side_is_up[stage]) if stage else 0
            pltpu.make_async_remote_copy(
                src_ref=send.at[sent_rows(phase, src, rows)],
                dst_ref=held.at[held_rows(phase, place + at, rows)],
                send_sem=send_sem,
                recv_sem=recv_sems.at[phase, 1 - side_sign[stage] if stage else 1],
                device_id=target,
                device_id_type=MESH,
            ).start()

        for phase in phases:
            for stage, cx in ORDER:
                cy = side_sign[stage] if stage else 0
                far = 1 if stage else 0
                if stage or cx:
                    rows = 8 * (tiles if cx else deep)
                    start(phase, SENT[cx], inner[-cx, far], stage, rows, neighbour(cx, cy, 0))
                for ring in range(rings):
                    at = halos[-cx, far] + ring
                    target = neighbour(cx, cy, -1 if ring == 0 else 1)
                    start(phase, HALO[cx], at, stage, REST, target)

    def first_tile(stage):
        return counts[0] + counts[1] * side_is_up[stage] if stage else 0

    rows_in = [8 * counts[far] - (8 - REST) * 3 * rings for far in (0, 1)]

    def arrival(phase, stage):
        rows = held.at[held_rows(phase, first_tile(stage), rows_in[1 if stage else 0])]
        which = 1 + side_sign[stage] if stage else 1
        pltpu.make_async_copy(rows, rows, recv_sems.at[phase, which]).wait()

    def merged_tiles(phase, stage):
        first = first_tile(stage)
        far = 1 if stage else 0

        def halo(cx):
            at = first + halos[cx, far]
            top = held[held_rows(phase, at + rings - 1), :]
            return jnp.where(row < 4, held[held_rows(phase, at), :], pltpu.roll(top, 8 - REST, 0))

        def tile(cx, number):
            return held[held_rows(phase, first + inner[cx, far] + number), :]

        both = []
        for s in range(2):
            row_of_tiles = []
            for v in range(deep + 1):
                k = v - 1
                if v == 0:
                    low, own, high = halo(-1), halo(0), halo(1)
                else:
                    own = tile(0, k) if stage else send[sent_rows(phase, MIDDLE + k), :]
                    if k in riders:
                        host = tile_of[k - 2 + s]
                        low = gather(tile(-1, host), leave_low)
                        high = gather(tile(1, host), leave_high)
                    else:
                        low, high = tile(-1, tile_of[k]), tile(1, tile_of[k])
                row_of_tiles.append(jnp.where(is_own[s], own, jnp.where(is_low[s], low, high)))
            both.append(row_of_tiles)
        return both

    def page_of(stage, j):
        return REACH * (stage - 1) + j if stage else 0

    depth_y = [None] + [
        jnp.where(side_is_up[stage] > 0, place_y, SIDE - 1 - place_y) for stage in (1, 2)
    ]

    def spread_out(tiles_in, out, parts, stage):
        for v in range(deep + 1):
            for part in range(parts):
                value = gather(tiles_in[part // 3][v], turn_x[part])
                pages = {0: value}
                if stage:
                    base = out[0, part, pl.ds(8 * v, 8), :]
                    pages = {
                        page_of(stage, j): jnp.where(depth_y[stage] < j, value, base)
                        for j in range(1, REACH + 1)
                    }
                for page, value in pages.items():
                    out[page, part, pl.ds(8 * v, 8), :] = value
                    if v == 0:
                        out[page, part, pl.ds(8 * (deep + 1), 8), :] = value

    def contract(sums, parts, vec):
        dx, dy, dz, tx, ty, tz, three = parts
        for first in (0, 3):
            vx, vy, vz = vec[first : first + 3]
            along = tx * vx + ty * vy + tz * vz
            for part, (d, v) in enumerate(((dx, vx), (dy, vy), (dz, vz))):
                term = d * along - three * v
                at = first + part
                sums[at] = term if sums[at] is None else sums[at] + term

    def tile_number(k, page, sz):
        return (k * PAGES + page) * SPAN + sz + REACH

    def build_tile(k, page, sz):
        start = 8 + sz
        span = pl.ds(8 * k + start, 8)
        dx = near_geo[page, 0, span, :] - own_ref[page, k, 0]
        dy = near_geo[page, 1, span, :] - own_ref[page, k, 1]
        dz = near_geo[page, 2, span, :] - (own_ref[page, k, 2] - spacing * sz)
        weight = switch[k, page, pl.ds(start, 8), :]
        if page == 0 and sz == 0:
            weight = jnp.where(group == REACH, 0.0, weight)
        square = dx * dx + dy * dy + dz * dz
        if page == 0 and sz == 0:
            square = jnp.maximum(square, 1.0)
        inverse = lax.rsqrt(square)
        inverse_square = inverse * inverse
        damp = square * (square * inverse) * (near_geo[page, 3, span, :] * own_ref[page, k, 3])
        damping = jnp.exp2(damp * (-1.0 / math.log(2.0)))
        fade = jnp.maximum(cutoff_square - square, 0.0)
        scale = fade * fade * (inverse_square * inverse) * weight
        three = scale - scale * damping
        five = (three - scale * (damp * damping)) * (3.0 * inverse_square)
        parts = (dx, dy, dz, five * dx, five * dy, five * dz, three)
        for part, value in enumerate(parts):
            tensor[tile_number(k, page, sz), part] = value
        return parts

    def load_tile(k, page, sz):
        return [tensor[tile_number(k, page, sz), part] for part in range(7)]

    def back_roll(stage, j):
        return lax.rem(128 - SIDE * side_sign[stage] * j, 128) if stage else 0

    def gather_groups(sums, stage, j, total):
        back = back_roll(stage, j)
        ends_in = (lane + back) // GROUP % 8
        first, second = total
        for step in range(4):
            comes = (ends_in + step) % 4
            quad = sums[3]
            for part in range(3):
                quad = jnp.where(comes == part, sums[part], quad)
            pair = jnp.where(comes % 2 == 0, sums[4], sums[5])
            shift = back + GROUP * step
            if stage:
                shift = lax.rem(shift, 128)
            if stage or step:
                quad, pair = pltpu.roll(quad, shift, 1), pltpu.roll(pair, shift, 1)
            first = quad if first is None else first + quad
            second = pair if second is None else second + pair
        return first, second

    upper = group >= 4

    def fold(total):
        kept = jnp.where(upper, total[1], total[0])
        moved = jnp.where(upper, total[0], total[1])
        return kept + pltpu.roll(moved, 64, 1)

    def used(stage):
        for j in range(1, REACH + 1) if stage else [0]:
            yield j, [sz for sz in SHIFTS if j < REACH or abs(sz) < REACH]

    def stage_tiles(stage, k):
        for j, shifts in used(stage):
            for sz in shifts:
                build_tile(k, page_of(stage, j), sz)

    def stage_sums(make_tile, stage, k):
        result = []
        for j, shifts in used(stage):
            sums = [None] * 6
            page = page_of(stage, j)
            for sz in shifts:
                span = pl.ds(8 * k + 8 + sz, 8)
                vec = [near[page, part, span, :] for part in range(6)]
                contract(sums, make_tile(k, page, sz), vec)
            result.append((sums, stage, j))
        return result

    def operate(phase, make_tile, vector, prepare=None):
        totals = [(None, None)] * deep
        waiting = [[] for _ in range(deep)]
        image = []
        for stage in range(3):
            if prepare is not None:
                prepare(stage)
            if prepare is not None and stage == 2:
                with scope("tiles"):
                    for k in range(deep):
                        stage_tiles(stage, k)
                make_tile = load_tile
            with scope(f"arrive{phase}_{stage}"):
                arrival(phase, stage)
            with scope(f"stage{phase}_{stage}"):
                spread_out(merged_tiles(phase, stage), near, 6, stage)
                for k in range(deep):
                    for item in waiting[k]:
                        totals[k] = gather_groups(*item, totals[k])
                    waiting[k] = stage_sums(make_tile, stage, k)
                    if stage == 2:
                        for item in waiting[k]:
                            totals[k] = gather_groups(*item, totals[k])
                        image.append(vector[k] / polar[k] - mask[k] * fold(totals[k]))
        return image

    def build_switch(tiles_in, stage):
        def full(at):
            return jnp.broadcast_to(jnp.asarray(at, jnp.int32), (8, 128))

        own_lane = OWN[1] + GROUP * (FLAGS - 3)
        low_lane = LOW[1][FLAGS - 3]
        cy = side_sign[stage] if stage else 0
        for cz in (-1, 0, 1):
            low_at = full(low_lane + 7 - 3 * (cy + 1) - cz)
            high_at = full(own_lane + SIDE * (cy + 1) + cz + 2)
            middle_at = full(own_lane + SIDE * (2 + cy * cz) if stage else own_lane)
            theirs = jnp.where(reached < 0, low_at, middle_at)
            ours = jnp.where(reached < SIDE, middle_at, high_at)
            ahead = cy > 0 if stage else cz > 0
            use_own = jnp.where(ahead, reached, reached - SIDE) >= 0
            for k in range(deep):
                v = (k + 1 + cz) % (deep + 1)
                there = gather(tiles_in[1][v], theirs)
                here = gather(send[sent_rows(0, MIDDLE + k), :], ours)
                value = jnp.where(use_own, here, there)
                if stage == 0 and cz == 0:
                    inside_own = jnp.logical_and(reached >= 0, reached < SIDE)
                    value = jnp.where(inside_own, 1.0 / cutoff_square**2, value)
                value = jnp.where(group < SPAN, value, 0.0)
                span = pl.ds(8 * (cz + 1), 8)
                if stage == 0:
                    switch[k, 0, span, :] = value
                for j in range(1, REACH + 1) if stage else []:
                    switch[k, page_of(stage, j), span, :] = jnp.where(
                        depth_y[stage] < j, value, switch[k, 0, span, :]
                    )

    everyone = []
    for far in list(range(1, sizes[1])) + [0]:
        y = lax.rem(me[1] + side_sign[2] * far + sizes[1], sizes[1])
        for cx in range(sizes[0]):
            x = lax.rem(me[0] + cx, sizes[0])
            for cz in range(sizes[2]):
                if far or cx or cz:
                    everyone.append((x, y, lax.rem(me[2] + cz, sizes[2])))

    in_set = [group < 3, jnp.logical_and(group >= 3, group < 6)]

    def put_sums(number, products):
        values = []
        for first, second in products:
            value = first[0] * second[0]
            for k in range(1, deep):
                value = value + first[k] * second[k]
            line = jnp.sum(value, axis=0, keepdims=True)
            for s in range(2):
                chosen = jnp.where(in_set[s][0:1], line, 0.0)
                values.append(jnp.sum(chosen, axis=1, keepdims=True))
        line = jnp.broadcast_to(values[0], (1, 128))
        for index in range(1, len(values)):
            line = jnp.where(group[0:1] == index, values[index], line)
        sums_out[number] = line
        sums_in[number, my_id] = line

    def send_sums(number):
        for target in everyone:
            pltpu.make_async_remote_copy(
                src_ref=sums_out.at[number],
                dst_ref=sums_in.at[number, my_id],
                send_sem=sum_send,
                recv_sem=sum_recv.at[number],
                device_id=target,
                device_id_type=MESH,
            ).start()

    def end_sums(number):
        rows = sums_in.at[number, pl.ds(0, total_devices - 1)]
        pltpu.make_async_copy(rows, rows, sum_recv.at[number]).wait()
        lines = [sums_in[number, index] for index in range(total_devices)]
        while len(lines) > 1:
            lines = [
                lines[index] + lines[index + 1] if index + 1 < len(lines) else lines[index]
                for index in range(0, len(lines), 2)
            ]
        return jnp.broadcast_to(lines[0], (8, 128))

    def total_by(first_set, line, index):
        return gather(line, jnp.where(first_set, GROUP * 2 * index, GROUP * (2 * index + 1)))

    def as_rows(value):
        result = value
        for step in range(1, 8):
            moved = pltpu.roll(pltpu.roll(value, 8 - step, 0), GROUP * step, 1)
            result = jnp.where((group - row) % 8 == step, moved, result)
        return result

    def each(function, *vectors):
        return [function(k, *(vector[k] for vector in vectors)) for k in range(deep)]

    with scope("setup"):
        pltpu.make_async_copy(lines, lines, load_sem).wait()
        pltpu.make_async_copy(pairs_hbm, pairs_ref, send_sem).wait()
        pltpu.make_async_copy(count_hbm, count_ref, sum_send).wait()
        site_x = spacing * (place_x.astype(jnp.float32) + 0.5)
        site_y = spacing * (place_y.astype(jnp.float32) + 0.5)
        site_z = spacing * (row.astype(jnp.float32) + 0.5)
        polar, mask, source, geometry = [], [], [], []
        for k in range(deep):
            places = [
                rows_of(coords_ref[3 * k + part]) - offset
                for part, offset in enumerate((site_x, site_y, site_z))
            ]
            polar_k = rows_of(polar_ref[k])
            mask_k = jnp.where(unpack < count_ref[k], 1.0, 0.0)
            root = lax.rsqrt(polar_k)
            slot = 14 + jnp.where(
                place_x == 0, place_y, 4 + 3 * place_y + place_x - 1
            )
            flag = pairs_ref[k, 0, 0] == slot
            for entry in range(1, 13):
                flag = jnp.logical_or(flag, pairs_ref[k, 0, entry] == slot)
            flags = jnp.where(flag, 1.0 / cutoff_square**2, 0.0)
            geometry.append(packed(places + [root, flags]))
            for stage in range(3):
                for j in range(1, REACH + 1) if stage else [0]:
                    for part, value in enumerate(places + [thole * root]):
                        if stage:
                            shift_y = side_sign[stage] * j
                            value = pltpu.roll(value, lax.rem(128 + SIDE * shift_y, 128), 1)
                            if part == 1:
                                value = value - spacing * shift_y.astype(jnp.float32)
                        own_ref[page_of(stage, j), k, part] = value - far_x if part == 0 else value
            polar.append(polar_k)
            mask.append(mask_k)
            field_k = packed([rows_of(field_ref[6 * k + part]) for part in range(6)])
            source.append(field_k * mask_k)
        dipoles = each(lambda k, s: polar[k] * s, source)
        put(0, geometry)
        put(1, each(lambda k, d: d * mask[k], dipoles))
    with scope("barrier"):
        pl.semaphore_wait(barrier, len(greeted))
    with scope("send0"):
        exchange(0, 1)

    def prepare(stage):
        with scope(f"geoarrive_{stage}"):
            arrival(0, stage)
        with scope(f"geo_{stage}"):
            tiles_in = merged_tiles(0, stage)
            spread_out(tiles_in, near_geo, 4, stage)
            build_switch(tiles_in, stage)

    image = operate(1, build_tile, dipoles, prepare)
    with scope("finish0"):
        residual = each(lambda k, s, a: s - a, source, image)
        precond = each(lambda k, r: polar[k] * r, residual)
        put(2, each(lambda k, p: p * mask[k], precond))
    with scope("send1"):
        exchange(2)
    image = operate(2, load_tile, precond)
    with scope("finish1"):
        turned = each(lambda k, q: polar[k] * q, image)
        put(3, each(lambda k, t: t * mask[k], turned))
        put_sums(0, [(residual, precond), (precond, image)])
    with scope("send2"):
        exchange(3)
        send_sums(0)
    turned_image = operate(3, load_tile, turned)
    with scope("sum1wait"):
        first_total = end_sums(0)
        norm, curve = (total_by(group < 3, first_total, index) for index in range(2))
    with scope("mid"):
        gamma = norm / curve
        dipoles = each(lambda k, d, p: d + gamma * p, dipoles, precond)
        residual = each(lambda k, r, q: r - gamma * q, residual, image)
        second = each(lambda k, r: polar[k] * r, residual)
        second_image = each(lambda k, q, t: q - gamma * t, image, turned_image)
        put_sums(
            1,
            [
                (residual, second), (second, second_image), (second, image),
                (precond, second_image),
            ],
        )
        send_sums(1)
    with scope("turn"):
        dipoles, residual, precond, second, image, second_image = (
            each(lambda k, value: as_rows(value), vector)
            for vector in (dipoles, residual, precond, second, image, second_image)
        )
        norm, curve = (total_by(row < 3, first_total, index) for index in range(2))
    with scope("sum2wait"):
        last_total = end_sums(1)
    with scope("out"):
        norm_next, second_curve, cross, cross_back = (
            total_by(row < 3, last_total, index) for index in range(4)
        )
        ratio = norm_next / norm
        gamma = norm_next / (second_curve + ratio * (cross + cross_back + ratio * curve))
        for k in range(deep):
            direction = second[k] + ratio * precond[k]
            along = second_image[k] + ratio * image[k]
            for out, value in (
                (dip_out, dipoles[k] + gamma * direction),
                (res_out, residual[k] - gamma * along),
            ):
                for part in range(6):
                    out[6 * k + part] = value[part : part + 1]
    with scope("sendwait"):
        rows = held.at[pl.ds(0, 4 * (rows_in[0] + 2 * rows_in[1]))]
        pltpu.make_async_copy(rows, rows, send_sem).wait()
        rows = sums_in.at[:, pl.ds(0, total_devices - 1)]
        pltpu.make_async_copy(rows, rows, sum_send).wait()


def store(dipoles, residual, dip_out, res_out, sems):
    copies = [
        pltpu.make_async_copy(dipoles, dip_out, sems.at[0]),
        pltpu.make_async_copy(residual, res_out, sems.at[1]),
    ]
    for copy in copies:
        copy.start()
    for copy in copies:
        copy.wait()


def on_device(sizes, coords, polar, field, atom_count, pair_list):
    deep, slots = coords.shape[2], coords.shape[-1]
    assert coords.shape[0:2] == (1, 1) and slots == 128
    vmem = pl.BlockSpec(memory_space=pltpu.VMEM)
    hbm = pl.BlockSpec(memory_space=pl.ANY)
    rows = 8 * deep
    devices = sizes[0] * sizes[1] * sizes[2]
    tiles, counts = (plan(deep, 1 if sizes[2] == 2 else 2)[index] for index in (2, 5))

    def buffer(*shape):
        return pltpu.VMEM(shape, jnp.float32)

    line = pltpu.VMEM((6 * deep, 1, slots), jnp.float32)
    result = jax.ShapeDtypeStruct((6 * deep, 1, slots), jnp.float32)
    dma = pltpu.SemaphoreType.DMA
    dipoles, residual = pl.pallas_call(
        functools.partial(kernel, sizes, deep),
        out_shape=(line, line),
        in_specs=[hbm] * 5,
        out_specs=(vmem, vmem),
        scratch_shapes=[
            pltpu.SMEM((deep, 1, pair_list.shape[-1]), jnp.int32),
            pltpu.SMEM((deep,), jnp.int32),
            buffer(10 * deep, 1, slots),
            buffer(4 * 8 * (deep + 2 * tiles + 3), slots),
            buffer(4 * 8 * (counts[0] + 2 * counts[1]), slots),
            buffer(PAGES, 6, rows + 16, slots),
            buffer(PAGES, 4, rows + 16, slots),
            buffer(PAGES, deep, 4, 8, slots),
            buffer(deep, PAGES, 24, slots),
            buffer(PAGES * SPAN * deep, 7, 8, slots),
            buffer(2, 1, slots),
            buffer(2, devices, 1, slots),
            dma,
            dma,
            dma((4, 3)),
            dma,
            dma((2,)),
        ],
        compiler_params=pltpu.CompilerParams(collective_id=0, has_side_effects=True),
    )(
        pair_list.reshape(deep, 1, -1),
        atom_count.reshape(deep),
        coords.reshape(3 * deep, 1, slots),
        polar.reshape(deep, 1, slots),
        field.reshape(6 * deep, 1, slots),
    )
    dipoles, residual = pl.pallas_call(
        store,
        out_shape=(result, result),
        in_specs=[vmem, vmem],
        out_specs=(hbm, hbm),
        scratch_shapes=[dma((2,))],
    )(
        pltpu.with_memory_space_constraint(dipoles, pltpu.VMEM),
        pltpu.with_memory_space_constraint(residual, pltpu.VMEM),
    )
    return dipoles.reshape(field.shape), residual.reshape(field.shape)


def solution(mesh):
    sizes = tuple(mesh.shape[name] for name in AXES)
    block = P(*AXES, None, None)
    return jax.shard_map(
        functools.partial(on_device, sizes),
        mesh=mesh,
        in_specs=(block, P(*AXES, None), block, P(*AXES), P(*AXES, None)),
        out_specs=(block, block),
        check_vma=False,
    )
```

```python
import functools
import math

import jax
import jax.numpy as jnp
from jax import lax
from jax.experimental import pallas as pl
from jax.experimental.pallas import tpu as pltpu
from jax.sharding import PartitionSpec as P

MESH = pl.DeviceIdType.MESH
AXES = ("gx", "gy", "gz")
spacing = 2.2
cutoff_square = 49.0
thole = 0.39
SIDE = 4
GROUP = SIDE * SIDE
REACH = 3
SHIFTS = range(-REACH, REACH + 1)
PAGES = 1 + 2 * REACH
SPAN = 2 * REACH + 1
ORDER = [(2, -1), (2, 1), (1, -1), (1, 1), (2, 0), (0, -1), (0, 1), (1, 0), (0, 0)]
COLUMNS = [(cx, cy) for cx in (-1, 0, 1) for cy in (-1, 0, 1)]
REST = 6
EDGE = 12
OWN = (0, 48)
LOW = ((48, 60, 72), (36, 96, 108))
HIGH = ((84, 96, 108), (0, 12, 24))
RIDE_LOW = 0
RIDE_HIGH = 36
WIDE_LOW = (84, 0)
WIDE_HIGH = (48, 12)
WIDE_FLAGS = 120
FLAGS = 4


def gather(value, index):
    return jnp.take_along_axis(value, index, axis=1, mode="promise_in_bounds")


def plan(deep, rings):
    riders = [k for k in range(deep) if k % 3 == 2]
    tile_of, tiles = {}, 0
    for k in range(deep):
        if k not in riders:
            tile_of[k] = tiles
            tiles += 1
    inner, halos, counts = {}, {}, {}
    for cy in (0, 1):
        total = 0
        for cx in (-1, 0, 1):
            if (cx, cy) != (0, 0):
                inner[cx, cy] = total
                total += tiles if cx else deep
        for cx in (-1, 0, 1):
            halos[cx, cy] = total
            total += rings
        counts[cy] = total
    return riders, tile_of, tiles, inner, halos, counts


def kernel(
    sizes, deep, pairs_hbm, count_hbm, coords_hbm, polar_hbm, field_hbm, dip_out, res_out,
    pairs_ref, count_ref, lines, send, held, send_wide, held_wide, near, near_geo, own_ref,
    switch, tensor, sums_out, sums_in, load_sem, send_sem, recv_sems, sum_send, sum_recv,
):
    total_devices = sizes[0] * sizes[1] * sizes[2]
    rings = 1 if sizes[2] == 2 else 2
    riders, tile_of, tiles, inner, halos, counts = plan(deep, rings)
    me = [lax.axis_index(name) for name in AXES]
    my_id = (me[0] * sizes[1] + me[1]) * sizes[2] + me[2]
    scope = jax.named_scope
    up = jnp.where(2 * me[1] < sizes[1], 1, 0)
    side_is_up = (None, up, 1 - up)
    side_sign = (None, 2 * up - 1, 1 - 2 * up)

    def device_at(linear):
        return (
            linear // (sizes[1] * sizes[2]),
            linear // sizes[2] % sizes[1],
            linear % sizes[2],
        )

    def neighbour(cx, cy, cz):
        return tuple(
            lax.rem(place + step + size, size)
            for place, step, size in zip(me, (cx, cy, cz), sizes)
        )

    with scope("signal"):
        barrier = pltpu.get_barrier_semaphore()
        if max(sizes) <= 5:
            steps = [(1, -1, 0) if size > 2 else (1, 0) for size in sizes]
            greeted = [
                neighbour(cx, cy, cz)
                for cx in steps[0] for cy in steps[1] for cz in steps[2]
                if (cx, cy, cz) != (0, 0, 0)
            ]
        else:
            greeted = [
                device_at(lax.rem(my_id + step, total_devices)) for step in range(1, total_devices)
            ]
        for target in greeted:
            pl.semaphore_signal(barrier, inc=1, device_id=target, device_id_type=MESH)
        coords_ref = lines.at[pl.ds(0, 3 * deep)]
        polar_ref = lines.at[pl.ds(3 * deep, deep)]
        field_ref = lines.at[pl.ds(4 * deep, 6 * deep)]
        for src, dst, sem in (
            (coords_hbm, coords_ref, load_sem),
            (polar_hbm, polar_ref, load_sem),
            (field_hbm, field_ref, load_sem),
            (pairs_hbm, pairs_ref, send_sem),
            (count_hbm, count_ref, sum_send),
        ):
            pltpu.make_async_copy(src, dst, sem).start()

    lane = lax.broadcasted_iota(jnp.int32, (8, 128), 1)
    row = lax.broadcasted_iota(jnp.int32, (8, 128), 0)
    group = lane // GROUP
    place_y = lane // SIDE % SIDE
    place_x = lane % SIDE
    site = lane % GROUP
    shift_x = group - REACH
    unpack = GROUP * row + site
    far_x = spacing * shift_x.astype(jnp.float32)

    def within(first, size):
        return jnp.logical_and(lane >= first, lane < first + size)

    def choose(cases, default):
        for condition, value in cases:
            default = jnp.where(condition, value, default)
        return default

    def edge_index(bases, at, first_x):
        cases = []
        for base, start in zip(bases, at):
            local = lane - base
            value = start + SIDE * (local // 3) + local % 3 + first_x
            cases.append((within(base, EDGE), value))
        return choose(cases, jnp.zeros_like(lane))

    all_parts = [GROUP * part for part in range(6)]
    take_low = edge_index(LOW[0] + LOW[1], all_parts, 1)
    take_high = edge_index(HIGH[0] + HIGH[1], all_parts, 0)
    ride_low = [
        edge_index([RIDE_LOW + EDGE * part for part in range(3)], all_parts[3 * s : 3 * s + 3], 1)
        for s in range(2)
    ]
    ride_high = [
        edge_index([RIDE_HIGH + EDGE * part for part in range(3)], all_parts[3 * s : 3 * s + 3], 0)
        for s in range(2)
    ]

    def unride(regions, starts):
        cases = []
        for bases, start in zip(regions, starts):
            for part, base in enumerate(bases):
                cases.append((within(base, EDGE), lane - base + start + EDGE * part))
        return choose(cases, jnp.zeros_like(lane))

    leave_low = unride(LOW, (RIDE_LOW, RIDE_LOW))
    leave_high = unride(HIGH, (RIDE_HIGH, RIDE_HIGH))
    part_low = unride(LOW, WIDE_LOW)
    part_high = unride(HIGH, WIDE_HIGH)
    wide_low, wide_high = (
        edge_index([at + EDGE * part for at in starts for part in range(3)], all_parts, first_x)
        for starts, first_x in ((WIDE_LOW, 1), (WIDE_HIGH, 0))
    )
    has_ninth = jnp.logical_or(row == 1, row == 7)
    flag = jnp.where(has_ninth, 8, jnp.maximum(lane - WIDE_FLAGS, 0))
    flag_lane = OWN[1] + GROUP * (FLAGS - 3) + SIDE * (flag // 3) + 1 + flag % 3
    take_wide_low = jnp.where(lane >= WIDE_FLAGS, flag_lane, take_low)

    def inside(bases, size):
        result = within(bases[0], size)
        for base in bases[1:]:
            result = jnp.logical_or(result, within(base, size))
        return result

    is_own = [within(OWN[s], 3 * GROUP) for s in range(2)]
    is_low = [inside(LOW[s], EDGE) for s in range(2)]

    reached = place_x + shift_x
    turn_x = []
    for part in range(6):
        s, c = part // 3, part % 3
        low = LOW[s][c] + 3 * place_y + reached + SIDE - 1
        high = HIGH[s][c] + 3 * place_y + jnp.minimum(reached - SIDE, 2)
        own = OWN[s] + GROUP * c + SIDE * place_y + reached
        turn_x.append(jnp.where(reached < 0, low, jnp.where(reached < SIDE, own, high)))

    def packed(parts):
        value = parts[0]
        for index in range(1, len(parts)):
            value = jnp.where(group == index, parts[index], value)
        return value

    def rows_of(line):
        return gather(jnp.broadcast_to(line, (8, 128)), unpack)

    MIDDLE = 0
    SENT = {0: 0, 1: deep + 1, -1: deep + 2 + tiles}
    HALO = {0: deep, 1: deep + 1 + tiles, -1: deep + 2 + 2 * tiles}

    sent_tiles = deep + 2 * tiles + 3
    held_tiles = counts[0] + 2 * counts[1]

    def sent_rows(phase, tile, amount=8):
        return pl.ds(8 * (phase * sent_tiles + tile), amount)

    def held_rows(phase, tile, amount=8):
        return pl.ds(pl.multiple_of(8 * (phase * held_tiles + tile), 8), amount)

    def put_tile(phase, tile, value):
        send[sent_rows(phase, tile), :] = value

    def ends(bottom, top):
        return jnp.where(row < REACH, bottom, pltpu.roll(top, REST, 0))

    def put_first(geometry, vector):
        for phase, blocks in ((0, geometry), (1, vector)):
            put_middle(phase, blocks)
        for place, take, part, is_part in (
            (0, take_wide_low, wide_low, inside((0, 84), 3 * EDGE)),
            (deep + 1, take_high, wide_high, within(12, 6 * EDGE)),
        ):
            cut = [
                jnp.where(is_part, gather(vector[k], part), gather(geometry[k], take))
                for k in range(deep)
            ]
            for index, value in enumerate(cut + [ends(cut[0], cut[-1])]):
                send_wide[pl.ds(8 * (place + index), 8), :] = value

    def put_middle(phase, blocks):
        for k in range(deep):
            put_tile(phase, MIDDLE + k, blocks[k])
        put_tile(phase, HALO[0], ends(blocks[0], blocks[deep - 1]))

    def put(phase, blocks):
        last = deep - 1
        put_middle(phase, blocks)
        for direction, take, ride, ride_at in (
            (1, take_low, ride_low, RIDE_LOW),
            (-1, take_high, ride_high, RIDE_HIGH),
        ):
            cut = {k: gather(blocks[k], take) for k in range(deep) if k not in riders or k == last}
            put_tile(phase, HALO[direction], ends(cut[0], cut[last]))
            for rider in riders:
                for s in range(2):
                    host = rider - 2 + s
                    cut[host] = jnp.where(
                        within(ride_at, 3 * EDGE), gather(blocks[rider], ride[s]), cut[host]
                    )
            for k in tile_of:
                put_tile(phase, SENT[direction] + tile_of[k], cut[k])

    def exchange(*phases):
        def start(phase, src, at, stage, rows, target):
            place = counts[0] + counts[1] * (1 - side_is_up[stage]) if stage else 0
            pltpu.make_async_remote_copy(
                src_ref=send.at[sent_rows(phase, src, rows)],
                dst_ref=held.at[held_rows(phase, place + at, rows)],
                send_sem=send_sem,
                recv_sem=recv_sems.at[phase, 1 - side_sign[stage] if stage else 1],
                device_id=target,
                device_id_type=MESH,
            ).start()

        for phase in phases:
            for stage, cx in ORDER:
                cy = side_sign[stage] if stage else 0
                far = 1 if stage else 0
                if stage or cx:
                    rows = 8 * (tiles if cx else deep)
                    start(phase, SENT[cx], inner[-cx, far], stage, rows, neighbour(cx, cy, 0))
                for ring in range(rings):
                    at = halos[-cx, far] + ring
                    target = neighbour(cx, cy, -1 if ring == 0 else 1)
                    start(phase, HALO[cx], at, stage, REST, target)

    wide_count = 2 * (deep + rings)

    def first_wide(stage):
        return wide_count * (1 + side_is_up[stage]) if stage else 0

    def wide_place(cx, ring=None):
        right = 1 if cx > 0 else 0
        return right * deep if ring is None else 2 * deep + right * rings + ring

    def wide_rows(stage, place, amount=8):
        return pl.ds(pl.multiple_of(8 * (first_wide(stage) + place), 8), amount)

    def exchange_first():
        def start(phase, src, dst, stage, target):
            pltpu.make_async_remote_copy(
                src_ref=src,
                dst_ref=dst,
                send_sem=send_sem,
                recv_sem=recv_sems.at[phase, 1 - side_sign[stage] if stage else 1],
                device_id=target,
                device_id_type=MESH,
            ).start()

        for phase in range(2):
            for stage, cx in ORDER:
                cy = side_sign[stage] if stage else 0
                far = 1 if stage else 0
                opposite = 3 - stage if stage else 0
                rows = 8 * deep
                if cx and phase == 0:
                    place = 0 if cx > 0 else deep + 1
                    start(
                        0,
                        send_wide.at[pl.ds(8 * place, rows)],
                        held_wide.at[wide_rows(opposite, wide_place(-cx), rows)],
                        stage,
                        neighbour(cx, cy, 0),
                    )
                    for ring in range(rings):
                        start(
                            0,
                            send_wide.at[pl.ds(8 * (place + deep), REST)],
                            held_wide.at[wide_rows(opposite, wide_place(-cx, ring), REST)],
                            stage,
                            neighbour(cx, cy, -1 if ring == 0 else 1),
                        )
                if not cx:
                    first = first_tile(opposite)
                    if stage:
                        start(
                            phase,
                            send.at[sent_rows(phase, SENT[0], rows)],
                            held.at[held_rows(phase, first + inner[0, far], rows)],
                            stage,
                            neighbour(0, cy, 0),
                        )
                    for ring in range(rings):
                        start(
                            phase,
                            send.at[sent_rows(phase, HALO[0], REST)],
                            held.at[held_rows(phase, first + halos[0, far] + ring, REST)],
                            stage,
                            neighbour(0, cy, -1 if ring == 0 else 1),
                        )

    def first_tile(stage):
        return counts[0] + counts[1] * side_is_up[stage] if stage else 0

    rows_in = []
    for phase in range(4):
        if phase < 2:
            sides = 2 * (8 * deep + REST * rings) if phase == 0 else 0
            rows_in.append([sides + REST * rings, sides + REST * rings + 8 * deep])
        else:
            rows_in.append([8 * counts[far] - (8 - REST) * 3 * rings for far in (0, 1)])

    def arrival(phase, stage):
        start = first_tile(stage) if phase > 1 else 0
        rows = held.at[held_rows(phase, start, rows_in[phase][1 if stage else 0])]
        which = 1 + side_sign[stage] if stage else 1
        pltpu.make_async_copy(rows, rows, recv_sems.at[phase, which]).wait()

    def joined(below, above):
        return jnp.where(row < 4, below, pltpu.roll(above, 8 - REST, 0))

    def wide_tile(stage, cx, v):
        if v:
            return held_wide[wide_rows(stage, wide_place(cx) + v - 1), :]
        return joined(
            held_wide[wide_rows(stage, wide_place(cx, 0)), :],
            held_wide[wide_rows(stage, wide_place(cx, rings - 1)), :],
        )

    def merged_tiles(phase, stage):
        first = first_tile(stage)
        far = 1 if stage else 0

        def halo(cx):
            at = first + halos[cx, far]
            return joined(
                held[held_rows(phase, at), :], held[held_rows(phase, at + rings - 1), :]
            )

        def tile(cx, number):
            return held[held_rows(phase, first + inner[cx, far] + number), :]

        wide = []
        for v in range(deep + 1) if phase < 2 else []:
            low, high = wide_tile(stage, -1, v), wide_tile(stage, 1, v)
            if phase == 1:
                low, high = gather(low, part_low), gather(high, part_high)
            wide.append((low, high))
        both = []
        for s in range(2):
            row_of_tiles = []
            for v in range(deep + 1):
                k = v - 1
                if wide:
                    low, high = wide[v]
                    if v == 0:
                        own = halo(0)
                    else:
                        own = tile(0, k) if stage else send[sent_rows(phase, MIDDLE + k), :]
                elif v == 0:
                    low, own, high = halo(-1), halo(0), halo(1)
                else:
                    own = tile(0, k) if stage else send[sent_rows(phase, MIDDLE + k), :]
                    if k in riders:
                        host = tile_of[k - 2 + s]
                        low = gather(tile(-1, host), leave_low)
                        high = gather(tile(1, host), leave_high)
                    else:
                        low, high = tile(-1, tile_of[k]), tile(1, tile_of[k])
                row_of_tiles.append(jnp.where(is_own[s], own, jnp.where(is_low[s], low, high)))
            both.append(row_of_tiles)
        return both

    def page_of(stage, j):
        return REACH * (stage - 1) + j if stage else 0

    depth_y = [None] + [
        jnp.where(side_is_up[stage] > 0, place_y, SIDE - 1 - place_y) for stage in (1, 2)
    ]

    def spread_out(tiles_in, out, parts, stage):
        for v in range(deep + 1):
            for part in range(parts):
                value = gather(tiles_in[part // 3][v], turn_x[part])
                pages = {0: value}
                if stage:
                    base = out[0, part, pl.ds(8 * v, 8), :]
                    pages = {
                        page_of(stage, j): jnp.where(depth_y[stage] < j, value, base)
                        for j in range(1, REACH + 1)
                    }
                for page, value in pages.items():
                    out[page, part, pl.ds(8 * v, 8), :] = value
                    if v == 0:
                        out[page, part, pl.ds(8 * (deep + 1), 8), :] = value

    def contract(sums, parts, vec):
        dx, dy, dz, tx, ty, tz, three = parts
        for first in (0, 3):
            vx, vy, vz = vec[first : first + 3]
            along = tx * vx + ty * vy + tz * vz
            for part, (d, v) in enumerate(((dx, vx), (dy, vy), (dz, vz))):
                term = d * along - three * v
                at = first + part
                sums[at] = term if sums[at] is None else sums[at] + term

    def tile_number(k, page, sz):
        return (k * PAGES + page) * SPAN + sz + REACH

    def build_tile(k, page, sz):
        start = 8 + sz
        span = pl.ds(8 * k + start, 8)
        dx = near_geo[page, 0, span, :] - own_ref[page, k, 0]
        dy = near_geo[page, 1, span, :] - own_ref[page, k, 1]
        dz = near_geo[page, 2, span, :] - (own_ref[page, k, 2] - spacing * sz)
        weight = switch[k, page, pl.ds(start, 8), :]
        if page == 0 and sz == 0:
            weight = jnp.where(group == REACH, 0.0, weight)
        square = dx * dx + dy * dy + dz * dz
        if page == 0 and sz == 0:
            square = jnp.maximum(square, 1.0)
        inverse = lax.rsqrt(square)
        inverse_square = inverse * inverse
        damp = square * (square * inverse) * (near_geo[page, 3, span, :] * own_ref[page, k, 3])
        damping = jnp.exp2(damp * (-1.0 / math.log(2.0)))
        fade = jnp.maximum(cutoff_square - square, 0.0)
        scale = fade * fade * (inverse_square * inverse) * weight
        three = scale - scale * damping
        five = (three - scale * (damp * damping)) * (3.0 * inverse_square)
        parts = (dx, dy, dz, five * dx, five * dy, five * dz, three)
        for part, value in enumerate(parts):
            tensor[tile_number(k, page, sz), part] = value
        return parts

    def load_tile(k, page, sz):
        return [tensor[tile_number(k, page, sz), part] for part in range(7)]

    def back_roll(stage, j):
        return lax.rem(128 - SIDE * side_sign[stage] * j, 128) if stage else 0

    def gather_groups(sums, stage, j, total):
        back = back_roll(stage, j)
        ends_in = (lane + back) // GROUP % 8
        first, second = total
        for step in range(4):
            comes = (ends_in + step) % 4
            quad = sums[3]
            for part in range(3):
                quad = jnp.where(comes == part, sums[part], quad)
            pair = jnp.where(comes % 2 == 0, sums[4], sums[5])
            shift = back + GROUP * step
            if stage:
                shift = lax.rem(shift, 128)
            if stage or step:
                quad, pair = pltpu.roll(quad, shift, 1), pltpu.roll(pair, shift, 1)
            first = quad if first is None else first + quad
            second = pair if second is None else second + pair
        return first, second

    upper = group >= 4

    def fold(total):
        kept = jnp.where(upper, total[1], total[0])
        moved = jnp.where(upper, total[0], total[1])
        return kept + pltpu.roll(moved, 64, 1)

    def used(stage):
        for j in range(1, REACH + 1) if stage else [0]:
            yield j, [sz for sz in SHIFTS if j < REACH or abs(sz) < REACH]

    def stage_tiles(stage, k):
        for j, shifts in used(stage):
            for sz in shifts:
                build_tile(k, page_of(stage, j), sz)

    def stage_sums(make_tile, stage, k):
        result = []
        for j, shifts in used(stage):
            sums = [None] * 6
            page = page_of(stage, j)
            for sz in shifts:
                span = pl.ds(8 * k + 8 + sz, 8)
                vec = [near[page, part, span, :] for part in range(6)]
                contract(sums, make_tile(k, page, sz), vec)
            result.append((sums, stage, j))
        return result

    def operate(phase, make_tile, vector, prepare=None):
        totals = [(None, None)] * deep
        waiting = [[] for _ in range(deep)]
        image = []
        for stage in range(3):
            if prepare is not None:
                prepare(stage)
            if prepare is not None and stage == 2:
                with scope("tiles"):
                    for k in range(deep):
                        stage_tiles(stage, k)
                make_tile = load_tile
            with scope(f"arrive{phase}_{stage}"):
                arrival(phase, stage)
            with scope(f"stage{phase}_{stage}"):
                spread_out(merged_tiles(phase, stage), near, 6, stage)
                for k in range(deep):
                    for item in waiting[k]:
                        totals[k] = gather_groups(*item, totals[k])
                    waiting[k] = stage_sums(make_tile, stage, k)
                    if stage == 2:
                        for item in waiting[k]:
                            totals[k] = gather_groups(*item, totals[k])
                        image.append(vector[k] / polar[k] - mask[k] * fold(totals[k]))
        return image

    def build_switch(tiles_in, stage):
        def full(at):
            return jnp.broadcast_to(jnp.asarray(at, jnp.int32), (8, 128))

        own_lane = OWN[1] + GROUP * (FLAGS - 3)

        def same_rows(tile, low_row, high_row):
            return jnp.where(row < 4, tile[low_row : low_row + 1], tile[high_row : high_row + 1])

        cy = side_sign[stage] if stage else 0
        for cz in (-1, 0, 1):
            low_flag = 7 - 3 * (cy + 1) - cz
            ninth = low_flag == 8 if stage and cz == -1 else None
            low_at = low_flag if ninth is None else jnp.where(ninth, 0, low_flag)
            low_at = full(WIDE_FLAGS + low_at)
            high_at = full(own_lane + SIDE * (cy + 1) + cz + 2)
            middle_at = full(own_lane + SIDE * (2 + cy * cz) if stage else own_lane)
            ours = jnp.where(reached < SIDE, middle_at, high_at)
            ahead = cy > 0 if stage else cz > 0
            use_own = jnp.where(ahead, reached, reached - SIDE) >= 0
            for k in range(deep):
                v = (k + 1 + cz) % (deep + 1)
                tile = wide_tile(stage, -1, v)
                flags = same_rows(tile, 0, 6)
                if ninth is not None:
                    flags = jnp.where(ninth, same_rows(tile, 1, 7), flags)
                there = jnp.where(
                    reached < 0, gather(flags, low_at), gather(tiles_in[1][v], middle_at)
                )
                here = gather(send[sent_rows(0, MIDDLE + k), :], ours)
                value = jnp.where(use_own, here, there)
                if stage == 0 and cz == 0:
                    inside_own = jnp.logical_and(reached >= 0, reached < SIDE)
                    value = jnp.where(inside_own, 1.0 / cutoff_square**2, value)
                value = jnp.where(group < SPAN, value, 0.0)
                span = pl.ds(8 * (cz + 1), 8)
                if stage == 0:
                    switch[k, 0, span, :] = value
                for j in range(1, REACH + 1) if stage else []:
                    switch[k, page_of(stage, j), span, :] = jnp.where(
                        depth_y[stage] < j, value, switch[k, 0, span, :]
                    )

    everyone = []
    for far in list(range(1, sizes[1])) + [0]:
        y = lax.rem(me[1] + side_sign[2] * far + sizes[1], sizes[1])
        for cx in range(sizes[0]):
            x = lax.rem(me[0] + cx, sizes[0])
            for cz in range(sizes[2]):
                if far or cx or cz:
                    everyone.append((x, y, lax.rem(me[2] + cz, sizes[2])))

    in_set = [group < 3, jnp.logical_and(group >= 3, group < 6)]

    def put_sums(number, products):
        values = []
        for first, second in products:
            value = first[0] * second[0]
            for k in range(1, deep):
                value = value + first[k] * second[k]
            line = jnp.sum(value, axis=0, keepdims=True)
            for s in range(2):
                chosen = jnp.where(in_set[s][0:1], line, 0.0)
                values.append(jnp.sum(chosen, axis=1, keepdims=True))
        line = jnp.broadcast_to(values[0], (1, 128))
        for index in range(1, len(values)):
            line = jnp.where(group[0:1] == index, values[index], line)
        sums_out[number] = line
        sums_in[number, my_id] = line

    def send_sums(number):
        for target in everyone:
            pltpu.make_async_remote_copy(
                src_ref=sums_out.at[number],
                dst_ref=sums_in.at[number, my_id],
                send_sem=sum_send,
                recv_sem=sum_recv.at[number],
                device_id=target,
                device_id_type=MESH,
            ).start()

    def end_sums(number):
        rows = sums_in.at[number, pl.ds(0, total_devices - 1)]
        pltpu.make_async_copy(rows, rows, sum_recv.at[number]).wait()
        lines = [sums_in[number, index] for index in range(total_devices)]
        while len(lines) > 1:
            lines = [
                lines[index] + lines[index + 1] if index + 1 < len(lines) else lines[index]
                for index in range(0, len(lines), 2)
            ]
        return jnp.broadcast_to(lines[0], (8, 128))

    def total_by(first_set, line, index):
        return gather(line, jnp.where(first_set, GROUP * 2 * index, GROUP * (2 * index + 1)))

    def as_rows(value):
        result = value
        for step in range(1, 8):
            moved = pltpu.roll(pltpu.roll(value, 8 - step, 0), GROUP * step, 1)
            result = jnp.where((group - row) % 8 == step, moved, result)
        return result

    def each(function, *vectors):
        return [function(k, *(vector[k] for vector in vectors)) for k in range(deep)]

    with scope("setup"):
        pltpu.make_async_copy(lines, lines, load_sem).wait()
        pltpu.make_async_copy(pairs_hbm, pairs_ref, send_sem).wait()
        pltpu.make_async_copy(count_hbm, count_ref, sum_send).wait()
        site_x = spacing * (place_x.astype(jnp.float32) + 0.5)
        site_y = spacing * (place_y.astype(jnp.float32) + 0.5)
        site_z = spacing * (row.astype(jnp.float32) + 0.5)
        polar, mask, source, geometry = [], [], [], []
        for k in range(deep):
            places = [
                rows_of(coords_ref[3 * k + part]) - offset
                for part, offset in enumerate((site_x, site_y, site_z))
            ]
            polar_k = rows_of(polar_ref[k])
            mask_k = jnp.where(unpack < count_ref[k], 1.0, 0.0)
            root = lax.rsqrt(polar_k)
            slot = 14 + jnp.where(
                place_x == 0, place_y, 4 + 3 * place_y + place_x - 1
            )
            flag = pairs_ref[k, 0, 0] == slot
            for entry in range(1, 13):
                flag = jnp.logical_or(flag, pairs_ref[k, 0, entry] == slot)
            flags = jnp.where(flag, 1.0 / cutoff_square**2, 0.0)
            geometry.append(packed(places + [root, flags]))
            for stage in range(3):
                for j in range(1, REACH + 1) if stage else [0]:
                    for part, value in enumerate(places + [thole * root]):
                        if stage:
                            shift_y = side_sign[stage] * j
                            value = pltpu.roll(value, lax.rem(128 + SIDE * shift_y, 128), 1)
                            if part == 1:
                                value = value - spacing * shift_y.astype(jnp.float32)
                        own_ref[page_of(stage, j), k, part] = value - far_x if part == 0 else value
            polar.append(polar_k)
            mask.append(mask_k)
            field_k = packed([rows_of(field_ref[6 * k + part]) for part in range(6)])
            source.append(field_k * mask_k)
        dipoles = each(lambda k, s: polar[k] * s, source)
        put_first(geometry, each(lambda k, d: d * mask[k], dipoles))
    with scope("barrier"):
        pl.semaphore_wait(barrier, len(greeted))
    with scope("send0"):
        exchange_first()

    def prepare(stage):
        with scope(f"geoarrive_{stage}"):
            arrival(0, stage)
        with scope(f"geo_{stage}"):
            tiles_in = merged_tiles(0, stage)
            spread_out(tiles_in, near_geo, 4, stage)
            build_switch(tiles_in, stage)

    image = operate(1, build_tile, dipoles, prepare)
    with scope("finish0"):
        residual = each(lambda k, s, a: s - a, source, image)
        precond = each(lambda k, r: polar[k] * r, residual)
        put(2, each(lambda k, p: p * mask[k], precond))
    with scope("send1"):
        exchange(2)
    image = operate(2, load_tile, precond)
    with scope("finish1"):
        turned = each(lambda k, q: polar[k] * q, image)
        put(3, each(lambda k, t: t * mask[k], turned))
        put_sums(0, [(residual, precond), (precond, image)])
    with scope("send2"):
        exchange(3)
        send_sums(0)
    turned_image = operate(3, load_tile, turned)
    with scope("sum1wait"):
        first_total = end_sums(0)
        norm, curve = (total_by(group < 3, first_total, index) for index in range(2))
    with scope("mid"):
        gamma = norm / curve
        dipoles = each(lambda k, d, p: d + gamma * p, dipoles, precond)
        residual = each(lambda k, r, q: r - gamma * q, residual, image)
        second = each(lambda k, r: polar[k] * r, residual)
        second_image = each(lambda k, q, t: q - gamma * t, image, turned_image)
        put_sums(
            1,
            [
                (residual, second), (second, second_image), (second, image),
                (precond, second_image),
            ],
        )
        send_sums(1)
    with scope("turn"):
        dipoles, residual, precond, second, image, second_image = (
            each(lambda k, value: as_rows(value), vector)
            for vector in (dipoles, residual, precond, second, image, second_image)
        )
        norm, curve = (total_by(row < 3, first_total, index) for index in range(2))
    with scope("sum2wait"):
        last_total = end_sums(1)
    with scope("out"):
        norm_next, second_curve, cross, cross_back = (
            total_by(row < 3, last_total, index) for index in range(4)
        )
        ratio = norm_next / norm
        gamma = norm_next / (second_curve + ratio * (cross + cross_back + ratio * curve))
        for k in range(deep):
            direction = second[k] + ratio * precond[k]
            along = second_image[k] + ratio * image[k]
            for out, value in (
                (dip_out, dipoles[k] + gamma * direction),
                (res_out, residual[k] - gamma * along),
            ):
                for part in range(6):
                    out[6 * k + part] = value[part : part + 1]
    with scope("sendwait"):
        rows = held.at[pl.ds(0, sum(middle + 2 * side for middle, side in rows_in))]
        pltpu.make_async_copy(rows, rows, send_sem).wait()
        rows = sums_in.at[:, pl.ds(0, total_devices - 1)]
        pltpu.make_async_copy(rows, rows, sum_send).wait()


def store(dipoles, residual, dip_out, res_out, sems):
    copies = [
        pltpu.make_async_copy(dipoles, dip_out, sems.at[0]),
        pltpu.make_async_copy(residual, res_out, sems.at[1]),
    ]
    for copy in copies:
        copy.start()
    for copy in copies:
        copy.wait()


def on_device(sizes, coords, polar, field, atom_count, pair_list):
    deep, slots = coords.shape[2], coords.shape[-1]
    assert coords.shape[0:2] == (1, 1) and slots == 128
    vmem = pl.BlockSpec(memory_space=pltpu.VMEM)
    hbm = pl.BlockSpec(memory_space=pl.ANY)
    rows = 8 * deep
    devices = sizes[0] * sizes[1] * sizes[2]
    rings = 1 if sizes[2] == 2 else 2
    tiles, counts = (plan(deep, rings)[index] for index in (2, 5))

    def buffer(*shape):
        return pltpu.VMEM(shape, jnp.float32)

    line = pltpu.VMEM((6 * deep, 1, slots), jnp.float32)
    result = jax.ShapeDtypeStruct((6 * deep, 1, slots), jnp.float32)
    dma = pltpu.SemaphoreType.DMA
    dipoles, residual = pl.pallas_call(
        functools.partial(kernel, sizes, deep),
        out_shape=(line, line),
        in_specs=[hbm] * 5,
        out_specs=(vmem, vmem),
        scratch_shapes=[
            pltpu.SMEM((deep, 1, pair_list.shape[-1]), jnp.int32),
            pltpu.SMEM((deep,), jnp.int32),
            buffer(10 * deep, 1, slots),
            buffer(4 * 8 * (deep + 2 * tiles + 3), slots),
            buffer(4 * 8 * (counts[0] + 2 * counts[1]), slots),
            buffer(8 * 2 * (deep + 1), slots),
            buffer(8 * 3 * 2 * (deep + rings), slots),
            buffer(PAGES, 6, rows + 16, slots),
            buffer(PAGES, 4, rows + 16, slots),
            buffer(PAGES, deep, 4, 8, slots),
            buffer(deep, PAGES, 24, slots),
            buffer(PAGES * SPAN * deep, 7, 8, slots),
            buffer(2, 1, slots),
            buffer(2, devices, 1, slots),
            dma,
            dma,
            dma((4, 3)),
            dma,
            dma((2,)),
        ],
        compiler_params=pltpu.CompilerParams(collective_id=0, has_side_effects=True),
    )(
        pair_list.reshape(deep, 1, -1),
        atom_count.reshape(deep),
        coords.reshape(3 * deep, 1, slots),
        polar.reshape(deep, 1, slots),
        field.reshape(6 * deep, 1, slots),
    )
    dipoles, residual = pl.pallas_call(
        store,
        out_shape=(result, result),
        in_specs=[vmem, vmem],
        out_specs=(hbm, hbm),
        scratch_shapes=[dma((2,))],
    )(
        pltpu.with_memory_space_constraint(dipoles, pltpu.VMEM),
        pltpu.with_memory_space_constraint(residual, pltpu.VMEM),
    )
    return dipoles.reshape(field.shape), residual.reshape(field.shape)


def solution(mesh):
    sizes = tuple(mesh.shape[name] for name in AXES)
    block = P(*AXES, None, None)
    return jax.shard_map(
        functools.partial(on_device, sizes),
        mesh=mesh,
        in_specs=(block, P(*AXES, None), block, P(*AXES), P(*AXES, None)),
        out_specs=(block, block),
        check_vma=False,
    )
```

```python
import functools
import math

import jax
import jax.numpy as jnp
from jax import lax
from jax.experimental import pallas as pl
from jax.experimental.pallas import tpu as pltpu
from jax.sharding import PartitionSpec as P

MESH = pl.DeviceIdType.MESH
AXES = ("gx", "gy", "gz")
spacing = 2.2
cutoff_square = 49.0
thole = 0.39
SIDE = 4
GROUP = SIDE * SIDE
REACH = 3
SHIFTS = range(-REACH, REACH + 1)
PAGES = 1 + 2 * REACH
SPAN = 2 * REACH + 1
ORDER = [(2, -1), (2, 1), (1, -1), (1, 1), (2, 0), (0, -1), (0, 1), (1, 0), (0, 0)]
COLUMNS = [(cx, cy) for cx in (-1, 0, 1) for cy in (-1, 0, 1)]
REST = 6
EDGE = 12
OWN = (0, 48)
LOW = ((48, 60, 72), (36, 96, 108))
HIGH = ((84, 96, 108), (0, 12, 24))
RIDE_LOW = 0
RIDE_HIGH = 36
WIDE_LOW = (84, 0)
WIDE_HIGH = (48, 12)
WIDE_FLAGS = 120
FLAGS = 4


def gather(value, index):
    return jnp.take_along_axis(value, index, axis=1, mode="promise_in_bounds")


def plan(deep, rings):
    riders = [k for k in range(deep) if k % 3 == 2]
    tile_of, tiles = {}, 0
    for k in range(deep):
        if k not in riders:
            tile_of[k] = tiles
            tiles += 1
    inner, halos, counts = {}, {}, {}
    for cy in (0, 1):
        total = 0
        for cx in (-1, 0, 1):
            if (cx, cy) != (0, 0):
                inner[cx, cy] = total
                total += tiles if cx else deep
        for cx in (-1, 0, 1):
            halos[cx, cy] = total
            total += rings
        counts[cy] = total
    return riders, tile_of, tiles, inner, halos, counts


def kernel(
    sizes, deep, pairs_hbm, count_hbm, coords_hbm, polar_hbm, field_hbm, dip_out, res_out,
    pairs_ref, count_ref, lines, send, held, send_wide, held_wide, near, near_geo, own_ref,
    switch, tensor, sums_out, sums_in, load_sem, send_sem, recv_sems, sum_send, sum_recv,
):
    total_devices = sizes[0] * sizes[1] * sizes[2]
    rings = 1 if sizes[2] == 2 else 2
    riders, tile_of, tiles, inner, halos, counts = plan(deep, rings)
    me = [lax.axis_index(name) for name in AXES]
    my_id = (me[0] * sizes[1] + me[1]) * sizes[2] + me[2]
    scope = jax.named_scope
    up = jnp.where(2 * me[1] < sizes[1], 1, 0)
    side_is_up = (None, up, 1 - up)
    side_sign = (None, 2 * up - 1, 1 - 2 * up)

    def device_at(linear):
        return (
            linear // (sizes[1] * sizes[2]),
            linear // sizes[2] % sizes[1],
            linear % sizes[2],
        )

    def neighbour(cx, cy, cz):
        return tuple(
            lax.rem(place + step + size, size)
            for place, step, size in zip(me, (cx, cy, cz), sizes)
        )

    with scope("signal"):
        barrier = pltpu.get_barrier_semaphore()
        if max(sizes) <= 5:
            steps = [(1, -1, 0) if size > 2 else (1, 0) for size in sizes]
            greeted = [
                neighbour(cx, cy, cz)
                for cx in steps[0] for cy in steps[1] for cz in steps[2]
                if (cx, cy, cz) != (0, 0, 0)
            ]
        else:
            greeted = [
                device_at(lax.rem(my_id + step, total_devices)) for step in range(1, total_devices)
            ]
        for target in greeted:
            pl.semaphore_signal(barrier, inc=1, device_id=target, device_id_type=MESH)
        coords_ref = lines.at[pl.ds(0, 3 * deep)]
        polar_ref = lines.at[pl.ds(3 * deep, deep)]
        field_ref = lines.at[pl.ds(4 * deep, 6 * deep)]
        for src, dst, sem in (
            (coords_hbm, coords_ref, load_sem),
            (polar_hbm, polar_ref, load_sem),
            (field_hbm, field_ref, load_sem),
            (pairs_hbm, pairs_ref, send_sem),
            (count_hbm, count_ref, sum_send),
        ):
            pltpu.make_async_copy(src, dst, sem).start()

    lane = lax.broadcasted_iota(jnp.int32, (8, 128), 1)
    row = lax.broadcasted_iota(jnp.int32, (8, 128), 0)
    group = lane // GROUP
    place_y = lane // SIDE % SIDE
    place_x = lane % SIDE
    site = lane % GROUP
    shift_x = group - REACH
    unpack = GROUP * row + site
    far_x = spacing * shift_x.astype(jnp.float32)

    def within(first, size):
        return jnp.logical_and(lane >= first, lane < first + size)

    def choose(cases, default):
        for condition, value in cases:
            default = jnp.where(condition, value, default)
        return default

    def edge_index(bases, at, first_x):
        cases = []
        for base, start in zip(bases, at):
            local = lane - base
            value = start + SIDE * (local // 3) + local % 3 + first_x
            cases.append((within(base, EDGE), value))
        return choose(cases, jnp.zeros_like(lane))

    all_parts = [GROUP * part for part in range(6)]
    take_low = edge_index(LOW[0] + LOW[1], all_parts, 1)
    take_high = edge_index(HIGH[0] + HIGH[1], all_parts, 0)
    ride_low = [
        edge_index([RIDE_LOW + EDGE * part for part in range(3)], all_parts[3 * s : 3 * s + 3], 1)
        for s in range(2)
    ]
    ride_high = [
        edge_index([RIDE_HIGH + EDGE * part for part in range(3)], all_parts[3 * s : 3 * s + 3], 0)
        for s in range(2)
    ]

    def unride(regions, starts):
        cases = []
        for bases, start in zip(regions, starts):
            for part, base in enumerate(bases):
                cases.append((within(base, EDGE), lane - base + start + EDGE * part))
        return choose(cases, jnp.zeros_like(lane))

    leave_low = unride(LOW, (RIDE_LOW, RIDE_LOW))
    leave_high = unride(HIGH, (RIDE_HIGH, RIDE_HIGH))
    part_low = unride(LOW, WIDE_LOW)
    part_high = unride(HIGH, WIDE_HIGH)
    wide_low, wide_high = (
        edge_index([at + EDGE * part for at in starts for part in range(3)], all_parts, first_x)
        for starts, first_x in ((WIDE_LOW, 1), (WIDE_HIGH, 0))
    )
    has_ninth = jnp.logical_or(row == 1, row == 7)
    flag = jnp.where(has_ninth, 8, jnp.maximum(lane - WIDE_FLAGS, 0))
    flag_lane = OWN[1] + GROUP * (FLAGS - 3) + SIDE * (flag // 3) + 1 + flag % 3
    take_wide_low = jnp.where(lane >= WIDE_FLAGS, flag_lane, take_low)

    def inside(bases, size):
        result = within(bases[0], size)
        for base in bases[1:]:
            result = jnp.logical_or(result, within(base, size))
        return result

    is_own = [within(OWN[s], 3 * GROUP) for s in range(2)]
    is_low = [inside(LOW[s], EDGE) for s in range(2)]

    reached = place_x + shift_x
    turn_x = []
    for part in range(6):
        s, c = part // 3, part % 3
        low = LOW[s][c] + 3 * place_y + reached + SIDE - 1
        high = HIGH[s][c] + 3 * place_y + jnp.minimum(reached - SIDE, 2)
        own = OWN[s] + GROUP * c + SIDE * place_y + reached
        turn_x.append(jnp.where(reached < 0, low, jnp.where(reached < SIDE, own, high)))

    def packed(parts):
        value = parts[0]
        for index in range(1, len(parts)):
            value = jnp.where(group == index, parts[index], value)
        return value

    def rows_of(line):
        return gather(jnp.broadcast_to(line, (8, 128)), unpack)

    MIDDLE = 0
    SENT = {0: 0, 1: deep + 1, -1: deep + 2 + tiles}
    HALO = {0: deep, 1: deep + 1 + tiles, -1: deep + 2 + 2 * tiles}

    sent_tiles = deep + 2 * tiles + 3
    held_tiles = counts[0] + 2 * counts[1]

    def sent_rows(phase, tile, amount=8):
        return pl.ds(8 * (phase * sent_tiles + tile), amount)

    def held_rows(phase, tile, amount=8):
        return pl.ds(pl.multiple_of(8 * (phase * held_tiles + tile), 8), amount)

    def put_tile(phase, tile, value):
        send[sent_rows(phase, tile), :] = value

    def ends(bottom, top):
        return jnp.where(row < REACH, bottom, pltpu.roll(top, REST, 0))

    def put_first(geometry, vector):
        for phase, blocks in ((0, geometry), (1, vector)):
            put_middle(phase, blocks)
        for place, take, part, is_part in (
            (0, take_wide_low, wide_low, inside((0, 84), 3 * EDGE)),
            (deep + 1, take_high, wide_high, within(12, 6 * EDGE)),
        ):
            cut = [
                jnp.where(is_part, gather(vector[k], part), gather(geometry[k], take))
                for k in range(deep)
            ]
            for index, value in enumerate(cut + [ends(cut[0], cut[-1])]):
                send_wide[pl.ds(8 * (place + index), 8), :] = value

    def put_middle(phase, blocks):
        for k in range(deep):
            put_tile(phase, MIDDLE + k, blocks[k])
        put_tile(phase, HALO[0], ends(blocks[0], blocks[deep - 1]))

    def put(phase, blocks):
        last = deep - 1
        put_middle(phase, blocks)
        for direction, take, ride, ride_at in (
            (1, take_low, ride_low, RIDE_LOW),
            (-1, take_high, ride_high, RIDE_HIGH),
        ):
            cut = {k: gather(blocks[k], take) for k in range(deep) if k not in riders or k == last}
            put_tile(phase, HALO[direction], ends(cut[0], cut[last]))
            for rider in riders:
                for s in range(2):
                    host = rider - 2 + s
                    cut[host] = jnp.where(
                        within(ride_at, 3 * EDGE), gather(blocks[rider], ride[s]), cut[host]
                    )
            for k in tile_of:
                put_tile(phase, SENT[direction] + tile_of[k], cut[k])

    def exchange(phase, between=None):
        def start(phase, src, at, stage, rows, target):
            place = counts[0] + counts[1] * (1 - side_is_up[stage]) if stage else 0
            pltpu.make_async_remote_copy(
                src_ref=send.at[sent_rows(phase, src, rows)],
                dst_ref=held.at[held_rows(phase, place + at, rows)],
                send_sem=send_sem,
                recv_sem=recv_sems.at[phase, 1 - side_sign[stage] if stage else 1],
                device_id=target,
                device_id_type=MESH,
            ).start()

        for index, (stage, cx) in enumerate(ORDER):
            if index == 2 and between is not None:
                between()
            cy = side_sign[stage] if stage else 0
            far = 1 if stage else 0
            if stage or cx:
                rows = 8 * (tiles if cx else deep)
                start(phase, SENT[cx], inner[-cx, far], stage, rows, neighbour(cx, cy, 0))
            for ring in range(rings):
                at = halos[-cx, far] + ring
                target = neighbour(cx, cy, -1 if ring == 0 else 1)
                start(phase, HALO[cx], at, stage, REST, target)

    wide_count = 2 * (deep + rings)

    def first_wide(stage):
        return wide_count * (1 + side_is_up[stage]) if stage else 0

    def wide_place(cx, ring=None):
        right = 1 if cx > 0 else 0
        return right * deep if ring is None else 2 * deep + right * rings + ring

    def wide_rows(stage, place, amount=8):
        return pl.ds(pl.multiple_of(8 * (first_wide(stage) + place), 8), amount)

    def exchange_first():
        def start(phase, src, dst, stage, target):
            pltpu.make_async_remote_copy(
                src_ref=src,
                dst_ref=dst,
                send_sem=send_sem,
                recv_sem=recv_sems.at[phase, 1 - side_sign[stage] if stage else 1],
                device_id=target,
                device_id_type=MESH,
            ).start()

        for phase in range(2):
            for stage, cx in ORDER:
                cy = side_sign[stage] if stage else 0
                far = 1 if stage else 0
                opposite = 3 - stage if stage else 0
                rows = 8 * deep
                if cx and phase == 0:
                    place = 0 if cx > 0 else deep + 1
                    start(
                        0,
                        send_wide.at[pl.ds(8 * place, rows)],
                        held_wide.at[wide_rows(opposite, wide_place(-cx), rows)],
                        stage,
                        neighbour(cx, cy, 0),
                    )
                    for ring in range(rings):
                        start(
                            0,
                            send_wide.at[pl.ds(8 * (place + deep), REST)],
                            held_wide.at[wide_rows(opposite, wide_place(-cx, ring), REST)],
                            stage,
                            neighbour(cx, cy, -1 if ring == 0 else 1),
                        )
                if not cx:
                    first = first_tile(opposite)
                    if stage:
                        start(
                            phase,
                            send.at[sent_rows(phase, SENT[0], rows)],
                            held.at[held_rows(phase, first + inner[0, far], rows)],
                            stage,
                            neighbour(0, cy, 0),
                        )
                    for ring in range(rings):
                        start(
                            phase,
                            send.at[sent_rows(phase, HALO[0], REST)],
                            held.at[held_rows(phase, first + halos[0, far] + ring, REST)],
                            stage,
                            neighbour(0, cy, -1 if ring == 0 else 1),
                        )

    def first_tile(stage):
        return counts[0] + counts[1] * side_is_up[stage] if stage else 0

    rows_in = []
    for phase in range(4):
        if phase < 2:
            sides = 2 * (8 * deep + REST * rings) if phase == 0 else 0
            rows_in.append([sides + REST * rings, sides + REST * rings + 8 * deep])
        else:
            rows_in.append([8 * counts[far] - (8 - REST) * 3 * rings for far in (0, 1)])

    def arrival(phase, stage):
        start = first_tile(stage) if phase > 1 else 0
        rows = held.at[held_rows(phase, start, rows_in[phase][1 if stage else 0])]
        which = 1 + side_sign[stage] if stage else 1
        pltpu.make_async_copy(rows, rows, recv_sems.at[phase, which]).wait()

    def joined(below, above):
        return jnp.where(row < 4, below, pltpu.roll(above, 8 - REST, 0))

    def wide_tile(stage, cx, v):
        if v:
            return held_wide[wide_rows(stage, wide_place(cx) + v - 1), :]
        return joined(
            held_wide[wide_rows(stage, wide_place(cx, 0)), :],
            held_wide[wide_rows(stage, wide_place(cx, rings - 1)), :],
        )

    def merged_tiles(phase, stage):
        first = first_tile(stage)
        far = 1 if stage else 0

        def halo(cx):
            at = first + halos[cx, far]
            return joined(
                held[held_rows(phase, at), :], held[held_rows(phase, at + rings - 1), :]
            )

        def tile(cx, number):
            return held[held_rows(phase, first + inner[cx, far] + number), :]

        wide = []
        for v in range(deep + 1) if phase < 2 else []:
            low, high = wide_tile(stage, -1, v), wide_tile(stage, 1, v)
            if phase == 1:
                low, high = gather(low, part_low), gather(high, part_high)
            wide.append((low, high))
        both = []
        for s in range(2):
            row_of_tiles = []
            for v in range(deep + 1):
                k = v - 1
                if wide:
                    low, high = wide[v]
                    if v == 0:
                        own = halo(0)
                    else:
                        own = tile(0, k) if stage else send[sent_rows(phase, MIDDLE + k), :]
                elif v == 0:
                    low, own, high = halo(-1), halo(0), halo(1)
                else:
                    own = tile(0, k) if stage else send[sent_rows(phase, MIDDLE + k), :]
                    if k in riders:
                        host = tile_of[k - 2 + s]
                        low = gather(tile(-1, host), leave_low)
                        high = gather(tile(1, host), leave_high)
                    else:
                        low, high = tile(-1, tile_of[k]), tile(1, tile_of[k])
                row_of_tiles.append(jnp.where(is_own[s], own, jnp.where(is_low[s], low, high)))
            both.append(row_of_tiles)
        return both

    def page_of(stage, j):
        return REACH * (stage - 1) + j if stage else 0

    depth_y = [None] + [
        jnp.where(side_is_up[stage] > 0, place_y, SIDE - 1 - place_y) for stage in (1, 2)
    ]

    def spread_out(tiles_in, out, parts, stage):
        for v in range(deep + 1):
            for part in range(parts):
                value = gather(tiles_in[part // 3][v], turn_x[part])
                pages = {0: value}
                if stage:
                    base = out[0, part, pl.ds(8 * v, 8), :]
                    pages = {
                        page_of(stage, j): jnp.where(depth_y[stage] < j, value, base)
                        for j in range(1, REACH + 1)
                    }
                for page, value in pages.items():
                    out[page, part, pl.ds(8 * v, 8), :] = value
                    if v == 0:
                        out[page, part, pl.ds(8 * (deep + 1), 8), :] = value

    def contract(sums, parts, vec):
        dx, dy, dz, tx, ty, tz, three = parts
        for first in (0, 3):
            vx, vy, vz = vec[first : first + 3]
            along = tx * vx + ty * vy + tz * vz
            for part, (d, v) in enumerate(((dx, vx), (dy, vy), (dz, vz))):
                term = d * along - three * v
                at = first + part
                sums[at] = term if sums[at] is None else sums[at] + term

    def tile_number(k, page, sz):
        return (k * PAGES + page) * SPAN + sz + REACH

    def build_tile(k, page, sz):
        start = 8 + sz
        span = pl.ds(8 * k + start, 8)
        dx = near_geo[page, 0, span, :] - own_ref[page, k, 0]
        dy = near_geo[page, 1, span, :] - own_ref[page, k, 1]
        dz = near_geo[page, 2, span, :] - (own_ref[page, k, 2] - spacing * sz)
        weight = switch[k, page, pl.ds(start, 8), :]
        if page == 0 and sz == 0:
            weight = jnp.where(group == REACH, 0.0, weight)
        square = dx * dx + dy * dy + dz * dz
        if page == 0 and sz == 0:
            square = jnp.maximum(square, 1.0)
        inverse = lax.rsqrt(square)
        inverse_square = inverse * inverse
        damp = square * (square * inverse) * (near_geo[page, 3, span, :] * own_ref[page, k, 3])
        damping = jnp.exp2(damp * (-1.0 / math.log(2.0)))
        fade = jnp.maximum(cutoff_square - square, 0.0)
        scale = fade * fade * (inverse_square * inverse) * weight
        three = scale - scale * damping
        five = (three - scale * (damp * damping)) * (3.0 * inverse_square)
        parts = (dx, dy, dz, five * dx, five * dy, five * dz, three)
        for part, value in enumerate(parts):
            tensor[tile_number(k, page, sz), part] = value
        return parts

    def load_tile(k, page, sz):
        return [tensor[tile_number(k, page, sz), part] for part in range(7)]

    def back_roll(stage, j):
        return lax.rem(128 - SIDE * side_sign[stage] * j, 128) if stage else 0

    def gather_groups(sums, stage, j, total):
        back = back_roll(stage, j)
        ends_in = (lane + back) // GROUP % 8
        first, second = total
        for step in range(4):
            comes = (ends_in + step) % 4
            quad = sums[3]
            for part in range(3):
                quad = jnp.where(comes == part, sums[part], quad)
            pair = jnp.where(comes % 2 == 0, sums[4], sums[5])
            shift = back + GROUP * step
            if stage:
                shift = lax.rem(shift, 128)
            if stage or step:
                quad, pair = pltpu.roll(quad, shift, 1), pltpu.roll(pair, shift, 1)
            first = quad if first is None else first + quad
            second = pair if second is None else second + pair
        return first, second

    upper = group >= 4

    def fold(total):
        kept = jnp.where(upper, total[1], total[0])
        moved = jnp.where(upper, total[0], total[1])
        return kept + pltpu.roll(moved, 64, 1)

    def used(stage):
        for j in range(1, REACH + 1) if stage else [0]:
            yield j, [sz for sz in SHIFTS if j < REACH or abs(sz) < REACH]

    def stage_tiles(stage, k):
        for j, shifts in used(stage):
            for sz in shifts:
                build_tile(k, page_of(stage, j), sz)

    def stage_sums(make_tile, stage, k):
        result = []
        for j, shifts in used(stage):
            sums = [None] * 6
            page = page_of(stage, j)
            for sz in shifts:
                span = pl.ds(8 * k + 8 + sz, 8)
                vec = [near[page, part, span, :] for part in range(6)]
                contract(sums, make_tile(k, page, sz), vec)
            result.append((sums, stage, j))
        return result

    def operate(phase, make_tile, vector, prepare=None):
        totals = [(None, None)] * deep
        waiting = [[] for _ in range(deep)]
        image = []
        for stage in range(3):
            if prepare is not None:
                prepare(stage)
            if prepare is not None and stage == 2:
                with scope("tiles"):
                    for k in range(deep):
                        stage_tiles(stage, k)
                make_tile = load_tile
            with scope(f"arrive{phase}_{stage}"):
                arrival(phase, stage)
            with scope(f"stage{phase}_{stage}"):
                spread_out(merged_tiles(phase, stage), near, 6, stage)
                for k in range(deep):
                    for item in waiting[k]:
                        totals[k] = gather_groups(*item, totals[k])
                    waiting[k] = stage_sums(make_tile, stage, k)
                    if stage == 2:
                        for item in waiting[k]:
                            totals[k] = gather_groups(*item, totals[k])
                        image.append(vector[k] / polar[k] - mask[k] * fold(totals[k]))
        return image

    def build_switch(tiles_in, stage):
        def full(at):
            return jnp.broadcast_to(jnp.asarray(at, jnp.int32), (8, 128))

        own_lane = OWN[1] + GROUP * (FLAGS - 3)

        def same_rows(tile, low_row, high_row):
            return jnp.where(row < 4, tile[low_row : low_row + 1], tile[high_row : high_row + 1])

        cy = side_sign[stage] if stage else 0
        for cz in (-1, 0, 1):
            low_flag = 7 - 3 * (cy + 1) - cz
            ninth = low_flag == 8 if stage and cz == -1 else None
            low_at = low_flag if ninth is None else jnp.where(ninth, 0, low_flag)
            low_at = full(WIDE_FLAGS + low_at)
            high_at = full(own_lane + SIDE * (cy + 1) + cz + 2)
            middle_at = full(own_lane + SIDE * (2 + cy * cz) if stage else own_lane)
            ours = jnp.where(reached < SIDE, middle_at, high_at)
            ahead = cy > 0 if stage else cz > 0
            use_own = jnp.where(ahead, reached, reached - SIDE) >= 0
            for k in range(deep):
                v = (k + 1 + cz) % (deep + 1)
                tile = wide_tile(stage, -1, v)
                flags = same_rows(tile, 0, 6)
                if ninth is not None:
                    flags = jnp.where(ninth, same_rows(tile, 1, 7), flags)
                there = jnp.where(
                    reached < 0, gather(flags, low_at), gather(tiles_in[1][v], middle_at)
                )
                here = gather(send[sent_rows(0, MIDDLE + k), :], ours)
                value = jnp.where(use_own, here, there)
                if stage == 0 and cz == 0:
                    inside_own = jnp.logical_and(reached >= 0, reached < SIDE)
                    value = jnp.where(inside_own, 1.0 / cutoff_square**2, value)
                value = jnp.where(group < SPAN, value, 0.0)
                span = pl.ds(8 * (cz + 1), 8)
                if stage == 0:
                    switch[k, 0, span, :] = value
                for j in range(1, REACH + 1) if stage else []:
                    switch[k, page_of(stage, j), span, :] = jnp.where(
                        depth_y[stage] < j, value, switch[k, 0, span, :]
                    )

    everyone = []
    for far in list(range(1, sizes[1])) + [0]:
        y = lax.rem(me[1] + side_sign[2] * far + sizes[1], sizes[1])
        for cx in range(sizes[0]):
            x = lax.rem(me[0] + cx, sizes[0])
            for cz in range(sizes[2]):
                if far or cx or cz:
                    everyone.append((x, y, lax.rem(me[2] + cz, sizes[2])))

    in_set = [group < 3, jnp.logical_and(group >= 3, group < 6)]

    def put_sums(number, products):
        values = []
        for first, second in products:
            value = first[0] * second[0]
            for k in range(1, deep):
                value = value + first[k] * second[k]
            line = jnp.sum(value, axis=0, keepdims=True)
            for s in range(2):
                chosen = jnp.where(in_set[s][0:1], line, 0.0)
                values.append(jnp.sum(chosen, axis=1, keepdims=True))
        line = jnp.broadcast_to(values[0], (1, 128))
        for index in range(1, len(values)):
            line = jnp.where(group[0:1] == index, values[index], line)
        sums_out[number] = line
        sums_in[number, my_id] = line

    def send_sums(number):
        for target in everyone:
            pltpu.make_async_remote_copy(
                src_ref=sums_out.at[number],
                dst_ref=sums_in.at[number, my_id],
                send_sem=sum_send,
                recv_sem=sum_recv.at[number],
                device_id=target,
                device_id_type=MESH,
            ).start()

    def end_sums(number):
        rows = sums_in.at[number, pl.ds(0, total_devices - 1)]
        pltpu.make_async_copy(rows, rows, sum_recv.at[number]).wait()
        lines = [sums_in[number, index] for index in range(total_devices)]
        while len(lines) > 1:
            lines = [
                lines[index] + lines[index + 1] if index + 1 < len(lines) else lines[index]
                for index in range(0, len(lines), 2)
            ]
        return jnp.broadcast_to(lines[0], (8, 128))

    def total_by(first_set, line, index):
        return gather(line, jnp.where(first_set, GROUP * 2 * index, GROUP * (2 * index + 1)))

    def as_rows(value):
        result = value
        for step in range(1, 8):
            moved = pltpu.roll(pltpu.roll(value, 8 - step, 0), GROUP * step, 1)
            result = jnp.where((group - row) % 8 == step, moved, result)
        return result

    def each(function, *vectors):
        return [function(k, *(vector[k] for vector in vectors)) for k in range(deep)]

    with scope("setup"):
        pltpu.make_async_copy(lines, lines, load_sem).wait()
        pltpu.make_async_copy(pairs_hbm, pairs_ref, send_sem).wait()
        pltpu.make_async_copy(count_hbm, count_ref, sum_send).wait()
        site_x = spacing * (place_x.astype(jnp.float32) + 0.5)
        site_y = spacing * (place_y.astype(jnp.float32) + 0.5)
        site_z = spacing * (row.astype(jnp.float32) + 0.5)
        polar, mask, source, geometry = [], [], [], []
        for k in range(deep):
            places = [
                rows_of(coords_ref[3 * k + part]) - offset
                for part, offset in enumerate((site_x, site_y, site_z))
            ]
            polar_k = rows_of(polar_ref[k])
            mask_k = jnp.where(unpack < count_ref[k], 1.0, 0.0)
            root = lax.rsqrt(polar_k)
            slot = 14 + jnp.where(
                place_x == 0, place_y, 4 + 3 * place_y + place_x - 1
            )
            flag = pairs_ref[k, 0, 0] == slot
            for entry in range(1, 13):
                flag = jnp.logical_or(flag, pairs_ref[k, 0, entry] == slot)
            flags = jnp.where(flag, 1.0 / cutoff_square**2, 0.0)
            geometry.append(packed(places + [root, flags]))
            for stage in range(3):
                for j in range(1, REACH + 1) if stage else [0]:
                    for part, value in enumerate(places + [thole * root]):
                        if stage:
                            shift_y = side_sign[stage] * j
                            value = pltpu.roll(value, lax.rem(128 + SIDE * shift_y, 128), 1)
                            if part == 1:
                                value = value - spacing * shift_y.astype(jnp.float32)
                        own_ref[page_of(stage, j), k, part] = value - far_x if part == 0 else value
            polar.append(polar_k)
            mask.append(mask_k)
            field_k = packed([rows_of(field_ref[6 * k + part]) for part in range(6)])
            source.append(field_k * mask_k)
        dipoles = each(lambda k, s: polar[k] * s, source)
        put_first(geometry, each(lambda k, d: d * mask[k], dipoles))
    with scope("barrier"):
        pl.semaphore_wait(barrier, len(greeted))
    with scope("send0"):
        exchange_first()

    def prepare(stage):
        with scope(f"geoarrive_{stage}"):
            arrival(0, stage)
        with scope(f"geo_{stage}"):
            tiles_in = merged_tiles(0, stage)
            spread_out(tiles_in, near_geo, 4, stage)
            build_switch(tiles_in, stage)

    image = operate(1, build_tile, dipoles, prepare)
    with scope("finish0"):
        residual = each(lambda k, s, a: s - a, source, image)
        precond = each(lambda k, r: polar[k] * r, residual)
        put(2, each(lambda k, p: p * mask[k], precond))
    with scope("send1"):
        exchange(2)
    image = operate(2, load_tile, precond)
    with scope("finish1"):
        turned = each(lambda k, q: polar[k] * q, image)
        put(3, each(lambda k, t: t * mask[k], turned))
        put_sums(0, [(residual, precond), (precond, image)])
    with scope("send2"):
        exchange(3, lambda: send_sums(0))
    turned_image = operate(3, load_tile, turned)
    with scope("sum1wait"):
        first_total = end_sums(0)
        norm, curve = (total_by(group < 3, first_total, index) for index in range(2))
    with scope("mid"):
        gamma = norm / curve
        dipoles = each(lambda k, d, p: d + gamma * p, dipoles, precond)
        residual = each(lambda k, r, q: r - gamma * q, residual, image)
        second = each(lambda k, r: polar[k] * r, residual)
        second_image = each(lambda k, q, t: q - gamma * t, image, turned_image)
        put_sums(
            1,
            [
                (residual, second), (second, second_image), (second, image),
                (precond, second_image),
            ],
        )
        send_sums(1)
    with scope("turn"):
        dipoles, residual, precond, second, image, second_image = (
            each(lambda k, value: as_rows(value), vector)
            for vector in (dipoles, residual, precond, second, image, second_image)
        )
        norm, curve = (total_by(row < 3, first_total, index) for index in range(2))
    with scope("sum2wait"):
        last_total = end_sums(1)
    with scope("out"):
        norm_next, second_curve, cross, cross_back = (
            total_by(row < 3, last_total, index) for index in range(4)
        )
        ratio = norm_next / norm
        gamma = norm_next / (second_curve + ratio * (cross + cross_back + ratio * curve))
        for k in range(deep):
            direction = second[k] + ratio * precond[k]
            along = second_image[k] + ratio * image[k]
            for out, value in (
                (dip_out, dipoles[k] + gamma * direction),
                (res_out, residual[k] - gamma * along),
            ):
                for part in range(6):
                    out[6 * k + part] = value[part : part + 1]
    with scope("sendwait"):
        rows = held.at[pl.ds(0, sum(middle + 2 * side for middle, side in rows_in))]
        pltpu.make_async_copy(rows, rows, send_sem).wait()
        rows = sums_in.at[:, pl.ds(0, total_devices - 1)]
        pltpu.make_async_copy(rows, rows, sum_send).wait()


def store(dipoles, residual, dip_out, res_out, sems):
    copies = [
        pltpu.make_async_copy(dipoles, dip_out, sems.at[0]),
        pltpu.make_async_copy(residual, res_out, sems.at[1]),
    ]
    for copy in copies:
        copy.start()
    for copy in copies:
        copy.wait()


def on_device(sizes, coords, polar, field, atom_count, pair_list):
    deep, slots = coords.shape[2], coords.shape[-1]
    assert coords.shape[0:2] == (1, 1) and slots == 128
    vmem = pl.BlockSpec(memory_space=pltpu.VMEM)
    hbm = pl.BlockSpec(memory_space=pl.ANY)
    rows = 8 * deep
    devices = sizes[0] * sizes[1] * sizes[2]
    rings = 1 if sizes[2] == 2 else 2
    tiles, counts = (plan(deep, rings)[index] for index in (2, 5))

    def buffer(*shape):
        return pltpu.VMEM(shape, jnp.float32)

    line = pltpu.VMEM((6 * deep, 1, slots), jnp.float32)
    result = jax.ShapeDtypeStruct((6 * deep, 1, slots), jnp.float32)
    dma = pltpu.SemaphoreType.DMA
    dipoles, residual = pl.pallas_call(
        functools.partial(kernel, sizes, deep),
        out_shape=(line, line),
        in_specs=[hbm] * 5,
        out_specs=(vmem, vmem),
        scratch_shapes=[
            pltpu.SMEM((deep, 1, pair_list.shape[-1]), jnp.int32),
            pltpu.SMEM((deep,), jnp.int32),
            buffer(10 * deep, 1, slots),
            buffer(4 * 8 * (deep + 2 * tiles + 3), slots),
            buffer(4 * 8 * (counts[0] + 2 * counts[1]), slots),
            buffer(8 * 2 * (deep + 1), slots),
            buffer(8 * 3 * 2 * (deep + rings), slots),
            buffer(PAGES, 6, rows + 16, slots),
            buffer(PAGES, 4, rows + 16, slots),
            buffer(PAGES, deep, 4, 8, slots),
            buffer(deep, PAGES, 24, slots),
            buffer(PAGES * SPAN * deep, 7, 8, slots),
            buffer(2, 1, slots),
            buffer(2, devices, 1, slots),
            dma,
            dma,
            dma((4, 3)),
            dma,
            dma((2,)),
        ],
        compiler_params=pltpu.CompilerParams(collective_id=0, has_side_effects=True),
    )(
        pair_list.reshape(deep, 1, -1),
        atom_count.reshape(deep),
        coords.reshape(3 * deep, 1, slots),
        polar.reshape(deep, 1, slots),
        field.reshape(6 * deep, 1, slots),
    )
    dipoles, residual = pl.pallas_call(
        store,
        out_shape=(result, result),
        in_specs=[vmem, vmem],
        out_specs=(hbm, hbm),
        scratch_shapes=[dma((2,))],
    )(
        pltpu.with_memory_space_constraint(dipoles, pltpu.VMEM),
        pltpu.with_memory_space_constraint(residual, pltpu.VMEM),
    )
    return dipoles.reshape(field.shape), residual.reshape(field.shape)


def solution(mesh):
    sizes = tuple(mesh.shape[name] for name in AXES)
    block = P(*AXES, None, None)
    return jax.shard_map(
        functools.partial(on_device, sizes),
        mesh=mesh,
        in_specs=(block, P(*AXES, None), block, P(*AXES), P(*AXES, None)),
        out_specs=(block, block),
        check_vma=False,
    )
```

```python
import functools
import math

import jax
import jax.numpy as jnp
from jax import lax
from jax.experimental import pallas as pl
from jax.experimental.pallas import tpu as pltpu
from jax.sharding import PartitionSpec as P

MESH = pl.DeviceIdType.MESH
AXES = ("gx", "gy", "gz")
spacing = 2.2
cutoff_square = 49.0
thole = 0.39
SIDE = 4
GROUP = SIDE * SIDE
REACH = 3
SHIFTS = range(-REACH, REACH + 1)
PAGES = 1 + 2 * REACH
SPAN = 2 * REACH + 1
ORDER = [(2, -1), (2, 1), (2, 0), (1, -1), (1, 1), (0, -1), (0, 1), (1, 0), (0, 0)]
COLUMNS = [(cx, cy) for cx in (-1, 0, 1) for cy in (-1, 0, 1)]
REST = 6
EDGE = 12
OWN = (0, 48)
LOW = ((48, 60, 72), (36, 96, 108))
HIGH = ((84, 96, 108), (0, 12, 24))
RIDE_LOW = 0
RIDE_HIGH = 36
WIDE_LOW = (84, 0)
WIDE_HIGH = (48, 12)
WIDE_FLAGS = 120
FLAGS = 4


def gather(value, index):
    return jnp.take_along_axis(value, index, axis=1, mode="promise_in_bounds")


def plan(deep, rings):
    riders = [k for k in range(deep) if k % 3 == 2]
    tile_of, tiles = {}, 0
    for k in range(deep):
        if k not in riders:
            tile_of[k] = tiles
            tiles += 1
    inner, halos, counts = {}, {}, {}
    for cy in (0, 1):
        total = 0
        for cx in (-1, 0, 1):
            if (cx, cy) != (0, 0):
                inner[cx, cy] = total
                total += tiles if cx else deep
        for cx in (-1, 0, 1):
            halos[cx, cy] = total
            total += rings
        counts[cy] = total
    return riders, tile_of, tiles, inner, halos, counts


def kernel(
    sizes, deep, pairs_hbm, count_hbm, coords_hbm, polar_hbm, field_hbm, dip_out, res_out,
    pairs_ref, count_ref, lines, send, held, send_wide, held_wide, near, near_geo, own_ref,
    switch, tensor, sums_out, sums_in, load_sem, send_sem, recv_sems, sum_send, sum_recv,
):
    total_devices = sizes[0] * sizes[1] * sizes[2]
    rings = 1 if sizes[2] == 2 else 2
    riders, tile_of, tiles, inner, halos, counts = plan(deep, rings)
    me = [lax.axis_index(name) for name in AXES]
    my_id = (me[0] * sizes[1] + me[1]) * sizes[2] + me[2]
    scope = jax.named_scope
    up = jnp.where(2 * me[1] < sizes[1], 1, 0)
    side_is_up = (None, up, 1 - up)
    side_sign = (None, 2 * up - 1, 1 - 2 * up)

    def device_at(linear):
        return (
            linear // (sizes[1] * sizes[2]),
            linear // sizes[2] % sizes[1],
            linear % sizes[2],
        )

    def neighbour(cx, cy, cz):
        return tuple(
            lax.rem(place + step + size, size)
            for place, step, size in zip(me, (cx, cy, cz), sizes)
        )

    with scope("signal"):
        barrier = pltpu.get_barrier_semaphore()
        if max(sizes) <= 5:
            steps = [(1, -1, 0) if size > 2 else (1, 0) for size in sizes]
            greeted = [
                neighbour(cx, cy, cz)
                for cx in steps[0] for cy in steps[1] for cz in steps[2]
                if (cx, cy, cz) != (0, 0, 0)
            ]
        else:
            greeted = [
                device_at(lax.rem(my_id + step, total_devices)) for step in range(1, total_devices)
            ]
        for target in greeted:
            pl.semaphore_signal(barrier, inc=1, device_id=target, device_id_type=MESH)
        coords_ref = lines.at[pl.ds(0, 3 * deep)]
        polar_ref = lines.at[pl.ds(3 * deep, deep)]
        field_ref = lines.at[pl.ds(4 * deep, 6 * deep)]
        for src, dst, sem in (
            (coords_hbm, coords_ref, load_sem),
            (polar_hbm, polar_ref, load_sem),
            (field_hbm, field_ref, load_sem),
            (pairs_hbm, pairs_ref, send_sem),
            (count_hbm, count_ref, sum_send),
        ):
            pltpu.make_async_copy(src, dst, sem).start()

    lane = lax.broadcasted_iota(jnp.int32, (8, 128), 1)
    row = lax.broadcasted_iota(jnp.int32, (8, 128), 0)
    group = lane // GROUP
    place_y = lane // SIDE % SIDE
    place_x = lane % SIDE
    site = lane % GROUP
    shift_x = group - REACH
    unpack = GROUP * row + site
    far_x = spacing * shift_x.astype(jnp.float32)

    def within(first, size):
        return jnp.logical_and(lane >= first, lane < first + size)

    def choose(cases, default):
        for condition, value in cases:
            default = jnp.where(condition, value, default)
        return default

    def edge_index(bases, at, first_x):
        cases = []
        for base, start in zip(bases, at):
            local = lane - base
            value = start + SIDE * (local // 3) + local % 3 + first_x
            cases.append((within(base, EDGE), value))
        return choose(cases, jnp.zeros_like(lane))

    all_parts = [GROUP * part for part in range(6)]
    take_low = edge_index(LOW[0] + LOW[1], all_parts, 1)
    take_high = edge_index(HIGH[0] + HIGH[1], all_parts, 0)
    ride_low = [
        edge_index([RIDE_LOW + EDGE * part for part in range(3)], all_parts[3 * s : 3 * s + 3], 1)
        for s in range(2)
    ]
    ride_high = [
        edge_index([RIDE_HIGH + EDGE * part for part in range(3)], all_parts[3 * s : 3 * s + 3], 0)
        for s in range(2)
    ]

    def unride(regions, starts):
        cases = []
        for bases, start in zip(regions, starts):
            for part, base in enumerate(bases):
                cases.append((within(base, EDGE), lane - base + start + EDGE * part))
        return choose(cases, jnp.zeros_like(lane))

    leave_low = unride(LOW, (RIDE_LOW, RIDE_LOW))
    leave_high = unride(HIGH, (RIDE_HIGH, RIDE_HIGH))
    part_low = unride(LOW, WIDE_LOW)
    part_high = unride(HIGH, WIDE_HIGH)
    wide_low, wide_high = (
        edge_index([at + EDGE * part for at in starts for part in range(3)], all_parts, first_x)
        for starts, first_x in ((WIDE_LOW, 1), (WIDE_HIGH, 0))
    )
    has_ninth = jnp.logical_or(row == 1, row == 7)
    flag = jnp.where(has_ninth, 8, jnp.maximum(lane - WIDE_FLAGS, 0))
    flag_lane = OWN[1] + GROUP * (FLAGS - 3) + SIDE * (flag // 3) + 1 + flag % 3
    take_wide_low = jnp.where(lane >= WIDE_FLAGS, flag_lane, take_low)

    def inside(bases, size):
        result = within(bases[0], size)
        for base in bases[1:]:
            result = jnp.logical_or(result, within(base, size))
        return result

    is_own = [within(OWN[s], 3 * GROUP) for s in range(2)]
    is_low = [inside(LOW[s], EDGE) for s in range(2)]

    reached = place_x + shift_x
    turn_x = []
    for part in range(6):
        s, c = part // 3, part % 3
        low = LOW[s][c] + 3 * place_y + reached + SIDE - 1
        high = HIGH[s][c] + 3 * place_y + jnp.minimum(reached - SIDE, 2)
        own = OWN[s] + GROUP * c + SIDE * place_y + reached
        turn_x.append(jnp.where(reached < 0, low, jnp.where(reached < SIDE, own, high)))

    def packed(parts):
        value = parts[0]
        for index in range(1, len(parts)):
            value = jnp.where(group == index, parts[index], value)
        return value

    def rows_of(line):
        return gather(jnp.broadcast_to(line, (8, 128)), unpack)

    MIDDLE = 0
    SENT = {0: 0, 1: deep + 1, -1: deep + 2 + tiles}
    HALO = {0: deep, 1: deep + 1 + tiles, -1: deep + 2 + 2 * tiles}

    sent_tiles = deep + 2 * tiles + 3
    held_tiles = counts[0] + 2 * counts[1]

    def sent_rows(phase, tile, amount=8):
        return pl.ds(8 * (phase * sent_tiles + tile), amount)

    def held_rows(phase, tile, amount=8):
        return pl.ds(pl.multiple_of(8 * (phase * held_tiles + tile), 8), amount)

    def put_tile(phase, tile, value):
        send[sent_rows(phase, tile), :] = value

    def ends(bottom, top):
        return jnp.where(row < REACH, bottom, pltpu.roll(top, REST, 0))

    def put_first(geometry, vector):
        for phase, blocks in ((0, geometry), (1, vector)):
            put_middle(phase, blocks)
        for place, take, part, is_part in (
            (0, take_wide_low, wide_low, inside((0, 84), 3 * EDGE)),
            (deep + 1, take_high, wide_high, within(12, 6 * EDGE)),
        ):
            cut = [
                jnp.where(is_part, gather(vector[k], part), gather(geometry[k], take))
                for k in range(deep)
            ]
            for index, value in enumerate(cut + [ends(cut[0], cut[-1])]):
                send_wide[pl.ds(8 * (place + index), 8), :] = value

    def put_middle(phase, blocks):
        for k in range(deep):
            put_tile(phase, MIDDLE + k, blocks[k])
        put_tile(phase, HALO[0], ends(blocks[0], blocks[deep - 1]))

    def put(phase, blocks):
        last = deep - 1
        put_middle(phase, blocks)
        for direction, take, ride, ride_at in (
            (1, take_low, ride_low, RIDE_LOW),
            (-1, take_high, ride_high, RIDE_HIGH),
        ):
            cut = {k: gather(blocks[k], take) for k in range(deep) if k not in riders or k == last}
            put_tile(phase, HALO[direction], ends(cut[0], cut[last]))
            for rider in riders:
                for s in range(2):
                    host = rider - 2 + s
                    cut[host] = jnp.where(
                        within(ride_at, 3 * EDGE), gather(blocks[rider], ride[s]), cut[host]
                    )
            for k in tile_of:
                put_tile(phase, SENT[direction] + tile_of[k], cut[k])

    def exchange(phase, between=None):
        def start(phase, src, at, stage, rows, target):
            place = counts[0] + counts[1] * (1 - side_is_up[stage]) if stage else 0
            pltpu.make_async_remote_copy(
                src_ref=send.at[sent_rows(phase, src, rows)],
                dst_ref=held.at[held_rows(phase, place + at, rows)],
                send_sem=send_sem,
                recv_sem=recv_sems.at[phase, 1 - side_sign[stage] if stage else 1],
                device_id=target,
                device_id_type=MESH,
            ).start()

        for index, (stage, cx) in enumerate(ORDER):
            if index == 2 and between is not None:
                between()
            cy = side_sign[stage] if stage else 0
            far = 1 if stage else 0
            if stage or cx:
                rows = 8 * (tiles if cx else deep)
                start(phase, SENT[cx], inner[-cx, far], stage, rows, neighbour(cx, cy, 0))
            for ring in range(rings):
                at = halos[-cx, far] + ring
                target = neighbour(cx, cy, -1 if ring == 0 else 1)
                start(phase, HALO[cx], at, stage, REST, target)

    wide_count = 2 * (deep + rings)

    def first_wide(stage):
        return wide_count * (1 + side_is_up[stage]) if stage else 0

    def wide_place(cx, ring=None):
        right = 1 if cx > 0 else 0
        return right * deep if ring is None else 2 * deep + right * rings + ring

    def wide_rows(stage, place, amount=8):
        return pl.ds(pl.multiple_of(8 * (first_wide(stage) + place), 8), amount)

    def exchange_first():
        def start(phase, src, dst, stage, target):
            pltpu.make_async_remote_copy(
                src_ref=src,
                dst_ref=dst,
                send_sem=send_sem,
                recv_sem=recv_sems.at[phase, 1 - side_sign[stage] if stage else 1],
                device_id=target,
                device_id_type=MESH,
            ).start()

        for phase in range(2):
            for stage, cx in ORDER:
                cy = side_sign[stage] if stage else 0
                far = 1 if stage else 0
                opposite = 3 - stage if stage else 0
                rows = 8 * deep
                if cx and phase == 0:
                    place = 0 if cx > 0 else deep + 1
                    start(
                        0,
                        send_wide.at[pl.ds(8 * place, rows)],
                        held_wide.at[wide_rows(opposite, wide_place(-cx), rows)],
                        stage,
                        neighbour(cx, cy, 0),
                    )
                    for ring in range(rings):
                        start(
                            0,
                            send_wide.at[pl.ds(8 * (place + deep), REST)],
                            held_wide.at[wide_rows(opposite, wide_place(-cx, ring), REST)],
                            stage,
                            neighbour(cx, cy, -1 if ring == 0 else 1),
                        )
                if not cx:
                    first = first_tile(opposite)
                    if stage:
                        start(
                            phase,
                            send.at[sent_rows(phase, SENT[0], rows)],
                            held.at[held_rows(phase, first + inner[0, far], rows)],
                            stage,
                            neighbour(0, cy, 0),
                        )
                    for ring in range(rings):
                        start(
                            phase,
                            send.at[sent_rows(phase, HALO[0], REST)],
                            held.at[held_rows(phase, first + halos[0, far] + ring, REST)],
                            stage,
                            neighbour(0, cy, -1 if ring == 0 else 1),
                        )

    def first_tile(stage):
        return counts[0] + counts[1] * side_is_up[stage] if stage else 0

    rows_in = []
    for phase in range(4):
        if phase < 2:
            sides = 2 * (8 * deep + REST * rings) if phase == 0 else 0
            rows_in.append([sides + REST * rings, sides + REST * rings + 8 * deep])
        else:
            rows_in.append([8 * counts[far] - (8 - REST) * 3 * rings for far in (0, 1)])

    def arrival(phase, stage):
        start = first_tile(stage) if phase > 1 else 0
        rows = held.at[held_rows(phase, start, rows_in[phase][1 if stage else 0])]
        which = 1 + side_sign[stage] if stage else 1
        pltpu.make_async_copy(rows, rows, recv_sems.at[phase, which]).wait()

    def joined(below, above):
        return jnp.where(row < 4, below, pltpu.roll(above, 8 - REST, 0))

    def wide_tile(stage, cx, v):
        if v:
            return held_wide[wide_rows(stage, wide_place(cx) + v - 1), :]
        return joined(
            held_wide[wide_rows(stage, wide_place(cx, 0)), :],
            held_wide[wide_rows(stage, wide_place(cx, rings - 1)), :],
        )

    def merged_tiles(phase, stage):
        first = first_tile(stage)
        far = 1 if stage else 0

        def halo(cx):
            at = first + halos[cx, far]
            return joined(
                held[held_rows(phase, at), :], held[held_rows(phase, at + rings - 1), :]
            )

        def tile(cx, number):
            return held[held_rows(phase, first + inner[cx, far] + number), :]

        wide = []
        for v in range(deep + 1) if phase < 2 else []:
            low, high = wide_tile(stage, -1, v), wide_tile(stage, 1, v)
            if phase == 1:
                low, high = gather(low, part_low), gather(high, part_high)
            wide.append((low, high))
        both = []
        for s in range(2):
            row_of_tiles = []
            for v in range(deep + 1):
                k = v - 1
                if wide:
                    low, high = wide[v]
                    if v == 0:
                        own = halo(0)
                    else:
                        own = tile(0, k) if stage else send[sent_rows(phase, MIDDLE + k), :]
                elif v == 0:
                    low, own, high = halo(-1), halo(0), halo(1)
                else:
                    own = tile(0, k) if stage else send[sent_rows(phase, MIDDLE + k), :]
                    if k in riders:
                        host = tile_of[k - 2 + s]
                        low = gather(tile(-1, host), leave_low)
                        high = gather(tile(1, host), leave_high)
                    else:
                        low, high = tile(-1, tile_of[k]), tile(1, tile_of[k])
                row_of_tiles.append(jnp.where(is_own[s], own, jnp.where(is_low[s], low, high)))
            both.append(row_of_tiles)
        return both

    def page_of(stage, j):
        return REACH * (stage - 1) + j if stage else 0

    depth_y = [None] + [
        jnp.where(side_is_up[stage] > 0, place_y, SIDE - 1 - place_y) for stage in (1, 2)
    ]

    def spread_out(tiles_in, out, parts, stage):
        for v in range(deep + 1):
            for part in range(parts):
                value = gather(tiles_in[part // 3][v], turn_x[part])
                pages = {0: value}
                if stage:
                    base = out[0, part, pl.ds(8 * v, 8), :]
                    pages = {
                        page_of(stage, j): jnp.where(depth_y[stage] < j, value, base)
                        for j in range(1, REACH + 1)
                    }
                for page, value in pages.items():
                    out[page, part, pl.ds(8 * v, 8), :] = value
                    if v == 0:
                        out[page, part, pl.ds(8 * (deep + 1), 8), :] = value

    def contract(sums, parts, vec):
        dx, dy, dz, tx, ty, tz, three = parts
        for first in (0, 3):
            vx, vy, vz = vec[first : first + 3]
            along = tx * vx + ty * vy + tz * vz
            for part, (d, v) in enumerate(((dx, vx), (dy, vy), (dz, vz))):
                term = d * along - three * v
                at = first + part
                sums[at] = term if sums[at] is None else sums[at] + term

    def tile_number(k, page, sz):
        return (k * PAGES + page) * SPAN + sz + REACH

    def build_tile(k, page, sz):
        start = 8 + sz
        span = pl.ds(8 * k + start, 8)
        dx = near_geo[page, 0, span, :] - own_ref[page, k, 0]
        dy = near_geo[page, 1, span, :] - own_ref[page, k, 1]
        dz = near_geo[page, 2, span, :] - (own_ref[page, k, 2] - spacing * sz)
        weight = switch[k, page, pl.ds(start, 8), :]
        if page == 0 and sz == 0:
            weight = jnp.where(group == REACH, 0.0, weight)
        square = dx * dx + dy * dy + dz * dz
        if page == 0 and sz == 0:
            square = jnp.maximum(square, 1.0)
        inverse = lax.rsqrt(square)
        inverse_square = inverse * inverse
        damp = square * (square * inverse) * (near_geo[page, 3, span, :] * own_ref[page, k, 3])
        damping = jnp.exp2(damp * (-1.0 / math.log(2.0)))
        fade = jnp.maximum(cutoff_square - square, 0.0)
        scale = fade * fade * (inverse_square * inverse) * weight
        three = scale - scale * damping
        five = (three - scale * (damp * damping)) * (3.0 * inverse_square)
        parts = (dx, dy, dz, five * dx, five * dy, five * dz, three)
        for part, value in enumerate(parts):
            tensor[tile_number(k, page, sz), part] = value
        return parts

    def load_tile(k, page, sz):
        return [tensor[tile_number(k, page, sz), part] for part in range(7)]

    def back_roll(stage, j):
        return lax.rem(128 - SIDE * side_sign[stage] * j, 128) if stage else 0

    def gather_groups(sums, stage, j, total):
        back = back_roll(stage, j)
        ends_in = (lane + back) // GROUP % 8
        first, second = total
        for step in range(4):
            comes = (ends_in + step) % 4
            quad = sums[3]
            for part in range(3):
                quad = jnp.where(comes == part, sums[part], quad)
            pair = jnp.where(comes % 2 == 0, sums[4], sums[5])
            shift = back + GROUP * step
            if stage:
                shift = lax.rem(shift, 128)
            if stage or step:
                quad, pair = pltpu.roll(quad, shift, 1), pltpu.roll(pair, shift, 1)
            first = quad if first is None else first + quad
            second = pair if second is None else second + pair
        return first, second

    upper = group >= 4

    def fold(total):
        kept = jnp.where(upper, total[1], total[0])
        moved = jnp.where(upper, total[0], total[1])
        return kept + pltpu.roll(moved, 64, 1)

    def used(stage):
        for j in range(1, REACH + 1) if stage else [0]:
            yield j, [sz for sz in SHIFTS if j < REACH or abs(sz) < REACH]

    def stage_tiles(stage, k):
        for j, shifts in used(stage):
            for sz in shifts:
                build_tile(k, page_of(stage, j), sz)

    def stage_sums(make_tile, stage, k):
        result = []
        for j, shifts in used(stage):
            sums = [None] * 6
            page = page_of(stage, j)
            for sz in shifts:
                span = pl.ds(8 * k + 8 + sz, 8)
                vec = [near[page, part, span, :] for part in range(6)]
                contract(sums, make_tile(k, page, sz), vec)
            result.append((sums, stage, j))
        return result

    def operate(phase, make_tile, vector, prepare=None):
        totals = [(None, None)] * deep
        waiting = [[] for _ in range(deep)]
        image = []
        for stage in range(3):
            if prepare is not None:
                prepare(stage)
            if prepare is not None and stage == 2:
                with scope("tiles"):
                    for k in range(deep):
                        stage_tiles(stage, k)
                make_tile = load_tile
            with scope(f"arrive{phase}_{stage}"):
                arrival(phase, stage)
            with scope(f"stage{phase}_{stage}"):
                spread_out(merged_tiles(phase, stage), near, 6, stage)
                for k in range(deep):
                    for item in waiting[k]:
                        totals[k] = gather_groups(*item, totals[k])
                    waiting[k] = stage_sums(make_tile, stage, k)
                    if stage == 2:
                        for item in waiting[k]:
                            totals[k] = gather_groups(*item, totals[k])
                        image.append(vector[k] / polar[k] - mask[k] * fold(totals[k]))
        return image

    def build_switch(tiles_in, stage):
        def full(at):
            return jnp.broadcast_to(jnp.asarray(at, jnp.int32), (8, 128))

        own_lane = OWN[1] + GROUP * (FLAGS - 3)

        def same_rows(tile, low_row, high_row):
            return jnp.where(row < 4, tile[low_row : low_row + 1], tile[high_row : high_row + 1])

        cy = side_sign[stage] if stage else 0
        for cz in (-1, 0, 1):
            low_flag = 7 - 3 * (cy + 1) - cz
            ninth = low_flag == 8 if stage and cz == -1 else None
            low_at = low_flag if ninth is None else jnp.where(ninth, 0, low_flag)
            low_at = full(WIDE_FLAGS + low_at)
            high_at = full(own_lane + SIDE * (cy + 1) + cz + 2)
            middle_at = full(own_lane + SIDE * (2 + cy * cz) if stage else own_lane)
            ours = jnp.where(reached < SIDE, middle_at, high_at)
            ahead = cy > 0 if stage else cz > 0
            use_own = jnp.where(ahead, reached, reached - SIDE) >= 0
            for k in range(deep):
                v = (k + 1 + cz) % (deep + 1)
                tile = wide_tile(stage, -1, v)
                flags = same_rows(tile, 0, 6)
                if ninth is not None:
                    flags = jnp.where(ninth, same_rows(tile, 1, 7), flags)
                there = jnp.where(
                    reached < 0, gather(flags, low_at), gather(tiles_in[1][v], middle_at)
                )
                here = gather(send[sent_rows(0, MIDDLE + k), :], ours)
                value = jnp.where(use_own, here, there)
                if stage == 0 and cz == 0:
                    inside_own = jnp.logical_and(reached >= 0, reached < SIDE)
                    value = jnp.where(inside_own, 1.0 / cutoff_square**2, value)
                value = jnp.where(group < SPAN, value, 0.0)
                span = pl.ds(8 * (cz + 1), 8)
                if stage == 0:
                    switch[k, 0, span, :] = value
                for j in range(1, REACH + 1) if stage else []:
                    switch[k, page_of(stage, j), span, :] = jnp.where(
                        depth_y[stage] < j, value, switch[k, 0, span, :]
                    )

    everyone = []
    for far in list(range(1, sizes[1])) + [0]:
        y = lax.rem(me[1] + side_sign[2] * far + sizes[1], sizes[1])
        for cx in range(sizes[0]):
            x = lax.rem(me[0] + cx, sizes[0])
            for cz in range(sizes[2]):
                if far or cx or cz:
                    everyone.append((x, y, lax.rem(me[2] + cz, sizes[2])))

    in_set = [group < 3, jnp.logical_and(group >= 3, group < 6)]

    def put_sums(number, products):
        values = []
        for first, second in products:
            value = first[0] * second[0]
            for k in range(1, deep):
                value = value + first[k] * second[k]
            line = jnp.sum(value, axis=0, keepdims=True)
            for s in range(2):
                chosen = jnp.where(in_set[s][0:1], line, 0.0)
                values.append(jnp.sum(chosen, axis=1, keepdims=True))
        line = jnp.broadcast_to(values[0], (1, 128))
        for index in range(1, len(values)):
            line = jnp.where(group[0:1] == index, values[index], line)
        sums_out[number] = line
        sums_in[number, my_id] = line

    def send_sums(number):
        for target in everyone:
            pltpu.make_async_remote_copy(
                src_ref=sums_out.at[number],
                dst_ref=sums_in.at[number, my_id],
                send_sem=sum_send,
                recv_sem=sum_recv.at[number],
                device_id=target,
                device_id_type=MESH,
            ).start()

    def end_sums(number):
        rows = sums_in.at[number, pl.ds(0, total_devices - 1)]
        pltpu.make_async_copy(rows, rows, sum_recv.at[number]).wait()
        lines = [sums_in[number, index] for index in range(total_devices)]
        while len(lines) > 1:
            lines = [
                lines[index] + lines[index + 1] if index + 1 < len(lines) else lines[index]
                for index in range(0, len(lines), 2)
            ]
        return jnp.broadcast_to(lines[0], (8, 128))

    def total_by(first_set, line, index):
        return gather(line, jnp.where(first_set, GROUP * 2 * index, GROUP * (2 * index + 1)))

    def as_rows(value):
        result = value
        for step in range(1, 8):
            moved = pltpu.roll(pltpu.roll(value, 8 - step, 0), GROUP * step, 1)
            result = jnp.where((group - row) % 8 == step, moved, result)
        return result

    def each(function, *vectors):
        return [function(k, *(vector[k] for vector in vectors)) for k in range(deep)]

    with scope("setup"):
        pltpu.make_async_copy(lines, lines, load_sem).wait()
        pltpu.make_async_copy(pairs_hbm, pairs_ref, send_sem).wait()
        pltpu.make_async_copy(count_hbm, count_ref, sum_send).wait()
        site_x = spacing * (place_x.astype(jnp.float32) + 0.5)
        site_y = spacing * (place_y.astype(jnp.float32) + 0.5)
        site_z = spacing * (row.astype(jnp.float32) + 0.5)
        polar, mask, source, geometry = [], [], [], []
        for k in range(deep):
            places = [
                rows_of(coords_ref[3 * k + part]) - offset
                for part, offset in enumerate((site_x, site_y, site_z))
            ]
            polar_k = rows_of(polar_ref[k])
            mask_k = jnp.where(unpack < count_ref[k], 1.0, 0.0)
            root = lax.rsqrt(polar_k)
            slot = 14 + jnp.where(
                place_x == 0, place_y, 4 + 3 * place_y + place_x - 1
            )
            flag = pairs_ref[k, 0, 0] == slot
            for entry in range(1, 13):
                flag = jnp.logical_or(flag, pairs_ref[k, 0, entry] == slot)
            flags = jnp.where(flag, 1.0 / cutoff_square**2, 0.0)
            geometry.append(packed(places + [root, flags]))
            for stage in range(3):
                for j in range(1, REACH + 1) if stage else [0]:
                    for part, value in enumerate(places + [thole * root]):
                        if stage:
                            shift_y = side_sign[stage] * j
                            value = pltpu.roll(value, lax.rem(128 + SIDE * shift_y, 128), 1)
                            if part == 1:
                                value = value - spacing * shift_y.astype(jnp.float32)
                        own_ref[page_of(stage, j), k, part] = value - far_x if part == 0 else value
            polar.append(polar_k)
            mask.append(mask_k)
            field_k = packed([rows_of(field_ref[6 * k + part]) for part in range(6)])
            source.append(field_k * mask_k)
        dipoles = each(lambda k, s: polar[k] * s, source)
        put_first(geometry, each(lambda k, d: d * mask[k], dipoles))
    with scope("barrier"):
        pl.semaphore_wait(barrier, len(greeted))
    with scope("send0"):
        exchange_first()

    def prepare(stage):
        with scope(f"geoarrive_{stage}"):
            arrival(0, stage)
        with scope(f"geo_{stage}"):
            tiles_in = merged_tiles(0, stage)
            spread_out(tiles_in, near_geo, 4, stage)
            build_switch(tiles_in, stage)

    image = operate(1, build_tile, dipoles, prepare)
    with scope("finish0"):
        residual = each(lambda k, s, a: s - a, source, image)
        precond = each(lambda k, r: polar[k] * r, residual)
        put(2, each(lambda k, p: p * mask[k], precond))
    with scope("send1"):
        exchange(2)
    image = operate(2, load_tile, precond)
    with scope("finish1"):
        turned = each(lambda k, q: polar[k] * q, image)
        put(3, each(lambda k, t: t * mask[k], turned))
        put_sums(0, [(residual, precond), (precond, image)])
    with scope("send2"):
        exchange(3, lambda: send_sums(0))
    turned_image = operate(3, load_tile, turned)
    with scope("sum1wait"):
        first_total = end_sums(0)
        norm, curve = (total_by(group < 3, first_total, index) for index in range(2))
    with scope("mid"):
        gamma = norm / curve
        dipoles = each(lambda k, d, p: d + gamma * p, dipoles, precond)
        residual = each(lambda k, r, q: r - gamma * q, residual, image)
        second = each(lambda k, r: polar[k] * r, residual)
        second_image = each(lambda k, q, t: q - gamma * t, image, turned_image)
        put_sums(
            1,
            [
                (residual, second), (second, second_image), (second, image),
                (precond, second_image),
            ],
        )
        send_sums(1)
    with scope("turn"):
        dipoles, residual, precond, second, image, second_image = (
            each(lambda k, value: as_rows(value), vector)
            for vector in (dipoles, residual, precond, second, image, second_image)
        )
        norm, curve = (total_by(row < 3, first_total, index) for index in range(2))
    with scope("sum2wait"):
        last_total = end_sums(1)
    with scope("out"):
        norm_next, second_curve, cross, cross_back = (
            total_by(row < 3, last_total, index) for index in range(4)
        )
        ratio = norm_next / norm
        gamma = norm_next / (second_curve + ratio * (cross + cross_back + ratio * curve))
        for k in range(deep):
            direction = second[k] + ratio * precond[k]
            along = second_image[k] + ratio * image[k]
            for out, value in (
                (dip_out, dipoles[k] + gamma * direction),
                (res_out, residual[k] - gamma * along),
            ):
                for part in range(6):
                    out[6 * k + part] = value[part : part + 1]
    with scope("sendwait"):
        rows = held.at[pl.ds(0, sum(middle + 2 * side for middle, side in rows_in))]
        pltpu.make_async_copy(rows, rows, send_sem).wait()
        rows = sums_in.at[:, pl.ds(0, total_devices - 1)]
        pltpu.make_async_copy(rows, rows, sum_send).wait()


def store(dipoles, residual, dip_out, res_out, sems):
    copies = [
        pltpu.make_async_copy(dipoles, dip_out, sems.at[0]),
        pltpu.make_async_copy(residual, res_out, sems.at[1]),
    ]
    for copy in copies:
        copy.start()
    for copy in copies:
        copy.wait()


def on_device(sizes, coords, polar, field, atom_count, pair_list):
    deep, slots = coords.shape[2], coords.shape[-1]
    assert coords.shape[0:2] == (1, 1) and slots == 128
    vmem = pl.BlockSpec(memory_space=pltpu.VMEM)
    hbm = pl.BlockSpec(memory_space=pl.ANY)
    rows = 8 * deep
    devices = sizes[0] * sizes[1] * sizes[2]
    rings = 1 if sizes[2] == 2 else 2
    tiles, counts = (plan(deep, rings)[index] for index in (2, 5))

    def buffer(*shape):
        return pltpu.VMEM(shape, jnp.float32)

    line = pltpu.VMEM((6 * deep, 1, slots), jnp.float32)
    result = jax.ShapeDtypeStruct((6 * deep, 1, slots), jnp.float32)
    dma = pltpu.SemaphoreType.DMA
    dipoles, residual = pl.pallas_call(
        functools.partial(kernel, sizes, deep),
        out_shape=(line, line),
        in_specs=[hbm] * 5,
        out_specs=(vmem, vmem),
        scratch_shapes=[
            pltpu.SMEM((deep, 1, pair_list.shape[-1]), jnp.int32),
            pltpu.SMEM((deep,), jnp.int32),
            buffer(10 * deep, 1, slots),
            buffer(4 * 8 * (deep + 2 * tiles + 3), slots),
            buffer(4 * 8 * (counts[0] + 2 * counts[1]), slots),
            buffer(8 * 2 * (deep + 1), slots),
            buffer(8 * 3 * 2 * (deep + rings), slots),
            buffer(PAGES, 6, rows + 16, slots),
            buffer(PAGES, 4, rows + 16, slots),
            buffer(PAGES, deep, 4, 8, slots),
            buffer(deep, PAGES, 24, slots),
            buffer(PAGES * SPAN * deep, 7, 8, slots),
            buffer(2, 1, slots),
            buffer(2, devices, 1, slots),
            dma,
            dma,
            dma((4, 3)),
            dma,
            dma((2,)),
        ],
        compiler_params=pltpu.CompilerParams(collective_id=0, has_side_effects=True),
    )(
        pair_list.reshape(deep, 1, -1),
        atom_count.reshape(deep),
        coords.reshape(3 * deep, 1, slots),
        polar.reshape(deep, 1, slots),
        field.reshape(6 * deep, 1, slots),
    )
    dipoles, residual = pl.pallas_call(
        store,
        out_shape=(result, result),
        in_specs=[vmem, vmem],
        out_specs=(hbm, hbm),
        scratch_shapes=[dma((2,))],
    )(
        pltpu.with_memory_space_constraint(dipoles, pltpu.VMEM),
        pltpu.with_memory_space_constraint(residual, pltpu.VMEM),
    )
    return dipoles.reshape(field.shape), residual.reshape(field.shape)


def solution(mesh):
    sizes = tuple(mesh.shape[name] for name in AXES)
    block = P(*AXES, None, None)
    return jax.shard_map(
        functools.partial(on_device, sizes),
        mesh=mesh,
        in_specs=(block, P(*AXES, None), block, P(*AXES), P(*AXES, None)),
        out_specs=(block, block),
        check_vma=False,
    )
```
